32 devices in a mesh: dp: 8 (over y, x, core), tensor: 4 (over z).
Axes of the slice: x: 2, y: 2, z: 4, core: 2. Of those that a mesh axis runs over, the one named last changes fastest.
Arguments:
- frames: bfloat16 [1024, 4, 84, 84], P(('dp', 'tensor')), may hold values from 0 to 1
- counts: int32 [4, 8], replicated, may hold values from 1 to 32, 128 in all within a row
- slot_ids: int32 [8, 64], P('dp'), may hold values from 0 to 127, as said below
- reset_flags: int32 [8, 128], P('dp'), may hold values 0 or 1
- hidden_state: float32 [2048, 1024], P('tensor', 'dp'), may hold values from -1 to 1
- cell_state: float32 [2048, 1024], P('tensor', 'dp'), may hold values from -6 to 6
- conv_first: bfloat16 [16, 4, 3, 3], replicated, may hold values from -1.5 to 1.5
- conv_second: bfloat16 [32, 16, 3, 3], replicated, may hold values from -0.75 to 0.75
- conv_third: bfloat16 [32, 32, 3, 3], replicated, may hold values from -0.5 to 0.5
- res_first: bfloat16 [32, 32, 3, 3], replicated, may hold values from -0.5 to 0.5
- res_second: bfloat16 [32, 32, 3, 3], replicated, may hold values from -0.5 to 0.5
- projection: bfloat16 [256, 3872], replicated, may hold values from -0.125 to 0.125
- input_weight: bfloat16 [4, 2048, 256], P(None, 'tensor'), may hold values from -0.375 to 0.375
- recur_weight: bfloat16 [4, 2048, 2048], P(None, 'tensor'), may hold values from -0.125 to 0.125
- gate_bias: float32 [4, 2048], P(None, 'tensor'), may hold values from -3 to 3
- head_weight: bfloat16 [19, 2048], P(None, 'tensor'), may hold values from -0.125 to 0.125
Outputs:
- policy_out: float32 [19, 1024], P(None, ('dp', 'tensor'))
- hidden_after: float32 [2048, 1024], P('tensor', 'dp')
- cell_after: float32 [2048, 1024], P('tensor', 'dp')
The draws below stay inside these ranges and needn't reach their ends.
Inputs may be any that keep to these rules, and one draw needn't show every extreme that they name: Arrival rows fill the first counts[t, a] slots of their device; each row of counts sums to 128. `slot_ids`: the entries of one dp index are distinct.
All inputs are finite; a program needn't handle non-finite values. No bound on the sum of `reset_flags` on one device may be relied on, other than what follows from the above.
Results may differ from the reference program's by a relative error of at most 0.008.
Values may be sent and summed in bfloat16 or wider, within the bound.
No kernel may reach another device: no remote copies, remote signals or barrier semaphores. Data moves between devices by JAX's collectives and lax.ppermute only.
A program may use at most 128 MiB of HBM per device.

```python
import math
import jax
import jax.numpy as jnp
import numpy as np
from jax import lax

STACK = 4
FRAME = 84
C1 = 16
C2 = 32
FLAT = 3872
FEAT = 256
H = 2048
ACTIONS = 18
ROWS_DEV = 16
CAP = 32
ROWS_GRP = 64
SLOTS = 128
ARRIVE = 1024
N_DP = 8
N_TENSOR = 4


def draw_slot_ids(key, part):
    keys = jax.random.split(jax.random.fold_in(key, 17), N_DP)

    def one_group(group_key):
        return jax.random.permutation(group_key, SLOTS)[:ROWS_GRP].astype(jnp.int32)
    return jax.vmap(one_group)(keys)


def place_ends(entries, own_key, least, largest):
    longest = entries.shape.index(max(entries.shape))
    spots = []
    for shift in (0, 1):
        where = [jax.random.randint(jax.random.fold_in(own_key, axis), (), 0, length) for axis, length in enumerate(entries.shape)]
        where[longest] = (where[longest] + shift) % entries.shape[longest]
        spots.append(tuple(where))
    return entries.at[spots[0]].set(least).at[spots[1]].set(largest)


def block_scale(rng, extent, pieces, smallest, largest):
    loudness, own = 1.0, jax.random.fold_in(rng, 6)
    for dim, shards_of in pieces:
        heights = jnp.exp(jax.random.uniform(jax.random.fold_in(own, dim), (shards_of,), jnp.float32, smallest / len(pieces), largest / len(pieces)))
        loudness = loudness * jnp.repeat(heights, extent[dim] // shards_of).reshape([-1 if axis == dim else 1 for axis in range(len(extent))])
    return loudness


def length_profile(amount, total, limit, skew):
    weights = [(1 << 20) // math.isqrt(grade ** skew) + 1 for grade in range(2, amount + 1)]
    surplus, holding = total - limit - (amount - 1), [1] * (amount - 1)
    while surplus > 0:
        movable = [i for i in range(amount - 1) if holding[i] < limit]
        mass, left = sum([weights[i] for i in movable]), surplus
        for i in movable:
            addition = min(limit - holding[i], max(1, left * weights[i] // mass), surplus)
            holding[i] = holding[i] + addition
            surplus = surplus - addition
    return np.array([limit] + holding)


def ragged_sizes(stream_key, number_of, total, most, lean):
    if number_of == 2:
        one = jax.random.randint(stream_key, (), max(1, total - most), min(most, total - 1) + 1)
        return jnp.stack([one, total - one])
    tallies = jnp.asarray(length_profile(number_of, total, most, lean), jnp.int32)
    twos = (number_of - 1) // 2
    giver, taker = tallies[1:1 + 2 * twos:2], tallies[2:2 + 2 * twos:2]
    slack = jnp.minimum(giver - 1, most - taker)
    moved = jax.random.randint(jax.random.fold_in(stream_key, 1), (twos,), 0, 1 << 20) % (slack + 1)
    tallies = tallies.at[1:1 + 2 * twos:2].set(giver - moved).at[2:2 + 2 * twos:2].set(taker + moved)
    return tallies[jax.random.permutation(jax.random.fold_in(stream_key, 2), number_of)]


def gaussian(key, extent, scale, limit, pieces=(), kind=jnp.bfloat16):
    loudness = block_scale(key, extent, pieces, -0.22, 0.18) if pieces else 1.0
    array = jax.random.normal(key, extent, jnp.float32) * scale * loudness
    return jnp.minimum(jnp.maximum(array, -limit), limit).astype(kind)


def setup_inputs(seed: int = 0) -> dict:
    key_list = jax.random.split(jax.random.key(seed), 17)
    return {
        "frames": jnp.clip(1.0 * jax.random.uniform(key_list[0], (ARRIVE, STACK, FRAME, FRAME), jnp.float32) ** block_scale(key_list[0], (ARRIVE, STACK, FRAME, FRAME), ((0, 32),), -0.2, 0.2), 0.0, 1.0).astype(jnp.bfloat16),
        "counts": jax.vmap(lambda own: ragged_sizes(own, N_DP, ROWS_DEV * N_DP, CAP, 2))(jax.random.split(key_list[1], N_TENSOR)).reshape((N_TENSOR, N_DP)).astype(jnp.int32),
        "slot_ids": draw_slot_ids(jax.random.fold_in(key_list[16], 71), 0),
        "reset_flags": place_ends((jax.random.randint(key_list[3], (N_DP, SLOTS), 0, 4) < 1).astype(jnp.int32), jax.random.fold_in(key_list[3], 1), 0, 1),
        "hidden_state": jnp.clip(jax.random.uniform(key_list[4], (H, N_DP * SLOTS), jnp.float32, -1.0, 1.0) * block_scale(key_list[4], (H, N_DP * SLOTS), ((0, 4), (1, 8)), -0.4, 0.0), -1.0, 1.0),
        "cell_state": gaussian(key_list[5], (H, N_DP * SLOTS), 1.0, 6.0, ((0, 4), (1, 8)), jnp.float32),
        "conv_first": gaussian(key_list[6], (C1, STACK, 3, 3), 18 ** -0.5, 1.5),
        "conv_second": gaussian(key_list[7], (C2, C1, 3, 3), 72 ** -0.5, 0.75),
        "conv_third": gaussian(key_list[8], (C2, C2, 3, 3), 144 ** -0.5, 0.5),
        "res_first": gaussian(key_list[9], (C2, C2, 3, 3), 144 ** -0.5, 0.5),
        "res_second": gaussian(key_list[10], (C2, C2, 3, 3), 144 ** -0.5, 0.5),
        "projection": gaussian(key_list[11], (FEAT, FLAT), (FLAT // 2) ** -0.5, 0.125),
        "input_weight": gaussian(key_list[12], (4, H, FEAT), FEAT ** -0.5, 0.375, ((1, 4),)),
        "recur_weight": gaussian(key_list[13], (4, H, H), H ** -0.5, 0.125, ((1, 4),)),
        "gate_bias": gaussian(key_list[14], (4, H), 0.5, 3.0, ((1, 4),), jnp.float32),
        "head_weight": gaussian(key_list[15], (ACTIONS + 1, H), H ** -0.5, 0.125, ((1, 4),)),
    }


def rounded(values):
    return lax.optimization_barrier(values.astype(jnp.bfloat16)).astype(jnp.float32)


def conv_same(inputs, kernel):
    return lax.conv_general_dilated(inputs, kernel.astype(jnp.float32), (1, 1), "SAME", dimension_numbers=("NCHW", "OIHW", "NCHW"), precision=lax.Precision.HIGHEST)


def pooled(inputs):
    return lax.reduce_window(inputs, -jnp.inf, lax.max, (1, 1, 3, 3), (1, 1, 2, 2), "SAME")


def encode(images, conv_first, conv_second, conv_third, res_first, res_second, projection):
    section_one = rounded(jax.nn.relu(pooled(conv_same(images.astype(jnp.float32), conv_first))))
    section_two = rounded(jax.nn.relu(pooled(conv_same(section_one, conv_second))))
    section_three = rounded(pooled(conv_same(section_two, conv_third)))
    residual_in = rounded(jax.nn.relu(conv_same(jax.nn.relu(section_three), res_first)))
    encoded_map = rounded(jax.nn.relu(section_three + conv_same(residual_in, res_second)))
    flattened = encoded_map.reshape(encoded_map.shape[0], -1)
    product = lax.dot_general(projection.astype(jnp.float32), flattened, (((1,), (1,)), ((), ())), precision=lax.Precision.HIGHEST)
    return rounded(jax.nn.relu(product))


def reference(frames, counts, slot_ids, reset_flags, hidden_state, cell_state, conv_first, conv_second, conv_third, res_first, res_second, projection, input_weight, recur_weight, gate_bias, head_weight):
    hidden_width = hidden_state.shape[0]
    slot_count = hidden_state.shape[1] // N_DP
    starts = jnp.cumsum(counts, axis=1, dtype=jnp.int32) - counts
    range_ends = starts + counts
    tensor_rows = jnp.arange(N_TENSOR, dtype=jnp.int32)
    positions = jnp.arange(ROWS_DEV, dtype=jnp.int32)
    input_rows = input_weight.astype(jnp.float32).reshape(4 * hidden_width, -1)
    recur_rows = recur_weight.astype(jnp.float32).reshape(4 * hidden_width, hidden_width)
    head_rows = head_weight.astype(jnp.float32)
    gate_offset = gate_bias.reshape(4 * hidden_width, 1)

    def one_group(dp_index):
        balanced_ranks = positions[None, :] * N_DP + dp_index
        source = jnp.sum((range_ends[:, :, None] <= balanced_ranks[:, None, :]).astype(jnp.int32), axis=1)
        offset = balanced_ranks - jnp.take_along_axis(starts, source, axis=1)
        arrival = ((source * N_TENSOR + tensor_rows[:, None]) * CAP + offset).reshape(-1).astype(jnp.int32)
        images = jnp.take(frames, arrival, axis=0)
        features = encode(images, conv_first, conv_second, conv_third, res_first, res_second, projection)
        chosen = lax.dynamic_index_in_dim(slot_ids, dp_index, 0, keepdims=False)
        flags = lax.dynamic_index_in_dim(reset_flags, dp_index, 0, keepdims=False)
        keep_state = (1 - jnp.take(flags, chosen)).astype(jnp.float32)
        hidden_group = lax.dynamic_slice_in_dim(hidden_state, dp_index * slot_count, slot_count, 1)
        cell_group = lax.dynamic_slice_in_dim(cell_state, dp_index * slot_count, slot_count, 1)
        prev_hidden = jnp.take(hidden_group, chosen, axis=1) * keep_state[None, :]
        prev_cell = jnp.take(cell_group, chosen, axis=1) * keep_state[None, :]
        gate_sums = jnp.dot(input_rows, features, precision=lax.Precision.HIGHEST)
        gate_sums = gate_sums + jnp.dot(recur_rows, rounded(prev_hidden), precision=lax.Precision.HIGHEST)
        gate_sums = (gate_sums + gate_offset).reshape(4, hidden_width, -1)
        next_cell = jax.nn.sigmoid(gate_sums[1]) * prev_cell + jax.nn.sigmoid(gate_sums[0]) * jnp.tanh(gate_sums[2])
        next_hidden = jax.nn.sigmoid(gate_sums[3]) * jnp.tanh(next_cell)
        head_values = jnp.dot(head_rows, rounded(next_hidden), precision=lax.Precision.HIGHEST)
        return head_values, hidden_group.at[:, chosen].set(next_hidden), cell_group.at[:, chosen].set(next_cell), arrival

    head_values, hidden_groups, cell_groups, arrivals = lax.map(one_group, jnp.arange(N_DP, dtype=jnp.int32))
    outputs_wide = head_values.shape[1]
    policy_out = jnp.zeros((outputs_wide, frames.shape[0]), jnp.float32)
    policy_out = policy_out.at[:, arrivals.reshape(-1)].set(jnp.moveaxis(head_values, 0, 1).reshape(outputs_wide, -1))
    hidden_after = jnp.moveaxis(hidden_groups, 0, 1).reshape(hidden_width, -1)
    cell_after = jnp.moveaxis(cell_groups, 0, 1).reshape(hidden_width, -1)
    return policy_out, hidden_after, cell_after
```

```python
import functools

import jax
import jax.numpy as jnp
import numpy as np
from jax import lax
from jax.experimental import pallas as pl
from jax.experimental.pallas import tpu as pltpu
from jax.sharding import PartitionSpec as P

F32, BF16, I32 = jnp.float32, jnp.bfloat16, jnp.int32
LANES = 128
PACK = 16
Y1, Y2, P3, Y4 = 12, 6, 2, 4
NN = (((1,), (0,)), ((), ()))
NT = (((1,), (1,)), ((), ()))
TN = (((0,), (0,)), ((), ()))
VMEM = pl.BlockSpec(memory_space=pltpu.VMEM)
SMEM = pl.BlockSpec(memory_space=pltpu.SMEM)


def mm(a, b, dims=NN, precision=None):
    return lax.dot_general(a, b, dims, precision=precision, preferred_element_type=F32)


def iota(shape, axis):
    return lax.broadcasted_iota(I32, shape, axis)


def log2(n):
    assert n & (n - 1) == 0
    return n.bit_length() - 1


def one_hot(mask):
    return jnp.where(mask, 1.0, 0.0).astype(BF16)


class Sizes:
    def __init__(self, frames, first, second, projection):
        self.cap, self.c0, self.f, _ = frames
        self.c1, self.c2, self.feat = first[0], second[0], projection[0]
        self.w1 = -(-self.f // 2)
        self.w2 = -(-self.w1 // 2)
        self.w3 = -(-self.w2 // 2)
        self.n1 = LANES // self.w1
        self.n2 = 2 * self.n1
        assert self.f % 4 == 0 and self.w2 % 2 == 1 and self.n2 * self.w2 <= LANES
        assert self.f % Y1 == 0 and Y1 % 2 == 0 and self.w1 % Y2 == 0 and Y2 % 2 == 0
        self.pad1 = PACK // self.c0
        self.win1 = Y1 + 2 * self.pad1
        self.win2 = Y2 + 3
        self.win3 = 2 * P3 + 3
        self.win4 = Y4 + 2
        self.subs = -(-self.cap // self.n1)
        self.groups = -(-self.cap // self.n2)
        self.blocks3 = -(-self.w3 // P3)
        self.blocks4 = -(-self.w3 // Y4)
        self.wide = -(-self.w3 * self.cap // LANES) * LANES
        assert self.wide - self.w3 * self.cap >= self.cap

    def tables(self):
        rows = []
        four = np.arange(4 * LANES)
        quarter, lane = four // LANES, four % LANES

        def source(width, half, where, count):
            image, j = lane // half, lane % half
            x = 2 * j + quarter - 1
            live = (image < count) & (x >= 0) & (x < width)
            return np.where(live, where(image) + x, -1)

        for i in range(self.n1):
            own = source(self.f, self.w1, lambda image: 0 * image, self.n1)
            rows.append(np.where(lane // self.w1 == i, own, -1))
        rows.append(
            source(
                self.w1,
                self.w2,
                lambda image: image // self.n1 * LANES + image % self.n1 * self.w1,
                self.n2,
            )
        )
        rows.append(source(self.w2, self.w3, lambda image: image * self.w2, self.n2))
        final = np.arange(self.wide)
        x, image = final // self.cap, final % self.cap
        rows.append(np.where(x < self.w3, image * self.w3 + x, -(1 << 20)))
        k1, k2 = np.arange(3 * self.win1 * self.c0), np.arange(3 * self.win2 * self.c1)
        k3, k4 = np.arange(self.win3 * self.c2), np.arange(self.win4 * self.c2)
        for k, window, c in ((k1, self.win1, self.c0), (k2, self.win2, self.c1)):
            rows += [k // (window * c), k % (window * c) // c, k % c]
        for k, c in ((k3, self.c2), (k4, self.c2)):
            rows += [k // c, k % c]
        n = self.c2 * self.w3
        k = np.arange(n)
        rows.append(k % self.w3 * self.c2 + k // self.w3)
        k = np.arange(PACK * self.w3)
        rows += [k % self.w3, k // self.w3]
        width = max(len(r) for r in rows)
        table = np.full((-(-len(rows) // 8) * 8, width), -(1 << 20), np.int32)
        for i, r in enumerate(rows):
            table[i, : len(r)] = r
        return table, [len(r) for r in rows]


def encoder_kernel(
    z, lengths, dp, tensor, dp_index, tensor_index,
    counts, frames, w1, w2, w3, r1, r2, proj, table, out,
    p1, p2, p3, t1, t2, t3, t4, t5, g1, s1, g2, s2, g3, s3, total, x4, x5, projx,
):
    def row(i):
        return table[i : i + 1, : lengths[i]]

    def pick(rows, i):
        return one_hot(iota((rows, lengths[i]), 0) == row(i))

    for i in range(z.n1):
        p1[i] = pick(z.f, i)
    p2[...] = pick(2 * LANES, z.n1)
    p3[...] = pick(LANES, z.n1 + 1)
    base = z.n1 + 3

    def banded(m, cout, band, kx):
        a = one_hot((iota((m, cout), 0) & (cout - 1)) == iota((m, cout), 1))
        gap = band - (iota((m, kx), 0) >> log2(cout))
        return a, gap

    def band_all(weights, m, cin, cout, index, first):
        kx = lengths[index]
        a, gap = banded(m, cout, row(index + 1), kx)
        acc = jnp.zeros((m, kx), F32)
        for dy in range(3):
            part = jnp.zeros((m, kx), F32)
            for dx in range(3):
                mixed = mm(a, weights[dy, dx], NT).astype(BF16)
                spread = one_hot(
                    (iota((cin, kx), 0) == row(index + 2)) & (row(index) == dx)
                )
                part = part + mm(mixed, spread)
            acc = jnp.where(gap == first + dy, part, acc)
        return acc.astype(BF16)

    def band_each(weights, m, cin, cout, index, target):
        kx = lengths[index]
        a, gap = banded(m, cout, row(index), kx)
        spread = one_hot(iota((cin, kx), 0) == row(index + 1))
        for dx in range(3):
            acc = jnp.zeros((m, kx), F32)
            for dy in range(3):
                mixed = mm(a, weights[dy, dx]).astype(BF16)
                acc = jnp.where(gap == dy, mm(mixed, spread), acc)
            target[dx] = acc.astype(BF16)

    t1[...] = band_all(w1, (Y1 + 1) * z.c1, z.c0, z.c1, base, z.pad1 - 1)
    t2[...] = band_all(w2, (Y2 + 1) * z.c2, z.c1, z.c2, base + 3, 0)
    band_each(w3, (2 * P3 + 1) * z.c2, z.c2, z.c2, base + 6, t3)
    band_each(r1, Y4 * z.c2, z.c2, z.c2, base + 8, t4)
    band_each(r2, Y4 * z.c2, z.c2, z.c2, base + 8, t5)

    for ref, top, rows in ((g1, PACK, z.f * z.c0), (g2, z.c1, z.w1 * z.c1), (g3, 2 * z.c2, z.w2 * z.c2)):
        for q in range(4):
            ref[q, :top] = jnp.zeros((top, LANES), BF16)
            low = ref.shape[1] - top - rows
            ref[q, top + rows :] = jnp.zeros((low, LANES), BF16)
    for ref in (x4, x5):
        for q in range(3):
            ref[q, : z.c2] = jnp.zeros((z.c2, z.wide), BF16)
            low = ref.shape[1] - z.c2 - z.w3 * z.c2
            ref[q, z.c2 + z.w3 * z.c2 :] = jnp.zeros((low, z.wide), BF16)
    total[...] = jnp.zeros(total.shape, F32)

    own = counts[tensor_index(), dp_index()]
    subs = lax.div(own + (z.n1 - 1), z.n1)
    groups = lax.div(own + (z.n2 - 1), z.n2)
    s1[subs] = jnp.zeros(s1.shape[1:], BF16)

    def sides(ref, dx, low, rows):
        return jnp.concatenate(
            [ref[dx, low : low + rows, :], ref[dx + 1, low : low + rows, :]], axis=1
        )

    def lane_is(rows, half, count, j):
        lane = iota((rows, LANES), 1)
        mask = lane == j
        for i in range(1, count):
            mask = mask | (lane == i * half + j)
        return mask

    def pool_low(acc, half, count):
        even, odd = acc[:, :LANES], acc[:, LANES:]
        nxt = pltpu.roll(even, LANES - 1, 1)
        nxt = jnp.where(lane_is(even.shape[0], half, count, half - 1), even, nxt)
        return jnp.maximum(jnp.maximum(even, odd), nxt)

    def pool_rows(m, c, pairs, last):
        done = []
        for i in range(pairs):
            top = jnp.maximum(m[2 * i * c : (2 * i + 1) * c], m[(2 * i + 1) * c : (2 * i + 2) * c])
            if not (last and i == pairs - 1):
                top = jnp.maximum(top, m[(2 * i + 2) * c : (2 * i + 3) * c])
            done.append(top)
        return jnp.concatenate(done, axis=0)

    def conv_one(s, _):
        mixed = None
        for i in range(z.n1):
            image = frames[jnp.minimum(s * z.n1 + i, z.cap - 1)]
            part = mm(image, p1[i])
            mixed = part if mixed is None else mixed + part
        mixed = mixed.astype(BF16)
        for q in range(4):
            g1[q, PACK : PACK + z.f * z.c0, :] = mixed[:, q * LANES : (q + 1) * LANES]
        for b in range(z.f // Y1):
            low = b * Y1 * z.c0
            around = jnp.concatenate([sides(g1, dx, low, z.win1 * z.c0) for dx in range(3)], axis=0)
            m = pool_low(mm(t1[...], around), z.w1, z.n1)
            rows = pool_rows(m, z.c1, Y1 // 2, b == z.f // Y1 - 1)
            size = Y1 // 2 * z.c1
            s1[s, b * size : (b + 1) * size, :] = jnp.maximum(rows, 0.0).astype(BF16)
        return 0

    lax.fori_loop(0, subs, conv_one, 0)

    def conv_rest(g, _):
        both = jnp.concatenate([s1[2 * g], s1[2 * g + 1]], axis=1)
        mixed = mm(both, p2[...]).astype(BF16)
        for q in range(4):
            g2[q, z.c1 : z.c1 + z.w1 * z.c1, :] = mixed[:, q * LANES : (q + 1) * LANES]
        for b in range(z.w1 // Y2):
            low = b * Y2 * z.c1
            around = jnp.concatenate([sides(g2, dx, low, z.win2 * z.c1) for dx in range(3)], axis=0)
            m = pool_low(mm(t2[...], around), z.w2, z.n2)
            rows = pool_rows(m, z.c2, Y2 // 2, b == z.w1 // Y2 - 1)
            size = Y2 // 2 * z.c2
            s2[b * size : (b + 1) * size, :] = jnp.maximum(rows, 0.0).astype(BF16)
        mixed = mm(s2[...], p3[...]).astype(BF16)
        for q in range(4):
            g3[q, 2 * z.c2 : 2 * z.c2 + z.w2 * z.c2, :] = mixed[:, q * LANES : (q + 1) * LANES]
        c = z.c2
        for b in range(z.blocks3):
            low = b * 2 * P3 * c
            acc = None
            for dx in range(3):
                part = mm(t3[dx], sides(g3, dx, low, z.win3 * c))
                acc = part if acc is None else acc + part
            even, odd = acc[:, :LANES], acc[:, LANES:]
            n = even.shape[0]
            before = jnp.where(lane_is(n, z.w3, z.n2, 0), even, pltpu.roll(odd, 1, 1))
            odd = jnp.where(lane_is(n, z.w3, z.n2, z.w3 - 1), even, odd)
            m = jnp.maximum(jnp.maximum(even, odd), before)
            for i in range(P3):
                pooled = b * P3 + i
                if pooled >= z.w3:
                    continue
                rows = [2 * i + d for d in range(3) if 0 <= 2 * pooled - 1 + d < z.w2]
                top = None
                for r in rows:
                    piece = m[r * c : (r + 1) * c]
                    top = piece if top is None else jnp.maximum(top, piece)
                s3[pooled * c : (pooled + 1) * c, :] = top.astype(BF16)
        shape = (LANES, z.wide)
        line = iota(shape, 0)
        place = one_hot((line == row(z.n1 + 2) - g * (z.n2 * z.w3)) & (line < z.n2 * z.w3))
        total[...] += mm(s3[...], place)
        return 0

    lax.fori_loop(0, groups, conv_rest, 0)

    c, n = z.c2, z.w3 * z.c2
    live = iota((n, z.wide), 1) < z.w3 * z.cap

    def spread_x(ref, value):
        ref[0, c : c + n, :] = pltpu.roll(value, z.cap, 1).astype(BF16)
        ref[1, c : c + n, :] = value.astype(BF16)
        ref[2, c : c + n, :] = pltpu.roll(value, z.wide - z.cap, 1).astype(BF16)

    def residual(ref, kernel, add):
        pieces = []
        for b in range(z.blocks4):
            low = b * Y4 * c
            acc = None
            for dx in range(3):
                part = mm(kernel[dx], ref[dx, low : low + z.win4 * c, :])
                acc = part if acc is None else acc + part
            pieces.append(acc[: min(Y4, z.w3 - b * Y4) * c])
        value = jnp.concatenate(pieces, axis=0)
        if add is not None:
            value = value + add
        return jnp.maximum(value, 0.0)

    spread_x(x4, jnp.maximum(total[...], 0.0))
    inner = residual(x4, t4, None).astype(BF16).astype(F32)
    spread_x(x5, jnp.where(live, inner, 0.0))
    encoded = residual(x5, t5, total[...]).astype(BF16)

    last = len(lengths) - 3
    order = one_hot(iota((n, n), 0) == row(last))
    turned = jnp.swapaxes(encoded, 0, 1)
    turned = mm(turned, order).astype(BF16)
    block = PACK * z.w3
    wanted = iota((block, block), 0)
    regroup = one_hot(((wanted >> log2(PACK)) == row(last + 1)) & ((wanted & (PACK - 1)) == row(last + 2)))
    for b in range(n // PACK):
        moved = mm(regroup, proj[b * block : (b + 1) * block, :]).astype(BF16)
        for x in range(z.w3):
            projx[x, b * PACK : (b + 1) * PACK, :] = moved[x * PACK : (x + 1) * PACK]
    acc = None
    for x in range(z.w3):
        part = mm(turned[x * z.cap : (x + 1) * z.cap], projx[x])
        acc = part if acc is None else acc + part
    features = jnp.maximum(acc, 0.0).astype(BF16)

    start = jnp.int32(0)
    for a in range(dp):
        start = start + jnp.where(a < dp_index(), counts[tensor_index(), a], 0)
    depth = z.cap // dp
    shape = (dp * tensor * depth, z.cap)
    r = iota(shape, 0)
    receiver, level = r >> log2(tensor * depth), r & (depth - 1)
    arrival = ((receiver - start) & (dp - 1)) + level * dp
    route = one_hot((iota(shape, 1) == arrival) & (arrival < own))
    out[...] = mm(route, features).astype(BF16)


def encode_rows(frames, counts, kernels, projection):
    first, second, third, res_first, res_second = kernels
    z = Sizes(frames.shape, first.shape, second.shape, projection.shape)
    table, lengths = z.tables()
    dp, tensor = lax.axis_size("dp"), lax.axis_size("tensor")
    images = jnp.transpose(frames, (0, 2, 1, 3)).reshape(z.cap, z.f * z.c0, z.f)
    ci_co, co_ci = (2, 3, 1, 0), (2, 3, 0, 1)
    n = z.w3 * z.c2
    scratch = [
        pltpu.VMEM((z.n1, z.f, 4 * LANES), BF16),
        pltpu.VMEM((2 * LANES, 4 * LANES), BF16),
        pltpu.VMEM((LANES, 4 * LANES), BF16),
        pltpu.VMEM(((Y1 + 1) * z.c1, 3 * z.win1 * z.c0), BF16),
        pltpu.VMEM(((Y2 + 1) * z.c2, 3 * z.win2 * z.c1), BF16),
        pltpu.VMEM((3, (2 * P3 + 1) * z.c2, z.win3 * z.c2), BF16),
        pltpu.VMEM((3, Y4 * z.c2, z.win4 * z.c2), BF16),
        pltpu.VMEM((3, Y4 * z.c2, z.win4 * z.c2), BF16),
        pltpu.VMEM((4, z.f * z.c0 + 2 * PACK, LANES), BF16),
        pltpu.VMEM((2 * z.groups + 1, z.w1 * z.c1, LANES), BF16),
        pltpu.VMEM((4, (z.w1 - Y2 + z.win2) * z.c1, LANES), BF16),
        pltpu.VMEM((z.w2 * z.c2, LANES), BF16),
        pltpu.VMEM((4, ((z.blocks3 - 1) * 2 * P3 + z.win3) * z.c2, LANES), BF16),
        pltpu.VMEM((n, LANES), BF16),
        pltpu.VMEM((n, z.wide), F32),
        pltpu.VMEM((3, ((z.blocks4 - 1) * Y4 + z.win4) * z.c2, z.wide), BF16),
        pltpu.VMEM((3, ((z.blocks4 - 1) * Y4 + z.win4) * z.c2, z.wide), BF16),
        pltpu.VMEM((z.w3, n, z.feat), BF16),
    ]
    body = functools.partial(
        encoder_kernel, z, lengths, dp, tensor,
        lambda: lax.axis_index("dp"), lambda: lax.axis_index("tensor"),
    )
    depth = z.cap // dp
    return pl.pallas_call(
        body,
        name="encoder",
        out_shape=jax.ShapeDtypeStruct((dp * tensor * depth, z.feat), BF16),
        in_specs=[SMEM] + [VMEM] * 8,
        out_specs=VMEM,
        scratch_shapes=scratch,
        compiler_params=pltpu.CompilerParams(vmem_limit_bytes=40 << 20),
        cost_estimate=pl.CostEstimate(flops=20_000_000_000, bytes_accessed=8_000_000, transcendentals=0),
    )(
        counts,
        images,
        jnp.transpose(first, ci_co),
        jnp.transpose(second, ci_co),
        jnp.transpose(third, co_ci),
        jnp.transpose(res_first, co_ci),
        jnp.transpose(res_second, co_ci),
        jnp.transpose(projection),
        jnp.asarray(table),
    )


def recurrent_kernel(index, weight, bias, *refs):
    *pieces, out, held, sems = refs
    gates, share, _ = weight.shape
    width = pieces[0].shape[0]
    copies = [pltpu.make_async_copy(weight.at[q], held.at[q], sems.at[q]) for q in range(gates)]
    for copy in copies:
        copy.start()
    tensor = len(pieces)
    for q in range(gates):
        copies[q].wait()
        column = jnp.broadcast_to(bias[q : q + 1, :], (out.shape[1], share))
        acc = None
        for back, piece in enumerate(pieces):
            low = pl.multiple_of(((index() - back) & (tensor - 1)) * width, width)
            part = mm(held[q, :, pl.ds(low, width)], piece[...])
            acc = part if acc is None else acc + part
        out[q * share : (q + 1) * share, :] = acc + jnp.transpose(column)


def recurrent(weight, bias, pieces):
    gates, share, hidden = weight.shape
    slots = pieces[0].shape[1]
    return pl.pallas_call(
        functools.partial(recurrent_kernel, lambda: lax.axis_index("tensor")),
        name="recurrent",
        out_shape=jax.ShapeDtypeStruct((gates * share, slots), F32),
        in_specs=[pl.BlockSpec(memory_space=pl.ANY)] + [VMEM] * (1 + len(pieces)),
        out_specs=VMEM,
        scratch_shapes=[
            pltpu.VMEM(weight.shape, BF16),
            pltpu.SemaphoreType.DMA((gates,)),
        ],
        compiler_params=pltpu.CompilerParams(vmem_limit_bytes=24 << 20),
        cost_estimate=pl.CostEstimate(
            flops=2 * gates * share * hidden * slots, bytes_accessed=2 * gates * share * hidden, transcendentals=0
        ),
    )(weight, bias, *pieces)


def core_kernel(dp_index, features, sums, weight, hidden, cell, heads, slots, counts, resets, sent, hidden_out, cell_out):
    tensor, dp = counts.shape
    rows, count = features.shape[0], slots.shape[1]
    depth = rows // (dp * tensor)
    share, places = hidden.shape
    mine = dp_index()
    exact = lax.Precision.HIGHEST
    tallies = counts[...].astype(F32)
    before = jnp.where(iota((dp, dp), 0) < iota((dp, dp), 1), 1.0, 0.0)
    starts = mm(tallies, before, precision=exact)
    line = iota((rows, 1), 0)
    sender, group, level = line >> log2(tensor * depth), (line >> log2(depth)) & (tensor - 1), line & (depth - 1)
    by_group = jnp.where(iota((rows, tensor), 1) == group, 1.0, 0.0)
    own = iota((rows, dp), 1) == sender

    def of_row(table):
        wide = mm(by_group, table, precision=exact)
        return jnp.sum(jnp.where(own, wide, 0.0), axis=1, keepdims=True).astype(I32)

    start = of_row(starts)
    end = of_row(starts + tallies)
    rank = start + ((mine - start) & (dp - 1)) + level * dp
    balanced = group * (count // tensor) + ((rank - mine) >> log2(dp))
    to_row = one_hot((iota((rows, count), 1) == balanced) & (rank < end))
    of_slot = one_hot(iota((places, count), 0) == slots[...])
    chosen = mm(to_row, of_slot, NT)
    taken = jnp.sum(chosen, axis=0, keepdims=True) > 0.5
    inputs = mm(features[...], chosen.astype(BF16), TN).astype(BF16)
    keep = 1.0 - resets[...].astype(F32)
    old_cell = cell[...]

    def gate(q):
        low = q * share
        return mm(weight[q], inputs) + sums[low : low + share, :]

    next_cell = jax.nn.sigmoid(gate(1)) * (old_cell * keep) + jax.nn.sigmoid(gate(0)) * jnp.tanh(gate(2))
    next_hidden = jax.nn.sigmoid(gate(3)) * jnp.tanh(next_cell)
    values = mm(heads[...], next_hidden.astype(BF16))
    sent[...] = mm(chosen, values, NT, precision=exact)
    cell_out[...] = jnp.where(taken, next_cell, old_cell)
    hidden_out[...] = jnp.where(taken, next_hidden, hidden[...])


def core(features, sums, weight, hidden, cell, heads, slots, counts, resets):
    share = hidden.shape[0]
    return pl.pallas_call(
        functools.partial(core_kernel, lambda: lax.axis_index("dp")),
        name="core",
        out_shape=(
            jax.ShapeDtypeStruct((features.shape[0], heads.shape[0]), F32),
            jax.ShapeDtypeStruct(hidden.shape, F32),
            jax.ShapeDtypeStruct(cell.shape, F32),
        ),
        in_specs=[VMEM] * 9,
        out_specs=(VMEM,) * 3,
        compiler_params=pltpu.CompilerParams(vmem_limit_bytes=24 << 20),
        cost_estimate=pl.CostEstimate(
            flops=8 * share * weight.shape[2] * hidden.shape[1], bytes_accessed=4_000_000, transcendentals=0
        ),
    )(features, sums, weight, hidden, cell, heads, slots, counts, resets)


def answers_kernel(tensor, dp_index, tensor_index, counts, received, out):
    dp = counts.shape[1]
    rows, cap = received.shape[0], out.shape[1]
    depth = cap // dp
    start = jnp.int32(0)
    for a in range(dp):
        start = start + jnp.where(a < dp_index(), counts[tensor_index(), a], 0)
    own = counts[tensor_index(), dp_index()]
    line = iota((rows, cap), 0)
    giver, level = line >> log2(tensor * depth), line & (depth - 1)
    arrival = ((giver - start) & (dp - 1)) + level * dp
    place = jnp.where((iota((rows, cap), 1) == arrival) & (arrival < own), 1.0, 0.0)
    out[...] = mm(received[...], place, TN, precision=lax.Precision.HIGHEST)


def answers(counts, received, cap):
    return pl.pallas_call(
        functools.partial(
            answers_kernel,
            counts.shape[0],
            lambda: lax.axis_index("dp"),
            lambda: lax.axis_index("tensor"),
        ),
        name="answers",
        out_shape=jax.ShapeDtypeStruct((received.shape[1], cap), F32),
        in_specs=[SMEM, VMEM],
        out_specs=VMEM,
    )(counts, received)


def body(
    frames, counts, slot_ids, reset_flags, hidden_state, cell_state,
    conv_first, conv_second, conv_third, res_first, res_second,
    projection, input_weight, recur_weight, gate_bias, head_weight,
):
    tensor = lax.axis_size("tensor")
    own = (hidden_state * (1 - reset_flags).astype(F32)).astype(BF16)
    pieces = [own] + [
        lax.ppermute(own, "tensor", [(i, (i + back) % tensor) for i in range(tensor)])
        for back in range(1, tensor)
    ]
    kernels = (conv_first, conv_second, conv_third, res_first, res_second)
    features = encode_rows(frames, counts, kernels, projection)
    features = lax.all_to_all(features, ("dp", "tensor"), 0, 0, tiled=True)
    sums = recurrent(recur_weight, gate_bias, pieces)
    sent, hidden_after, cell_after = core(
        features, sums, input_weight, hidden_state, cell_state, head_weight, slot_ids, counts, reset_flags
    )
    received = lax.all_to_all(sent, ("dp", "tensor"), 0, 0, tiled=True)
    return answers(counts, received, frames.shape[0]), hidden_after, cell_after


def solution(mesh):
    return jax.shard_map(
        body,
        mesh=mesh,
        in_specs=(
            P(("dp", "tensor"), None, None, None),
            P(),
            P("dp", None),
            P("dp", None),
            P("tensor", "dp"),
            P("tensor", "dp"),
            P(),
            P(),
            P(),
            P(),
            P(),
            P(),
            P(None, "tensor", None),
            P(None, "tensor", None),
            P(None, "tensor"),
            P(None, "tensor"),
        ),
        out_specs=(P(None, ("dp", "tensor")), P("tensor", "dp"), P("tensor", "dp")),
        check_vma=False,
    )
```

```python
import functools

import jax
import jax.numpy as jnp
import numpy as np
from jax import lax
from jax.experimental import pallas as pl
from jax.experimental.pallas import tpu as pltpu
from jax.sharding import PartitionSpec as P

F32, BF16, I32 = jnp.float32, jnp.bfloat16, jnp.int32
LANES = 128
VMEM_MOST = 67_043_328
PACK = 16
Y1, Y2, P3, Y4 = 12, 6, 2, 4
NN = (((1,), (0,)), ((), ()))
NT = (((1,), (1,)), ((), ()))
TN = (((0,), (0,)), ((), ()))
VMEM = pl.BlockSpec(memory_space=pltpu.VMEM)
SMEM = pl.BlockSpec(memory_space=pltpu.SMEM)
HBM = pl.BlockSpec(memory_space=pltpu.HBM)


def mm(a, b, dims=NN, precision=None):
    return lax.dot_general(a, b, dims, precision=precision, preferred_element_type=F32)


def iota(shape, axis):
    return lax.broadcasted_iota(I32, shape, axis)


def log2(n):
    assert n & (n - 1) == 0
    return n.bit_length() - 1


def one_hot(mask):
    return jnp.where(mask, 1.0, 0.0).astype(BF16)


class Sizes:
    def __init__(self, frames, first, second, projection):
        self.cap, self.c0, self.f, _ = frames
        self.c1, self.c2, self.feat = first[0], second[0], projection[0]
        self.w1 = -(-self.f // 2)
        self.w2 = -(-self.w1 // 2)
        self.w3 = -(-self.w2 // 2)
        self.n1 = LANES // self.w1
        self.n2 = 2 * self.n1
        assert self.f % 4 == 0 and self.w2 % 2 == 1 and self.n2 * self.w2 <= LANES
        assert self.f % Y1 == 0 and Y1 % 2 == 0 and self.w1 % Y2 == 0 and Y2 % 2 == 0
        self.pad1 = PACK // self.c0
        self.win1 = Y1 + 2 * self.pad1
        self.win2 = Y2 + 3
        self.win3 = 2 * P3 + 3
        self.win4 = Y4 + 2
        self.subs = -(-self.cap // self.n1)
        self.groups = -(-self.cap // self.n2)
        self.blocks3 = -(-self.w3 // P3)
        self.blocks4 = -(-self.w3 // Y4)
        self.wide = -(-self.w3 * self.cap // LANES) * LANES
        assert self.wide - self.w3 * self.cap >= self.cap

    def tables(self):
        rows = []
        four = np.arange(4 * LANES)
        quarter, lane = four // LANES, four % LANES

        def source(width, half, where, count):
            image, j = lane // half, lane % half
            x = 2 * j + quarter - 1
            live = (image < count) & (x >= 0) & (x < width)
            return np.where(live, where(image) + x, -1)

        for i in range(self.n1):
            own = source(self.f, self.w1, lambda image: 0 * image, self.n1)
            rows.append(np.where(lane // self.w1 == i, own, -1))
        rows.append(
            source(
                self.w1,
                self.w2,
                lambda image: image // self.n1 * LANES + image % self.n1 * self.w1,
                self.n2,
            )
        )
        rows.append(source(self.w2, self.w3, lambda image: image * self.w2, self.n2))
        final = np.arange(self.wide)
        x, image = final // self.cap, final % self.cap
        rows.append(np.where(x < self.w3, image * self.w3 + x, -(1 << 20)))
        k1, k2 = np.arange(3 * self.win1 * self.c0), np.arange(3 * self.win2 * self.c1)
        k3, k4 = np.arange(self.win3 * self.c2), np.arange(self.win4 * self.c2)
        for k, window, c in ((k1, self.win1, self.c0), (k2, self.win2, self.c1)):
            rows += [k // (window * c), k % (window * c) // c, k % c]
        for k, c in ((k3, self.c2), (k4, self.c2)):
            rows += [k // c, k % c]
        n = self.c2 * self.w3
        k = np.arange(n)
        rows.append(k % self.w3 * self.c2 + k // self.w3)
        k = np.arange(PACK * self.w3)
        rows += [k % self.w3, k // self.w3]
        width = max(len(r) for r in rows)
        table = np.full((-(-len(rows) // 8) * 8, width), -(1 << 20), np.int32)
        for i, r in enumerate(rows):
            table[i, : len(r)] = r
        return table, [len(r) for r in rows]


def encoder_kernel(
    z, lengths, dp, tensor, dp_index, tensor_index,
    *refs,
):
    far, out, near = refs[:9], refs[9], refs[10:19]
    p1, p2, p3, t1, t2, t3, t4, t5, g1, s1, g2, s2, g3, s3, total, x4, x5, projx, sems = refs[19:]
    counts, table, w1, w2, w3, r1, r2, frames, proj = near
    copies = [pltpu.make_async_copy(a, b, sems.at[i]) for i, (a, b) in enumerate(zip(far, near))]
    for copy in copies:
        copy.start()

    def row(i):
        return table[i : i + 1, : lengths[i]]

    def pick(rows, i):
        return one_hot(iota((rows, lengths[i]), 0) == row(i))

    def zero_padding():
        for ref, top, rows in ((g1, PACK, z.f * z.c0), (g2, z.c1, z.w1 * z.c1), (g3, 2 * z.c2, z.w2 * z.c2)):
            for q in range(4):
                ref[q, :top] = jnp.zeros((top, LANES), BF16)
                low = ref.shape[1] - top - rows
                ref[q, top + rows :] = jnp.zeros((low, LANES), BF16)
        for ref in (x4, x5):
            for q in range(3):
                ref[q, : z.c2] = jnp.zeros((z.c2, z.wide), BF16)
                low = ref.shape[1] - z.c2 - z.w3 * z.c2
                ref[q, z.c2 + z.w3 * z.c2 :] = jnp.zeros((low, z.wide), BF16)
        total[...] = jnp.zeros(total.shape, F32)

    zero_padding()
    for copy in copies[:7]:
        copy.wait()

    for i in range(z.n1):
        p1[i] = pick(z.f, i)
    p2[...] = pick(2 * LANES, z.n1)
    p3[...] = pick(LANES, z.n1 + 1)
    base = z.n1 + 3

    def banded(m, cout, band, kx):
        a = one_hot((iota((m, cout), 0) & (cout - 1)) == iota((m, cout), 1))
        gap = band - (iota((m, kx), 0) >> log2(cout))
        return a, gap

    def band_all(weights, m, cin, cout, index, first):
        kx = lengths[index]
        a, gap = banded(m, cout, row(index + 1), kx)
        acc = jnp.zeros((m, kx), F32)
        for dy in range(3):
            part = jnp.zeros((m, kx), F32)
            for dx in range(3):
                mixed = mm(a, weights[dy, dx], NT).astype(BF16)
                spread = one_hot(
                    (iota((cin, kx), 0) == row(index + 2)) & (row(index) == dx)
                )
                part = part + mm(mixed, spread)
            acc = jnp.where(gap == first + dy, part, acc)
        return acc.astype(BF16)

    def band_each(weights, m, cin, cout, index, target):
        kx = lengths[index]
        a, gap = banded(m, cout, row(index), kx)
        spread = one_hot(iota((cin, kx), 0) == row(index + 1))
        for dx in range(3):
            acc = jnp.zeros((m, kx), F32)
            for dy in range(3):
                mixed = mm(a, weights[dy, dx]).astype(BF16)
                acc = jnp.where(gap == dy, mm(mixed, spread), acc)
            target[dx] = acc.astype(BF16)

    t1[...] = band_all(w1, (Y1 + 1) * z.c1, z.c0, z.c1, base, z.pad1 - 1)
    t2[...] = band_all(w2, (Y2 + 1) * z.c2, z.c1, z.c2, base + 3, 0)
    band_each(w3, (2 * P3 + 1) * z.c2, z.c2, z.c2, base + 6, t3)
    band_each(r1, Y4 * z.c2, z.c2, z.c2, base + 8, t4)
    band_each(r2, Y4 * z.c2, z.c2, z.c2, base + 8, t5)

    own = counts[tensor_index(), dp_index()]
    subs = lax.div(own + (z.n1 - 1), z.n1)
    groups = lax.div(own + (z.n2 - 1), z.n2)
    s1[subs] = jnp.zeros(s1.shape[1:], BF16)

    def sides(ref, dx, low, rows):
        return jnp.concatenate(
            [ref[dx, low : low + rows, :], ref[dx + 1, low : low + rows, :]], axis=1
        )

    def lane_is(rows, half, count, j):
        lane = iota((rows, LANES), 1)
        mask = lane == j
        for i in range(1, count):
            mask = mask | (lane == i * half + j)
        return mask

    def pool_low(acc, half, count):
        even, odd = acc[:, :LANES], acc[:, LANES:]
        nxt = pltpu.roll(even, LANES - 1, 1)
        nxt = jnp.where(lane_is(even.shape[0], half, count, half - 1), even, nxt)
        return jnp.maximum(jnp.maximum(even, odd), nxt)

    def pool_rows(m, c, pairs, last):
        done = []
        for i in range(pairs):
            top = jnp.maximum(m[2 * i * c : (2 * i + 1) * c], m[(2 * i + 1) * c : (2 * i + 2) * c])
            if not (last and i == pairs - 1):
                top = jnp.maximum(top, m[(2 * i + 2) * c : (2 * i + 3) * c])
            done.append(top)
        return jnp.concatenate(done, axis=0)

    def conv_one(s, _):
        mixed = None
        for i in range(z.n1):
            image = frames[jnp.minimum(s * z.n1 + i, z.cap - 1)]
            part = mm(image, p1[i])
            mixed = part if mixed is None else mixed + part
        mixed = mixed.astype(BF16)
        for q in range(4):
            g1[q, PACK : PACK + z.f * z.c0, :] = mixed[:, q * LANES : (q + 1) * LANES]
        for b in range(z.f // Y1):
            low = b * Y1 * z.c0
            around = jnp.concatenate([sides(g1, dx, low, z.win1 * z.c0) for dx in range(3)], axis=0)
            m = pool_low(mm(t1[...], around), z.w1, z.n1)
            rows = pool_rows(m, z.c1, Y1 // 2, b == z.f // Y1 - 1)
            size = Y1 // 2 * z.c1
            s1[s, b * size : (b + 1) * size, :] = jnp.maximum(rows, 0.0).astype(BF16)
        return 0

    copies[7].wait()
    lax.fori_loop(0, subs, conv_one, 0)

    def conv_rest(g, _):
        both = jnp.concatenate([s1[2 * g], s1[2 * g + 1]], axis=1)
        mixed = mm(both, p2[...]).astype(BF16)
        for q in range(4):
            g2[q, z.c1 : z.c1 + z.w1 * z.c1, :] = mixed[:, q * LANES : (q + 1) * LANES]
        for b in range(z.w1 // Y2):
            low = b * Y2 * z.c1
            around = jnp.concatenate([sides(g2, dx, low, z.win2 * z.c1) for dx in range(3)], axis=0)
            m = pool_low(mm(t2[...], around), z.w2, z.n2)
            rows = pool_rows(m, z.c2, Y2 // 2, b == z.w1 // Y2 - 1)
            size = Y2 // 2 * z.c2
            s2[b * size : (b + 1) * size, :] = jnp.maximum(rows, 0.0).astype(BF16)
        mixed = mm(s2[...], p3[...]).astype(BF16)
        for q in range(4):
            g3[q, 2 * z.c2 : 2 * z.c2 + z.w2 * z.c2, :] = mixed[:, q * LANES : (q + 1) * LANES]
        c = z.c2
        for b in range(z.blocks3):
            low = b * 2 * P3 * c
            acc = None
            for dx in range(3):
                part = mm(t3[dx], sides(g3, dx, low, z.win3 * c))
                acc = part if acc is None else acc + part
            even, odd = acc[:, :LANES], acc[:, LANES:]
            n = even.shape[0]
            before = jnp.where(lane_is(n, z.w3, z.n2, 0), even, pltpu.roll(odd, 1, 1))
            odd = jnp.where(lane_is(n, z.w3, z.n2, z.w3 - 1), even, odd)
            m = jnp.maximum(jnp.maximum(even, odd), before)
            for i in range(P3):
                pooled = b * P3 + i
                if pooled >= z.w3:
                    continue
                rows = [2 * i + d for d in range(3) if 0 <= 2 * pooled - 1 + d < z.w2]
                top = None
                for r in rows:
                    piece = m[r * c : (r + 1) * c]
                    top = piece if top is None else jnp.maximum(top, piece)
                s3[pooled * c : (pooled + 1) * c, :] = top.astype(BF16)
        shape = (LANES, z.wide)
        line = iota(shape, 0)
        place = one_hot((line == row(z.n1 + 2) - g * (z.n2 * z.w3)) & (line < z.n2 * z.w3))
        total[...] += mm(s3[...], place)
        return 0

    lax.fori_loop(0, groups, conv_rest, 0)

    c, n = z.c2, z.w3 * z.c2
    live = iota((n, z.wide), 1) < z.w3 * z.cap

    def spread_x(ref, value):
        ref[0, c : c + n, :] = pltpu.roll(value, z.cap, 1).astype(BF16)
        ref[1, c : c + n, :] = value.astype(BF16)
        ref[2, c : c + n, :] = pltpu.roll(value, z.wide - z.cap, 1).astype(BF16)

    def residual(ref, kernel, add):
        pieces = []
        for b in range(z.blocks4):
            low = b * Y4 * c
            acc = None
            for dx in range(3):
                part = mm(kernel[dx], ref[dx, low : low + z.win4 * c, :])
                acc = part if acc is None else acc + part
            pieces.append(acc[: min(Y4, z.w3 - b * Y4) * c])
        value = jnp.concatenate(pieces, axis=0)
        if add is not None:
            value = value + add
        return jnp.maximum(value, 0.0)

    spread_x(x4, jnp.maximum(total[...], 0.0))
    inner = residual(x4, t4, None).astype(BF16).astype(F32)
    spread_x(x5, jnp.where(live, inner, 0.0))
    encoded = residual(x5, t5, total[...]).astype(BF16)

    last = len(lengths) - 3
    order = one_hot(iota((n, n), 0) == row(last))
    turned = jnp.swapaxes(encoded, 0, 1)
    turned = mm(turned, order).astype(BF16)
    copies[8].wait()
    block = PACK * z.w3
    wanted = iota((block, block), 0)
    regroup = one_hot(((wanted >> log2(PACK)) == row(last + 1)) & ((wanted & (PACK - 1)) == row(last + 2)))
    for b in range(n // PACK):
        moved = mm(regroup, proj[b * block : (b + 1) * block, :]).astype(BF16)
        for x in range(z.w3):
            projx[x, b * PACK : (b + 1) * PACK, :] = moved[x * PACK : (x + 1) * PACK]
    acc = None
    for x in range(z.w3):
        part = mm(turned[x * z.cap : (x + 1) * z.cap], projx[x])
        acc = part if acc is None else acc + part
    features = jnp.maximum(acc, 0.0).astype(BF16)

    start = jnp.int32(0)
    for a in range(dp):
        start = start + jnp.where(a < dp_index(), counts[tensor_index(), a], 0)
    depth = z.cap // dp
    shape = (dp * tensor * depth, z.cap)
    r = iota(shape, 0)
    receiver, level = r >> log2(tensor * depth), r & (depth - 1)
    arrival = ((receiver - start) & (dp - 1)) + level * dp
    route = one_hot((iota(shape, 1) == arrival) & (arrival < own))
    out[...] = mm(route, features).astype(BF16)


def encode_rows(frames, counts, kernels, projection):
    first, second, third, res_first, res_second = kernels
    z = Sizes(frames.shape, first.shape, second.shape, projection.shape)
    table, lengths = z.tables()
    dp, tensor = lax.axis_size("dp"), lax.axis_size("tensor")
    images = jnp.transpose(frames, (0, 2, 1, 3)).reshape(z.cap, z.f * z.c0, z.f)
    ci_co, co_ci = (2, 3, 1, 0), (2, 3, 0, 1)
    n = z.w3 * z.c2
    operands = (
        counts,
        jnp.asarray(table),
        jnp.transpose(first, ci_co),
        jnp.transpose(second, ci_co),
        jnp.transpose(third, co_ci),
        jnp.transpose(res_first, co_ci),
        jnp.transpose(res_second, co_ci),
        images,
        jnp.transpose(projection),
    )
    scratch = [pltpu.SMEM(counts.shape, I32)]
    scratch += [pltpu.VMEM(x.shape, x.dtype) for x in operands[1:]]
    scratch += [
        pltpu.VMEM((z.n1, z.f, 4 * LANES), BF16),
        pltpu.VMEM((2 * LANES, 4 * LANES), BF16),
        pltpu.VMEM((LANES, 4 * LANES), BF16),
        pltpu.VMEM(((Y1 + 1) * z.c1, 3 * z.win1 * z.c0), BF16),
        pltpu.VMEM(((Y2 + 1) * z.c2, 3 * z.win2 * z.c1), BF16),
        pltpu.VMEM((3, (2 * P3 + 1) * z.c2, z.win3 * z.c2), BF16),
        pltpu.VMEM((3, Y4 * z.c2, z.win4 * z.c2), BF16),
        pltpu.VMEM((3, Y4 * z.c2, z.win4 * z.c2), BF16),
        pltpu.VMEM((4, z.f * z.c0 + 2 * PACK, LANES), BF16),
        pltpu.VMEM((2 * z.groups + 1, z.w1 * z.c1, LANES), BF16),
        pltpu.VMEM((4, (z.w1 - Y2 + z.win2) * z.c1, LANES), BF16),
        pltpu.VMEM((z.w2 * z.c2, LANES), BF16),
        pltpu.VMEM((4, ((z.blocks3 - 1) * 2 * P3 + z.win3) * z.c2, LANES), BF16),
        pltpu.VMEM((n, LANES), BF16),
        pltpu.VMEM((n, z.wide), F32),
        pltpu.VMEM((3, ((z.blocks4 - 1) * Y4 + z.win4) * z.c2, z.wide), BF16),
        pltpu.VMEM((3, ((z.blocks4 - 1) * Y4 + z.win4) * z.c2, z.wide), BF16),
        pltpu.VMEM((z.w3, n, z.feat), BF16),
        pltpu.SemaphoreType.DMA((len(operands),)),
    ]
    body = functools.partial(
        encoder_kernel, z, lengths, dp, tensor,
        lambda: lax.axis_index("dp"), lambda: lax.axis_index("tensor"),
    )
    depth = z.cap // dp
    return pl.pallas_call(
        body,
        name="encoder",
        out_shape=jax.ShapeDtypeStruct((dp * tensor * depth, z.feat), BF16),
        in_specs=[HBM] * len(operands),
        out_specs=VMEM,
        scratch_shapes=scratch,
        compiler_params=pltpu.CompilerParams(vmem_limit_bytes=VMEM_MOST),
        cost_estimate=pl.CostEstimate(flops=20_000_000_000, bytes_accessed=8_000_000, transcendentals=0),
    )(*operands)


def recurrent_kernel(index, weight, *refs):
    *pieces, out, held, sems = refs
    gates, share, _ = weight.shape
    width = pieces[0].shape[0]
    copies = [pltpu.make_async_copy(weight.at[q], held.at[q], sems.at[q]) for q in range(gates)]
    for copy in copies:
        copy.start()
    tensor = len(pieces)
    for q in range(gates):
        copies[q].wait()
        acc = None
        for back, piece in enumerate(pieces):
            low = pl.multiple_of(((index() - back) & (tensor - 1)) * width, width)
            part = mm(held[q, :, pl.ds(low, width)], piece[...])
            acc = part if acc is None else acc + part
        out[q * share : (q + 1) * share, :] = acc


def recurrent(weight, pieces):
    gates, share, hidden = weight.shape
    slots = pieces[0].shape[1]
    return pl.pallas_call(
        functools.partial(recurrent_kernel, lambda: lax.axis_index("tensor")),
        name="recurrent",
        out_shape=jax.ShapeDtypeStruct((gates * share, slots), F32),
        in_specs=[HBM] + [VMEM] * len(pieces),
        out_specs=VMEM,
        scratch_shapes=[
            pltpu.VMEM(weight.shape, BF16),
            pltpu.SemaphoreType.DMA((gates,)),
        ],
        compiler_params=pltpu.CompilerParams(vmem_limit_bytes=24 << 20),
        cost_estimate=pl.CostEstimate(
            flops=2 * gates * share * hidden * slots, bytes_accessed=2 * gates * share * hidden, transcendentals=0
        ),
    )(weight, *pieces)


def core_kernel(dp_index, features, sums, bias, weight, hidden, cell, heads, slots, counts, resets, sent, hidden_out, cell_out):
    tensor, dp = counts.shape
    rows, count = features.shape[0], slots.shape[1]
    depth = rows // (dp * tensor)
    share, places = hidden.shape
    mine = dp_index()
    exact = lax.Precision.HIGHEST
    tallies = counts[...].astype(F32)
    before = jnp.where(iota((dp, dp), 0) < iota((dp, dp), 1), 1.0, 0.0)
    starts = mm(tallies, before, precision=exact)
    line = iota((rows, 1), 0)
    sender, group, level = line >> log2(tensor * depth), (line >> log2(depth)) & (tensor - 1), line & (depth - 1)
    by_group = jnp.where(iota((rows, tensor), 1) == group, 1.0, 0.0)
    own = iota((rows, dp), 1) == sender

    def of_row(table):
        wide = mm(by_group, table, precision=exact)
        return jnp.sum(jnp.where(own, wide, 0.0), axis=1, keepdims=True).astype(I32)

    start = of_row(starts)
    end = of_row(starts + tallies)
    rank = start + ((mine - start) & (dp - 1)) + level * dp
    balanced = group * (count // tensor) + ((rank - mine) >> log2(dp))
    to_row = one_hot((iota((rows, count), 1) == balanced) & (rank < end))
    of_slot = one_hot(iota((places, count), 0) == slots[...])
    chosen = mm(to_row, of_slot, NT)
    taken = jnp.sum(chosen, axis=0, keepdims=True) > 0.5
    inputs = mm(features[...], chosen.astype(BF16), TN).astype(BF16)
    keep = 1.0 - resets[...].astype(F32)
    old_cell = cell[...]

    def gate(q):
        low = q * share
        column = jnp.transpose(jnp.broadcast_to(bias[q : q + 1, :], (places, share)))
        return mm(weight[q], inputs) + (sums[low : low + share, :] * keep + column)

    next_cell = jax.nn.sigmoid(gate(1)) * (old_cell * keep) + jax.nn.sigmoid(gate(0)) * jnp.tanh(gate(2))
    next_hidden = jax.nn.sigmoid(gate(3)) * jnp.tanh(next_cell)
    values = mm(heads[...], next_hidden.astype(BF16))
    sent[...] = mm(chosen, values, NT, precision=exact)
    cell_out[...] = jnp.where(taken, next_cell, old_cell)
    hidden_out[...] = jnp.where(taken, next_hidden, hidden[...])


def core(features, sums, bias, weight, hidden, cell, heads, slots, counts, resets):
    share = hidden.shape[0]
    return pl.pallas_call(
        functools.partial(core_kernel, lambda: lax.axis_index("dp")),
        name="core",
        out_shape=(
            jax.ShapeDtypeStruct((features.shape[0], heads.shape[0]), F32),
            jax.ShapeDtypeStruct(hidden.shape, F32),
            jax.ShapeDtypeStruct(cell.shape, F32),
        ),
        in_specs=[VMEM] * 10,
        out_specs=(VMEM,) * 3,
        compiler_params=pltpu.CompilerParams(vmem_limit_bytes=24 << 20),
        cost_estimate=pl.CostEstimate(
            flops=8 * share * weight.shape[2] * hidden.shape[1], bytes_accessed=4_000_000, transcendentals=0
        ),
    )(features, sums, bias, weight, hidden, cell, heads, slots, counts, resets)


def answers_kernel(tensor, dp_index, tensor_index, counts, received, out):
    dp = counts.shape[1]
    rows, cap = received.shape[0], out.shape[1]
    depth = cap // dp
    start = jnp.int32(0)
    for a in range(dp):
        start = start + jnp.where(a < dp_index(), counts[tensor_index(), a], 0)
    own = counts[tensor_index(), dp_index()]
    line = iota((rows, cap), 0)
    giver, level = line >> log2(tensor * depth), line & (depth - 1)
    arrival = ((giver - start) & (dp - 1)) + level * dp
    place = jnp.where((iota((rows, cap), 1) == arrival) & (arrival < own), 1.0, 0.0)
    out[...] = mm(received[...], place, TN, precision=lax.Precision.HIGHEST)


def answers(counts, received, cap):
    return pl.pallas_call(
        functools.partial(
            answers_kernel,
            counts.shape[0],
            lambda: lax.axis_index("dp"),
            lambda: lax.axis_index("tensor"),
        ),
        name="answers",
        out_shape=jax.ShapeDtypeStruct((received.shape[1], cap), F32),
        in_specs=[SMEM, VMEM],
        out_specs=VMEM,
    )(counts, received)


def body(
    frames, counts, slot_ids, reset_flags, hidden_state, cell_state,
    conv_first, conv_second, conv_third, res_first, res_second,
    projection, input_weight, recur_weight, gate_bias, head_weight,
):
    tensor = lax.axis_size("tensor")
    own = hidden_state.astype(BF16)
    pieces = [own] + [
        lax.ppermute(own, "tensor", [(i, (i + back) % tensor) for i in range(tensor)])
        for back in range(1, tensor)
    ]
    kernels = (conv_first, conv_second, conv_third, res_first, res_second)
    features = encode_rows(frames, counts, kernels, projection)
    features, pieces = lax.optimization_barrier((features, pieces))
    features = lax.all_to_all(features, ("dp", "tensor"), 0, 0, tiled=True)
    sums = recurrent(recur_weight, pieces)
    sent, hidden_after, cell_after = core(
        features, sums, gate_bias, input_weight, hidden_state, cell_state, head_weight, slot_ids, counts, reset_flags
    )
    received = lax.all_to_all(sent, ("dp", "tensor"), 0, 0, tiled=True)
    return answers(counts, received, frames.shape[0]), hidden_after, cell_after


def solution(mesh):
    return jax.shard_map(
        body,
        mesh=mesh,
        in_specs=(
            P(("dp", "tensor"), None, None, None),
            P(),
            P("dp", None),
            P("dp", None),
            P("tensor", "dp"),
            P("tensor", "dp"),
            P(),
            P(),
            P(),
            P(),
            P(),
            P(),
            P(None, "tensor", None),
            P(None, "tensor", None),
            P(None, "tensor"),
            P(None, "tensor"),
        ),
        out_specs=(P(None, ("dp", "tensor")), P("tensor", "dp"), P("tensor", "dp")),
        check_vma=False,
    )
```

```python
import functools

import jax
import jax.numpy as jnp
import numpy as np
from jax import lax
from jax.experimental import pallas as pl
from jax.experimental.pallas import tpu as pltpu
from jax.sharding import PartitionSpec as P

F32, BF16, I32 = jnp.float32, jnp.bfloat16, jnp.int32
LANES = 128
VMEM_MOST = 67_043_328
PACK = 16
Y1, Y2, P3, Y4 = 12, 6, 2, 4
NN = (((1,), (0,)), ((), ()))
NT = (((1,), (1,)), ((), ()))
TN = (((0,), (0,)), ((), ()))
VMEM = pl.BlockSpec(memory_space=pltpu.VMEM)
SMEM = pl.BlockSpec(memory_space=pltpu.SMEM)
HBM = pl.BlockSpec(memory_space=pltpu.HBM)


def mm(a, b, dims=NN, precision=None):
    return lax.dot_general(a, b, dims, precision=precision, preferred_element_type=F32)


def iota(shape, axis):
    return lax.broadcasted_iota(I32, shape, axis)


def log2(n):
    assert n & (n - 1) == 0
    return n.bit_length() - 1


def one_hot(mask):
    return jnp.where(mask, 1.0, 0.0).astype(BF16)


class Sizes:
    def __init__(self, frames, first, second, projection):
        self.cap, self.c0, self.f, _ = frames
        self.c1, self.c2, self.feat = first[0], second[0], projection[0]
        self.w1 = -(-self.f // 2)
        self.w2 = -(-self.w1 // 2)
        self.w3 = -(-self.w2 // 2)
        self.n1 = LANES // self.w1
        self.n2 = 2 * self.n1
        assert self.f % 4 == 0 and self.w2 % 2 == 1 and self.n2 * self.w2 <= LANES
        assert self.f % Y1 == 0 and Y1 % 2 == 0 and self.w1 % Y2 == 0 and Y2 % 2 == 0
        self.pad1 = PACK // self.c0
        self.win1 = Y1 + 2 * self.pad1
        self.win2 = Y2 + 3
        self.win3 = 2 * P3 + 3
        self.win4 = Y4 + 2
        self.subs = -(-self.cap // self.n1)
        self.groups = -(-self.cap // self.n2)
        self.blocks3 = -(-self.w3 // P3)
        self.blocks4 = -(-self.w3 // Y4)
        self.wide = -(-self.w3 * self.cap // LANES) * LANES
        assert self.wide - self.w3 * self.cap >= self.cap

    def tables(self):
        rows = []
        four = np.arange(4 * LANES)
        quarter, lane = four // LANES, four % LANES

        def source(width, half, where, count):
            image, j = lane // half, lane % half
            x = 2 * j + quarter - 1
            live = (image < count) & (x >= 0) & (x < width)
            return np.where(live, where(image) + x, -1)

        for i in range(self.n1):
            own = source(self.f, self.w1, lambda image: 0 * image, self.n1)
            rows.append(np.where(lane // self.w1 == i, own, -1))
        rows.append(
            source(
                self.w1,
                self.w2,
                lambda image: image // self.n1 * LANES + image % self.n1 * self.w1,
                self.n2,
            )
        )
        rows.append(source(self.w2, self.w3, lambda image: image * self.w2, self.n2))
        final = np.arange(self.wide)
        x, image = final // self.cap, final % self.cap
        rows.append(np.where(x < self.w3, image * self.w3 + x, -(1 << 20)))
        k1, k2 = np.arange(3 * self.win1 * self.c0), np.arange(3 * self.win2 * self.c1)
        k3, k4 = np.arange(self.win3 * self.c2), np.arange(self.win4 * self.c2)
        for k, window, c in ((k1, self.win1, self.c0), (k2, self.win2, self.c1)):
            rows += [k // (window * c), k % (window * c) // c, k % c]
        for k, c in ((k3, self.c2), (k4, self.c2)):
            rows += [k // c, k % c]
        n = self.c2 * self.w3
        k = np.arange(n)
        rows.append(k % self.w3 * self.c2 + k // self.w3)
        k = np.arange(PACK * self.w3)
        rows += [k % self.w3, k // self.w3]
        width = max(len(r) for r in rows)
        table = np.full((-(-len(rows) // 8) * 8, width), -(1 << 20), np.int32)
        for i, r in enumerate(rows):
            table[i, : len(r)] = r
        return table, [len(r) for r in rows]


def encoder_kernel(
    z, lengths, dp, tensor, dp_index, tensor_index,
    *refs,
):
    far, out, near = refs[:9], refs[9], refs[10:19]
    p1, p2, p3, t1, t2, t3, t4, t5, g1, s1, g2, s2, g3, s3, total, x4, x5, projx, sems = refs[19:]
    counts, table, w1, w2, w3, r1, r2, frames, proj = near
    copies = [pltpu.make_async_copy(a, b, sems.at[i]) for i, (a, b) in enumerate(zip(far, near))]
    for copy in copies:
        copy.start()

    def row(i):
        return table[i : i + 1, : lengths[i]]

    def pick(rows, i):
        return one_hot(iota((rows, lengths[i]), 0) == row(i))

    def zero_padding():
        for ref, top, rows in ((g1, PACK, z.f * z.c0), (g2, z.c1, z.w1 * z.c1), (g3, 2 * z.c2, z.w2 * z.c2)):
            for q in range(4):
                ref[q, :top] = jnp.zeros((top, LANES), BF16)
                low = ref.shape[1] - top - rows
                ref[q, top + rows :] = jnp.zeros((low, LANES), BF16)
        for ref in (x4, x5):
            for q in range(3):
                ref[q, : z.c2] = jnp.zeros((z.c2, z.wide), BF16)
                low = ref.shape[1] - z.c2 - z.w3 * z.c2
                ref[q, z.c2 + z.w3 * z.c2 :] = jnp.zeros((low, z.wide), BF16)
        total[...] = jnp.zeros(total.shape, F32)

    zero_padding()
    for copy in copies[:7]:
        copy.wait()

    for i in range(z.n1):
        p1[i] = pick(z.f, i)
    p2[...] = pick(2 * LANES, z.n1)
    p3[...] = pick(LANES, z.n1 + 1)
    base = z.n1 + 3

    def banded(m, cout, band, kx):
        a = one_hot((iota((m, cout), 0) & (cout - 1)) == iota((m, cout), 1))
        gap = band - (iota((m, kx), 0) >> log2(cout))
        return a, gap

    def band_all(weights, m, cin, cout, index, first):
        kx = lengths[index]
        a, gap = banded(m, cout, row(index + 1), kx)
        acc = jnp.zeros((m, kx), F32)
        for dy in range(3):
            part = jnp.zeros((m, kx), F32)
            for dx in range(3):
                mixed = mm(a, weights[dy, dx], NT).astype(BF16)
                spread = one_hot(
                    (iota((cin, kx), 0) == row(index + 2)) & (row(index) == dx)
                )
                part = part + mm(mixed, spread)
            acc = jnp.where(gap == first + dy, part, acc)
        return acc.astype(BF16)

    def band_each(weights, m, cin, cout, index, target):
        kx = lengths[index]
        a, gap = banded(m, cout, row(index), kx)
        spread = one_hot(iota((cin, kx), 0) == row(index + 1))
        for dx in range(3):
            acc = jnp.zeros((m, kx), F32)
            for dy in range(3):
                mixed = mm(a, weights[dy, dx]).astype(BF16)
                acc = jnp.where(gap == dy, mm(mixed, spread), acc)
            target[dx] = acc.astype(BF16)

    t1[...] = band_all(w1, (Y1 + 1) * z.c1, z.c0, z.c1, base, z.pad1 - 1)
    t2[...] = band_all(w2, (Y2 + 1) * z.c2, z.c1, z.c2, base + 3, 0)
    band_each(w3, (2 * P3 + 1) * z.c2, z.c2, z.c2, base + 6, t3)
    band_each(r1, Y4 * z.c2, z.c2, z.c2, base + 8, t4)
    band_each(r2, Y4 * z.c2, z.c2, z.c2, base + 8, t5)

    own = counts[tensor_index(), dp_index()]
    subs = lax.div(own + (z.n1 - 1), z.n1)
    groups = lax.div(own + (z.n2 - 1), z.n2)
    s1[subs] = jnp.zeros(s1.shape[1:], BF16)

    def sides(ref, dx, low, rows):
        return jnp.concatenate(
            [ref[dx, low : low + rows, :], ref[dx + 1, low : low + rows, :]], axis=1
        )

    def lane_is(rows, half, count, j):
        lane = iota((rows, LANES), 1)
        mask = lane == j
        for i in range(1, count):
            mask = mask | (lane == i * half + j)
        return mask

    def pool_low(acc, half, count):
        even, odd = acc[:, :LANES], acc[:, LANES:]
        nxt = pltpu.roll(even, LANES - 1, 1)
        nxt = jnp.where(lane_is(even.shape[0], half, count, half - 1), even, nxt)
        return jnp.maximum(jnp.maximum(even, odd), nxt)

    def pool_rows(m, c, pairs, last):
        done = []
        for i in range(pairs):
            top = jnp.maximum(m[2 * i * c : (2 * i + 1) * c], m[(2 * i + 1) * c : (2 * i + 2) * c])
            if not (last and i == pairs - 1):
                top = jnp.maximum(top, m[(2 * i + 2) * c : (2 * i + 3) * c])
            done.append(top)
        return jnp.concatenate(done, axis=0)

    def conv_one(s, _):
        mixed = None
        for i in range(z.n1):
            image = frames[jnp.minimum(s * z.n1 + i, z.cap - 1)]
            part = mm(image, p1[i])
            mixed = part if mixed is None else mixed + part
        mixed = mixed.astype(BF16)
        for q in range(4):
            g1[q, PACK : PACK + z.f * z.c0, :] = mixed[:, q * LANES : (q + 1) * LANES]
        for b in range(z.f // Y1):
            low = b * Y1 * z.c0
            around = jnp.concatenate([sides(g1, dx, low, z.win1 * z.c0) for dx in range(3)], axis=0)
            m = pool_low(mm(t1[...], around), z.w1, z.n1)
            rows = pool_rows(m, z.c1, Y1 // 2, b == z.f // Y1 - 1)
            size = Y1 // 2 * z.c1
            s1[s, b * size : (b + 1) * size, :] = jnp.maximum(rows, 0.0).astype(BF16)
        return 0

    copies[7].wait()
    lax.fori_loop(0, subs, conv_one, 0)

    def conv_rest(g, _):
        both = jnp.concatenate([s1[2 * g], s1[2 * g + 1]], axis=1)
        mixed = mm(both, p2[...]).astype(BF16)
        for q in range(4):
            g2[q, z.c1 : z.c1 + z.w1 * z.c1, :] = mixed[:, q * LANES : (q + 1) * LANES]
        for b in range(z.w1 // Y2):
            low = b * Y2 * z.c1
            around = jnp.concatenate([sides(g2, dx, low, z.win2 * z.c1) for dx in range(3)], axis=0)
            m = pool_low(mm(t2[...], around), z.w2, z.n2)
            rows = pool_rows(m, z.c2, Y2 // 2, b == z.w1 // Y2 - 1)
            size = Y2 // 2 * z.c2
            s2[b * size : (b + 1) * size, :] = jnp.maximum(rows, 0.0).astype(BF16)
        mixed = mm(s2[...], p3[...]).astype(BF16)
        for q in range(4):
            g3[q, 2 * z.c2 : 2 * z.c2 + z.w2 * z.c2, :] = mixed[:, q * LANES : (q + 1) * LANES]
        c = z.c2
        for b in range(z.blocks3):
            low = b * 2 * P3 * c
            acc = None
            for dx in range(3):
                part = mm(t3[dx], sides(g3, dx, low, z.win3 * c))
                acc = part if acc is None else acc + part
            even, odd = acc[:, :LANES], acc[:, LANES:]
            n = even.shape[0]
            before = jnp.where(lane_is(n, z.w3, z.n2, 0), even, pltpu.roll(odd, 1, 1))
            odd = jnp.where(lane_is(n, z.w3, z.n2, z.w3 - 1), even, odd)
            m = jnp.maximum(jnp.maximum(even, odd), before)
            for i in range(P3):
                pooled = b * P3 + i
                if pooled >= z.w3:
                    continue
                rows = [2 * i + d for d in range(3) if 0 <= 2 * pooled - 1 + d < z.w2]
                top = None
                for r in rows:
                    piece = m[r * c : (r + 1) * c]
                    top = piece if top is None else jnp.maximum(top, piece)
                s3[pooled * c : (pooled + 1) * c, :] = top.astype(BF16)
        shape = (LANES, z.wide)
        line = iota(shape, 0)
        place = one_hot((line == row(z.n1 + 2) - g * (z.n2 * z.w3)) & (line < z.n2 * z.w3))
        total[...] += mm(s3[...], place)
        return 0

    lax.fori_loop(0, groups, conv_rest, 0)

    c, n = z.c2, z.w3 * z.c2
    live = iota((n, z.wide), 1) < z.w3 * z.cap

    def spread_x(ref, value):
        ref[0, c : c + n, :] = pltpu.roll(value, z.cap, 1).astype(BF16)
        ref[1, c : c + n, :] = value.astype(BF16)
        ref[2, c : c + n, :] = pltpu.roll(value, z.wide - z.cap, 1).astype(BF16)

    def residual(ref, kernel, add):
        pieces = []
        for b in range(z.blocks4):
            low = b * Y4 * c
            acc = None
            for dx in range(3):
                part = mm(kernel[dx], ref[dx, low : low + z.win4 * c, :])
                acc = part if acc is None else acc + part
            pieces.append(acc[: min(Y4, z.w3 - b * Y4) * c])
        value = jnp.concatenate(pieces, axis=0)
        if add is not None:
            value = value + add
        return jnp.maximum(value, 0.0)

    spread_x(x4, jnp.maximum(total[...], 0.0))
    inner = residual(x4, t4, None).astype(BF16).astype(F32)
    spread_x(x5, jnp.where(live, inner, 0.0))
    encoded = residual(x5, t5, total[...]).astype(BF16)

    last = len(lengths) - 3
    order = one_hot(iota((n, n), 0) == row(last))
    turned = jnp.swapaxes(encoded, 0, 1)
    turned = mm(turned, order).astype(BF16)
    copies[8].wait()
    block = PACK * z.w3
    wanted = iota((block, block), 0)
    regroup = one_hot(((wanted >> log2(PACK)) == row(last + 1)) & ((wanted & (PACK - 1)) == row(last + 2)))
    for b in range(n // PACK):
        moved = mm(regroup, proj[b * block : (b + 1) * block, :]).astype(BF16)
        for x in range(z.w3):
            projx[x, b * PACK : (b + 1) * PACK, :] = moved[x * PACK : (x + 1) * PACK]
    acc = None
    for x in range(z.w3):
        part = mm(turned[x * z.cap : (x + 1) * z.cap], projx[x])
        acc = part if acc is None else acc + part
    features = jnp.maximum(acc, 0.0).astype(BF16)

    start = jnp.int32(0)
    for a in range(dp):
        start = start + jnp.where(a < dp_index(), counts[tensor_index(), a], 0)
    depth = z.cap // dp
    shape = (dp * tensor * depth, z.cap)
    r = iota(shape, 0)
    receiver, level = r >> log2(tensor * depth), r & (depth - 1)
    arrival = ((receiver - start) & (dp - 1)) + level * dp
    route = one_hot((iota(shape, 1) == arrival) & (arrival < own))
    out[...] = mm(route, features).astype(BF16).reshape(out.shape)


def encode_rows(frames, counts, kernels, projection):
    first, second, third, res_first, res_second = kernels
    z = Sizes(frames.shape, first.shape, second.shape, projection.shape)
    table, lengths = z.tables()
    dp, tensor = lax.axis_size("dp"), lax.axis_size("tensor")
    images = jnp.transpose(frames, (0, 2, 1, 3)).reshape(z.cap, z.f * z.c0, z.f)
    ci_co, co_ci = (2, 3, 1, 0), (2, 3, 0, 1)
    n = z.w3 * z.c2
    operands = (
        counts,
        jnp.asarray(table),
        jnp.transpose(first, ci_co),
        jnp.transpose(second, ci_co),
        jnp.transpose(third, co_ci),
        jnp.transpose(res_first, co_ci),
        jnp.transpose(res_second, co_ci),
        images,
        jnp.transpose(projection),
    )
    scratch = [pltpu.SMEM(counts.shape, I32)]
    scratch += [pltpu.VMEM(x.shape, x.dtype) for x in operands[1:]]
    scratch += [
        pltpu.VMEM((z.n1, z.f, 4 * LANES), BF16),
        pltpu.VMEM((2 * LANES, 4 * LANES), BF16),
        pltpu.VMEM((LANES, 4 * LANES), BF16),
        pltpu.VMEM(((Y1 + 1) * z.c1, 3 * z.win1 * z.c0), BF16),
        pltpu.VMEM(((Y2 + 1) * z.c2, 3 * z.win2 * z.c1), BF16),
        pltpu.VMEM((3, (2 * P3 + 1) * z.c2, z.win3 * z.c2), BF16),
        pltpu.VMEM((3, Y4 * z.c2, z.win4 * z.c2), BF16),
        pltpu.VMEM((3, Y4 * z.c2, z.win4 * z.c2), BF16),
        pltpu.VMEM((4, z.f * z.c0 + 2 * PACK, LANES), BF16),
        pltpu.VMEM((2 * z.groups + 1, z.w1 * z.c1, LANES), BF16),
        pltpu.VMEM((4, (z.w1 - Y2 + z.win2) * z.c1, LANES), BF16),
        pltpu.VMEM((z.w2 * z.c2, LANES), BF16),
        pltpu.VMEM((4, ((z.blocks3 - 1) * 2 * P3 + z.win3) * z.c2, LANES), BF16),
        pltpu.VMEM((n, LANES), BF16),
        pltpu.VMEM((n, z.wide), F32),
        pltpu.VMEM((3, ((z.blocks4 - 1) * Y4 + z.win4) * z.c2, z.wide), BF16),
        pltpu.VMEM((3, ((z.blocks4 - 1) * Y4 + z.win4) * z.c2, z.wide), BF16),
        pltpu.VMEM((z.w3, n, z.feat), BF16),
        pltpu.SemaphoreType.DMA((len(operands),)),
    ]
    body = functools.partial(
        encoder_kernel, z, lengths, dp, tensor,
        lambda: lax.axis_index("dp"), lambda: lax.axis_index("tensor"),
    )
    depth = z.cap // dp
    return pl.pallas_call(
        body,
        name="encoder",
        out_shape=jax.ShapeDtypeStruct((dp * tensor, depth, z.feat), BF16),
        in_specs=[HBM] * len(operands),
        out_specs=VMEM,
        scratch_shapes=scratch,
        compiler_params=pltpu.CompilerParams(vmem_limit_bytes=VMEM_MOST),
        cost_estimate=pl.CostEstimate(flops=20_000_000_000, bytes_accessed=8_000_000, transcendentals=0),
    )(*operands)


def recurrent_kernel(index, weight, *refs):
    *pieces, out, held, sems = refs
    gates, share, _ = weight.shape
    width = pieces[0].shape[0]
    copies = [pltpu.make_async_copy(weight.at[q], held.at[q], sems.at[q]) for q in range(gates)]
    for copy in copies:
        copy.start()
    tensor = len(pieces)
    for q in range(gates):
        copies[q].wait()
        acc = None
        for back, piece in enumerate(pieces):
            low = pl.multiple_of(((index() - back) & (tensor - 1)) * width, width)
            part = mm(held[q, :, pl.ds(low, width)], piece[...])
            acc = part if acc is None else acc + part
        out[q * share : (q + 1) * share, :] = acc


def recurrent(weight, pieces):
    gates, share, hidden = weight.shape
    slots = pieces[0].shape[1]
    return pl.pallas_call(
        functools.partial(recurrent_kernel, lambda: lax.axis_index("tensor")),
        name="recurrent",
        out_shape=jax.ShapeDtypeStruct((gates * share, slots), F32),
        in_specs=[HBM] + [VMEM] * len(pieces),
        out_specs=VMEM,
        scratch_shapes=[
            pltpu.VMEM(weight.shape, BF16),
            pltpu.SemaphoreType.DMA((gates,)),
        ],
        compiler_params=pltpu.CompilerParams(vmem_limit_bytes=57 << 20),
        cost_estimate=pl.CostEstimate(
            flops=2 * gates * share * hidden * slots, bytes_accessed=2 * gates * share * hidden, transcendentals=0
        ),
    )(weight, *pieces)


def core_kernel(dp_index, features, sums, bias, weight, hidden, cell, heads, slots, counts, resets, sent, hidden_out, cell_out):
    tensor, dp = counts.shape
    depth, count = features.shape[1], slots.shape[1]
    rows = dp * tensor * depth
    share, places = hidden.shape
    mine = dp_index()
    exact = lax.Precision.HIGHEST
    tallies = counts[...].astype(F32)
    before = jnp.where(iota((dp, dp), 0) < iota((dp, dp), 1), 1.0, 0.0)
    starts = mm(tallies, before, precision=exact)
    line = iota((rows, 1), 0)
    sender, group, level = line >> log2(tensor * depth), (line >> log2(depth)) & (tensor - 1), line & (depth - 1)
    by_group = jnp.where(iota((rows, tensor), 1) == group, 1.0, 0.0)
    own = iota((rows, dp), 1) == sender

    def of_row(table):
        wide = mm(by_group, table, precision=exact)
        return jnp.sum(jnp.where(own, wide, 0.0), axis=1, keepdims=True).astype(I32)

    start = of_row(starts)
    end = of_row(starts + tallies)
    rank = start + ((mine - start) & (dp - 1)) + level * dp
    balanced = group * (count // tensor) + ((rank - mine) >> log2(dp))
    to_row = one_hot((iota((rows, count), 1) == balanced) & (rank < end))
    of_slot = one_hot(iota((places, count), 0) == slots[...])
    chosen = mm(to_row, of_slot, NT)
    taken = jnp.sum(chosen, axis=0, keepdims=True) > 0.5
    inputs = mm(features[...].reshape(rows, -1), chosen.astype(BF16), TN).astype(BF16)
    keep = 1.0 - resets[...].astype(F32)
    old_cell = cell[...]

    def gate(q):
        low = q * share
        column = jnp.transpose(jnp.broadcast_to(bias[q : q + 1, :], (places, share)))
        return mm(weight[q], inputs) + (sums[low : low + share, :] * keep + column)

    next_cell = jax.nn.sigmoid(gate(1)) * (old_cell * keep) + jax.nn.sigmoid(gate(0)) * jnp.tanh(gate(2))
    next_hidden = jax.nn.sigmoid(gate(3)) * jnp.tanh(next_cell)
    values = mm(heads[...], next_hidden.astype(BF16))
    sent[...] = mm(chosen, values, NT, precision=exact)
    cell_out[...] = jnp.where(taken, next_cell, old_cell)
    hidden_out[...] = jnp.where(taken, next_hidden, hidden[...])


def core(features, sums, bias, weight, hidden, cell, heads, slots, counts, resets):
    share = hidden.shape[0]
    return pl.pallas_call(
        functools.partial(core_kernel, lambda: lax.axis_index("dp")),
        name="core",
        out_shape=(
            jax.ShapeDtypeStruct((features.shape[0] * features.shape[1], heads.shape[0]), F32),
            jax.ShapeDtypeStruct(hidden.shape, F32),
            jax.ShapeDtypeStruct(cell.shape, F32),
        ),
        in_specs=[VMEM] * 10,
        out_specs=(VMEM,) * 3,
        compiler_params=pltpu.CompilerParams(vmem_limit_bytes=24 << 20),
        cost_estimate=pl.CostEstimate(
            flops=8 * share * weight.shape[2] * hidden.shape[1], bytes_accessed=4_000_000, transcendentals=0
        ),
    )(features, sums, bias, weight, hidden, cell, heads, slots, counts, resets)


def answers_kernel(tensor, dp_index, tensor_index, counts, received, out):
    dp = counts.shape[1]
    rows, cap = received.shape[0], out.shape[1]
    depth = cap // dp
    start = jnp.int32(0)
    for a in range(dp):
        start = start + jnp.where(a < dp_index(), counts[tensor_index(), a], 0)
    own = counts[tensor_index(), dp_index()]
    line = iota((rows, cap), 0)
    giver, level = line >> log2(tensor * depth), line & (depth - 1)
    arrival = ((giver - start) & (dp - 1)) + level * dp
    place = jnp.where((iota((rows, cap), 1) == arrival) & (arrival < own), 1.0, 0.0)
    out[...] = mm(received[...], place, TN, precision=lax.Precision.HIGHEST)


def answers(counts, received, cap):
    return pl.pallas_call(
        functools.partial(
            answers_kernel,
            counts.shape[0],
            lambda: lax.axis_index("dp"),
            lambda: lax.axis_index("tensor"),
        ),
        name="answers",
        out_shape=jax.ShapeDtypeStruct((received.shape[1], cap), F32),
        in_specs=[SMEM, VMEM],
        out_specs=VMEM,
    )(counts, received)


def body(
    frames, counts, slot_ids, reset_flags, hidden_state, cell_state,
    conv_first, conv_second, conv_third, res_first, res_second,
    projection, input_weight, recur_weight, gate_bias, head_weight,
):
    tensor = lax.axis_size("tensor")
    own = hidden_state.astype(BF16)
    pieces = [own] + [
        lax.ppermute(own, "tensor", [(i, (i + back) % tensor) for i in range(tensor)])
        for back in range(1, tensor)
    ]
    kernels = (conv_first, conv_second, conv_third, res_first, res_second)
    features = encode_rows(frames, counts, kernels, projection)
    features, pieces = lax.optimization_barrier((features, pieces))
    features = lax.all_to_all(features, ("dp", "tensor"), 0, 0, tiled=True)
    sums = recurrent(recur_weight, pieces)
    sent, hidden_after, cell_after = core(
        features, sums, gate_bias, input_weight, hidden_state, cell_state, head_weight, slot_ids, counts, reset_flags
    )
    received = lax.all_to_all(sent, ("dp", "tensor"), 0, 0, tiled=True)
    return answers(counts, received, frames.shape[0]), hidden_after, cell_after


def solution(mesh):
    return jax.shard_map(
        body,
        mesh=mesh,
        in_specs=(
            P(("dp", "tensor"), None, None, None),
            P(),
            P("dp", None),
            P("dp", None),
            P("tensor", "dp"),
            P("tensor", "dp"),
            P(),
            P(),
            P(),
            P(),
            P(),
            P(),
            P(None, "tensor", None),
            P(None, "tensor", None),
            P(None, "tensor"),
            P(None, "tensor"),
        ),
        out_specs=(P(None, ("dp", "tensor")), P("tensor", "dp"), P("tensor", "dp")),
        check_vma=False,
    )
```

```python
import functools

import jax
import jax.numpy as jnp
import numpy as np
from jax import lax
from jax.experimental import pallas as pl
from jax.experimental.pallas import tpu as pltpu
from jax.sharding import PartitionSpec as P

F32, BF16, I32 = jnp.float32, jnp.bfloat16, jnp.int32
LANES = 128
VMEM_MOST = 67_043_328
PACK = 16
Y1, Y2 = 12, 3
NN = (((1,), (0,)), ((), ()))
NT = (((1,), (1,)), ((), ()))
TN = (((0,), (0,)), ((), ()))
VMEM = pl.BlockSpec(memory_space=pltpu.VMEM)
SMEM = pl.BlockSpec(memory_space=pltpu.SMEM)
HBM = pl.BlockSpec(memory_space=pltpu.HBM)


def mm(a, b, dims=NN, precision=None):
    return lax.dot_general(a, b, dims, precision=precision, preferred_element_type=F32)


def iota(shape, axis):
    return lax.broadcasted_iota(I32, shape, axis)


def log2(n):
    assert n & (n - 1) == 0
    return n.bit_length() - 1


def one_hot(mask):
    return jnp.where(mask, 1.0, 0.0).astype(BF16)


class Sizes:
    def __init__(self, frames, first, second, projection):
        self.cap, self.c0, self.f, _ = frames
        self.c1, self.c2, self.feat = first[0], second[0], projection[0]
        self.w1 = -(-self.f // 2)
        self.w2 = -(-self.w1 // 2)
        self.w3 = -(-self.w2 // 2)
        self.n1 = LANES // self.w1
        self.n2 = 2 * self.n1
        self.n3 = 2 * self.n2
        assert self.f % 4 == 0 and self.w2 % 2 == 1 and self.n2 * self.w2 <= LANES
        assert self.f % Y1 == 0 and self.w1 % Y2 == 0 and self.w2 % Y2 == 0
        self.pad1 = PACK // self.c0
        self.win1 = Y1 + 2 * self.pad1
        self.win2 = Y2 + 2
        self.subs = -(-self.cap // self.n1)
        self.groups = -(-self.cap // self.n2)
        self.pairs = -(-self.cap // self.n3)
        self.blocks4 = -(-self.w3 // Y2)
        self.wide = -(-self.w3 * self.cap // LANES) * LANES
        assert self.wide - self.w3 * self.cap >= self.cap

    def tables(self):
        none = -(1 << 20)
        rows = []
        four = np.arange(4 * LANES)
        quarter, lane = four // LANES, four % LANES

        def source(x, width, live, where):
            return np.where(live & (x >= 0) & (x < width), where, none)

        j, i = lane // self.n1, lane % self.n1
        x = 2 * j + quarter - 1
        rows.append(source(x, self.f, j < self.w1, i * self.f + x))
        j, i = lane // self.n2, lane % self.n2
        x = 2 * j + quarter - 1
        rows.append(source(x, self.w1, j < self.w2, i // self.n1 * LANES + x * self.n1 + i % self.n1))
        six = np.arange(6 * LANES)
        dx, half, lane = six // (2 * LANES), six // LANES % 2, six % LANES
        evens = self.n2 * self.w3
        odd = lane >= evens
        j, i = np.where(odd, lane - evens, lane) // self.n2, lane % self.n2
        x = 2 * j + odd + dx - 1
        rows.append(source(x, self.w2, lane < self.n2 * self.w2, half * LANES + x * self.n2 + i))
        final = np.arange(self.wide)
        x, image = final // self.cap, final % self.cap
        for pair in range(self.pairs):
            i = image - pair * self.n3
            live = (i >= 0) & (i < self.n3)
            rows.append(source(x, self.w3, live, i // self.n2 * LANES + x * self.n2 + i % self.n2))
        for window, c in ((self.win1, self.c0), (self.win2, self.c1), (self.win2, self.c2)):
            k = np.arange(3 * window * c)
            rows += [k // (window * c), k % (window * c) // c, k % c]
        k = np.arange(self.c2 * self.w3)
        rows.append(k % self.w3 * self.c2 + k // self.w3)
        k = np.arange(PACK * self.w3)
        rows += [k % self.w3, k // self.w3]
        width = max(len(r) for r in rows)
        table = np.full((-(-len(rows) // 8) * 8, width), none, np.int32)
        for i, r in enumerate(rows):
            table[i, : len(r)] = r
        return table, [len(r) for r in rows]


def encoder_kernel(z, lengths, dp, tensor, dp_index, tensor_index, *refs):
    far, out, near = refs[:9], refs[9], refs[10:19]
    p1, p2, p3, t1, t2, t3, t4, t5, g1, s1, g2, s2, g3, s3, total, x4, x5, projx, sems = refs[19:]
    counts, table, w1, w2, w3, r1, r2, frames, proj = near
    copies = [pltpu.make_async_copy(a, b, sems.at[i]) for i, (a, b) in enumerate(zip(far, near))]
    for copy in copies:
        copy.start()

    def row(i):
        return table[i : i + 1, : lengths[i]]

    def pick(rows, i):
        return one_hot(iota((rows, lengths[i]), 0) == row(i))

    for ref, top, rows in ((g1, PACK, z.f * z.c0), (g2, z.c1, z.w1 * z.c1), (g3, z.c2, z.w2 * z.c2)):
        for q in range(ref.shape[0]):
            ref[q, :top] = jnp.zeros((top, ref.shape[2]), BF16)
            low = ref.shape[1] - top - rows
            ref[q, top + rows :] = jnp.zeros((low, ref.shape[2]), BF16)
    for ref in (x4, x5):
        for q in range(3):
            ref[q, : z.c2] = jnp.zeros((z.c2, z.wide), BF16)
            low = ref.shape[1] - z.c2 - z.w3 * z.c2
            ref[q, z.c2 + z.w3 * z.c2 :] = jnp.zeros((low, z.wide), BF16)
    total[...] = jnp.zeros(total.shape, F32)
    for copy in copies[:7]:
        copy.wait()
    own = counts[tensor_index(), dp_index()]
    subs = lax.div(own + (z.n1 - 1), z.n1)
    groups = lax.div(own + (z.n2 - 1), z.n2)
    pairs = lax.div(own + (z.n3 - 1), z.n3)
    s1[subs] = jnp.zeros(s1.shape[1:], BF16)
    s2[groups] = jnp.zeros(s2.shape[1:], BF16)

    p1[...] = pick(z.n1 * z.f, 0)
    p2[...] = pick(2 * LANES, 1)
    p3[...] = pick(2 * LANES, 2)
    base = 3 + z.pairs

    def banded(weights, target, rows, cin, cout, index, first, dims):
        which, line, channel = row(index), row(index + 1), row(index + 2)
        k = lengths[index]
        spread = [one_hot((iota((cin, k), 0) == channel) & (which == dx)) for dx in range(3)]
        lines = []
        for dy in range(3):
            acc = None
            for dx in range(3):
                part = mm(weights[dy, dx], spread[dx], dims)
                acc = part if acc is None else acc + part
            lines.append(acc)
        for y in range(rows):
            value = jnp.zeros((cout, k), F32)
            for dy in range(3):
                value = jnp.where(line == y + first + dy, lines[dy], value)
            target[y * cout : (y + 1) * cout, :] = value.astype(BF16)

    banded(w1, t1, Y1, z.c0, z.c1, base, z.pad1 - 1, TN)
    banded(w2, t2, Y2, z.c1, z.c2, base + 3, 0, TN)
    for weights, target in ((w3, t3), (r1, t4), (r2, t5)):
        banded(weights, target, Y2, z.c2, z.c2, base + 6, 0, NN)

    def sides(ref, dx, low, rows):
        return jnp.concatenate(
            [ref[dx, low : low + rows, :], ref[dx + 1, low : low + rows, :]], axis=1
        )

    def pool_low(acc, n, half):
        even, odd = acc[:, :LANES], acc[:, LANES:]
        nxt = pltpu.roll(even, LANES - n, 1)
        nxt = jnp.where(iota(even.shape, 1) < (half - 1) * n, nxt, even)
        return jnp.maximum(jnp.maximum(even, odd), nxt)

    def pool_rows(blocks, c, height, before, write):
        held, done = [], 0
        for m in blocks:
            held += [m[y * c : (y + 1) * c] for y in range(m.shape[0] // c)]
            while done < -(-height // 2):
                reach = [y for y in range(2 * done - before, 2 * done - before + 3) if 0 <= y < height]
                if reach[-1] >= len(held):
                    break
                top = held[reach[0]]
                for y in reach[1:]:
                    top = jnp.maximum(top, held[y])
                write(done, top)
                done += 1

    def conv_one(s, _):
        images = [frames[jnp.minimum(s * z.n1 + i, z.cap - 1)] for i in range(z.n1)]
        mixed = mm(jnp.concatenate(images, axis=1), p1[...]).astype(BF16)
        for q in range(4):
            g1[q, PACK : PACK + z.f * z.c0, :] = mixed[:, q * LANES : (q + 1) * LANES]

        def blocks():
            for b in range(z.f // Y1):
                low = b * Y1 * z.c0
                around = jnp.concatenate([sides(g1, dx, low, z.win1 * z.c0) for dx in range(3)], axis=0)
                yield pool_low(mm(t1[...], around), z.n1, z.w1)

        def write(y, top):
            s1[s, y * z.c1 : (y + 1) * z.c1, :] = jnp.maximum(top, 0.0).astype(BF16)

        pool_rows(blocks(), z.c1, z.f, 0, write)
        return 0

    def conv_two(g, _):
        both = jnp.concatenate([s1[2 * g], s1[2 * g + 1]], axis=1)
        mixed = mm(both, p2[...]).astype(BF16)
        for q in range(4):
            g2[q, z.c1 : z.c1 + z.w1 * z.c1, :] = mixed[:, q * LANES : (q + 1) * LANES]

        def blocks():
            for b in range(z.w1 // Y2):
                low = b * Y2 * z.c1
                around = jnp.concatenate([sides(g2, dx, low, z.win2 * z.c1) for dx in range(3)], axis=0)
                yield pool_low(mm(t2[...], around), z.n2, z.w2)

        def write(y, top):
            s2[g, y * z.c2 : (y + 1) * z.c2, :] = jnp.maximum(top, 0.0).astype(BF16)

        pool_rows(blocks(), z.c2, z.w1, 0, write)
        return 0

    def conv_three(p, _):
        both = jnp.concatenate([s2[2 * p], s2[2 * p + 1]], axis=1)
        mixed = mm(both, p3[...]).astype(BF16)
        for dx in range(3):
            g3[dx, z.c2 : z.c2 + z.w2 * z.c2, :] = mixed[:, dx * 2 * LANES : (dx + 1) * 2 * LANES]
        evens = z.n2 * z.w3

        def pool(acc):
            lane = iota(acc.shape, 1)
            same = jnp.where(lane < evens - z.n2, pltpu.roll(acc, LANES - evens, 1), acc)
            before = jnp.where(lane >= z.n2, pltpu.roll(acc, LANES - evens + z.n2, 1), acc)
            return jnp.maximum(jnp.maximum(acc, same), before)

        def blocks():
            for b in range(z.w2 // Y2):
                low = b * Y2 * z.c2
                around = jnp.concatenate([g3[dx, low : low + z.win2 * z.c2, :] for dx in range(3)], axis=0)
                acc = mm(t3[...], around)
                yield jnp.concatenate([pool(acc[:, :LANES]), pool(acc[:, LANES:])], axis=1)

        def write(y, top):
            s3[y * z.c2 : (y + 1) * z.c2, :] = top.astype(BF16)

        pool_rows(blocks(), z.c2, z.w2, 1, write)
        source = table[pl.ds(3 + p, 1), :][:, : z.wide]
        total[...] += mm(s3[...], one_hot(iota((2 * LANES, z.wide), 0) == source))
        return 0

    copies[7].wait()
    lax.fori_loop(0, subs, conv_one, 0)
    lax.fori_loop(0, groups, conv_two, 0)
    lax.fori_loop(0, pairs, conv_three, 0)

    c, n = z.c2, z.w3 * z.c2
    live = iota((n, z.wide), 1) < z.w3 * z.cap

    def spread_x(ref, value):
        ref[0, c : c + n, :] = pltpu.roll(value, z.cap, 1).astype(BF16)
        ref[1, c : c + n, :] = value.astype(BF16)
        ref[2, c : c + n, :] = pltpu.roll(value, z.wide - z.cap, 1).astype(BF16)

    def residual(ref, kernel, add):
        pieces = []
        for b in range(z.blocks4):
            low = b * Y2 * c
            around = jnp.concatenate([ref[dx, low : low + z.win2 * c, :] for dx in range(3)], axis=0)
            pieces.append(mm(kernel[...], around)[: min(Y2, z.w3 - b * Y2) * c])
        value = jnp.concatenate(pieces, axis=0)
        if add is not None:
            value = value + add
        return jnp.maximum(value, 0.0)

    spread_x(x4, jnp.maximum(total[...], 0.0))
    inner = residual(x4, t4, None).astype(BF16).astype(F32)
    spread_x(x5, jnp.where(live, inner, 0.0))
    encoded = residual(x5, t5, total[...]).astype(BF16)

    last = len(lengths) - 3
    order = one_hot(iota((n, n), 0) == row(last))
    turned = jnp.swapaxes(encoded, 0, 1)
    turned = mm(turned, order).astype(BF16)
    copies[8].wait()
    block = PACK * z.w3
    wanted = iota((block, block), 0)
    regroup = one_hot(((wanted >> log2(PACK)) == row(last + 1)) & ((wanted & (PACK - 1)) == row(last + 2)))
    for b in range(n // PACK):
        moved = mm(regroup, proj[b * block : (b + 1) * block, :]).astype(BF16)
        for x in range(z.w3):
            projx[x, b * PACK : (b + 1) * PACK, :] = moved[x * PACK : (x + 1) * PACK]
    acc = None
    for x in range(z.w3):
        part = mm(turned[x * z.cap : (x + 1) * z.cap], projx[x])
        acc = part if acc is None else acc + part
    features = jnp.maximum(acc, 0.0).astype(BF16)

    start = jnp.int32(0)
    for a in range(dp):
        start = start + jnp.where(a < dp_index(), counts[tensor_index(), a], 0)
    depth = z.cap // dp
    shape = (dp * tensor * depth, z.cap)
    r = iota(shape, 0)
    receiver, level = r >> log2(tensor * depth), r & (depth - 1)
    arrival = ((receiver - start) & (dp - 1)) + level * dp
    route = one_hot((iota(shape, 1) == arrival) & (arrival < own))
    out[...] = mm(route, features).astype(BF16).reshape(out.shape)


def encode_rows(frames, counts, kernels, projection):
    first, second, third, res_first, res_second = kernels
    z = Sizes(frames.shape, first.shape, second.shape, projection.shape)
    table, lengths = z.tables()
    dp, tensor = lax.axis_size("dp"), lax.axis_size("tensor")
    images = jnp.transpose(frames, (0, 2, 1, 3)).reshape(z.cap, z.f * z.c0, z.f)
    ci_co, co_ci = (2, 3, 1, 0), (2, 3, 0, 1)
    n = z.w3 * z.c2
    operands = (
        counts,
        jnp.asarray(table),
        jnp.transpose(first, ci_co),
        jnp.transpose(second, ci_co),
        jnp.transpose(third, co_ci),
        jnp.transpose(res_first, co_ci),
        jnp.transpose(res_second, co_ci),
        images,
        jnp.transpose(projection),
    )
    tall = pltpu.VMEM((3, (Y2 * z.blocks4 + 2) * z.c2, z.wide), BF16)
    band = pltpu.VMEM((Y2 * z.c2, 3 * z.win2 * z.c2), BF16)
    scratch = [pltpu.SMEM(counts.shape, I32)]
    scratch += [pltpu.VMEM(x.shape, x.dtype) for x in operands[1:]]
    scratch += [
        pltpu.VMEM((z.n1 * z.f, 4 * LANES), BF16),
        pltpu.VMEM((2 * LANES, 4 * LANES), BF16),
        pltpu.VMEM((2 * LANES, 6 * LANES), BF16),
        pltpu.VMEM((Y1 * z.c1, 3 * z.win1 * z.c0), BF16),
        pltpu.VMEM((Y2 * z.c2, 3 * z.win2 * z.c1), BF16),
        band,
        band,
        band,
        pltpu.VMEM((4, z.f * z.c0 + 2 * PACK, LANES), BF16),
        pltpu.VMEM((2 * z.groups + 1, z.w1 * z.c1, LANES), BF16),
        pltpu.VMEM((4, (z.w1 + 2) * z.c1, LANES), BF16),
        pltpu.VMEM((2 * z.pairs + 1, z.w2 * z.c2, LANES), BF16),
        pltpu.VMEM((3, (z.w2 + 2) * z.c2, 2 * LANES), BF16),
        pltpu.VMEM((n, 2 * LANES), BF16),
        pltpu.VMEM((n, z.wide), F32),
        tall,
        tall,
        pltpu.VMEM((z.w3, n, z.feat), BF16),
        pltpu.SemaphoreType.DMA((len(operands),)),
    ]
    body = functools.partial(
        encoder_kernel, z, lengths, dp, tensor,
        lambda: lax.axis_index("dp"), lambda: lax.axis_index("tensor"),
    )
    return pl.pallas_call(
        body,
        name="encoder",
        out_shape=jax.ShapeDtypeStruct((dp * tensor, z.cap // dp, z.feat), BF16),
        in_specs=[HBM] * len(operands),
        out_specs=VMEM,
        scratch_shapes=scratch,
        compiler_params=pltpu.CompilerParams(vmem_limit_bytes=VMEM_MOST),
        cost_estimate=pl.CostEstimate(flops=20_000_000_000, bytes_accessed=8_000_000, transcendentals=0),
    )(*operands)


def recurrent_kernel(index, weight, *refs):
    *pieces, out, held, sems = refs
    gates, share, _ = weight.shape
    width = pieces[0].shape[0]
    copies = [pltpu.make_async_copy(weight.at[q], held.at[q], sems.at[q]) for q in range(gates)]
    for copy in copies:
        copy.start()
    tensor = len(pieces)
    for q in range(gates):
        copies[q].wait()
        acc = None
        for back, piece in enumerate(pieces):
            low = pl.multiple_of(((index() - back) & (tensor - 1)) * width, width)
            part = mm(held[q, :, pl.ds(low, width)], piece[...])
            acc = part if acc is None else acc + part
        out[q * share : (q + 1) * share, :] = acc


def recurrent(weight, pieces):
    gates, share, hidden = weight.shape
    slots = pieces[0].shape[1]
    return pl.pallas_call(
        functools.partial(recurrent_kernel, lambda: lax.axis_index("tensor")),
        name="recurrent",
        out_shape=jax.ShapeDtypeStruct((gates * share, slots), F32),
        in_specs=[HBM] + [VMEM] * len(pieces),
        out_specs=VMEM,
        scratch_shapes=[
            pltpu.VMEM(weight.shape, BF16),
            pltpu.SemaphoreType.DMA((gates,)),
        ],
        compiler_params=pltpu.CompilerParams(vmem_limit_bytes=57 << 20),
        cost_estimate=pl.CostEstimate(
            flops=2 * gates * share * hidden * slots, bytes_accessed=2 * gates * share * hidden, transcendentals=0
        ),
    )(weight, *pieces)


def core_kernel(dp_index, features, sums, bias, weight, hidden, cell, heads, slots, counts, resets, sent, hidden_out, cell_out):
    tensor, dp = counts.shape
    depth, count = features.shape[1], slots.shape[1]
    rows = dp * tensor * depth
    share, places = hidden.shape
    mine = dp_index()
    exact = lax.Precision.HIGHEST
    tallies = counts[...].astype(F32)
    before = jnp.where(iota((dp, dp), 0) < iota((dp, dp), 1), 1.0, 0.0)
    starts = mm(tallies, before, precision=exact)
    line = iota((rows, 1), 0)
    sender, group, level = line >> log2(tensor * depth), (line >> log2(depth)) & (tensor - 1), line & (depth - 1)
    by_group = jnp.where(iota((rows, tensor), 1) == group, 1.0, 0.0)
    own = iota((rows, dp), 1) == sender

    def of_row(table):
        wide = mm(by_group, table, precision=exact)
        return jnp.sum(jnp.where(own, wide, 0.0), axis=1, keepdims=True).astype(I32)

    start = of_row(starts)
    end = of_row(starts + tallies)
    rank = start + ((mine - start) & (dp - 1)) + level * dp
    balanced = group * (count // tensor) + ((rank - mine) >> log2(dp))
    to_row = one_hot((iota((rows, count), 1) == balanced) & (rank < end))
    of_slot = one_hot(iota((places, count), 0) == slots[...])
    chosen = mm(to_row, of_slot, NT)
    taken = jnp.sum(chosen, axis=0, keepdims=True) > 0.5
    inputs = mm(features[...].reshape(rows, -1), chosen.astype(BF16), TN).astype(BF16)
    keep = 1.0 - resets[...].astype(F32)
    old_cell = cell[...]

    def gate(q):
        low = q * share
        column = jnp.transpose(jnp.broadcast_to(bias[q : q + 1, :], (places, share)))
        return mm(weight[q], inputs) + (sums[low : low + share, :] * keep + column)

    next_cell = jax.nn.sigmoid(gate(1)) * (old_cell * keep) + jax.nn.sigmoid(gate(0)) * jnp.tanh(gate(2))
    next_hidden = jax.nn.sigmoid(gate(3)) * jnp.tanh(next_cell)
    values = mm(heads[...], next_hidden.astype(BF16))
    sent[...] = mm(chosen, values, NT, precision=exact)
    cell_out[...] = jnp.where(taken, next_cell, old_cell)
    hidden_out[...] = jnp.where(taken, next_hidden, hidden[...])


def core(features, sums, bias, weight, hidden, cell, heads, slots, counts, resets):
    share = hidden.shape[0]
    return pl.pallas_call(
        functools.partial(core_kernel, lambda: lax.axis_index("dp")),
        name="core",
        out_shape=(
            jax.ShapeDtypeStruct((features.shape[0] * features.shape[1], heads.shape[0]), F32),
            jax.ShapeDtypeStruct(hidden.shape, F32),
            jax.ShapeDtypeStruct(cell.shape, F32),
        ),
        in_specs=[VMEM] * 10,
        out_specs=(VMEM,) * 3,
        compiler_params=pltpu.CompilerParams(vmem_limit_bytes=24 << 20),
        cost_estimate=pl.CostEstimate(
            flops=8 * share * weight.shape[2] * hidden.shape[1], bytes_accessed=4_000_000, transcendentals=0
        ),
    )(features, sums, bias, weight, hidden, cell, heads, slots, counts, resets)


def answers_kernel(tensor, dp_index, tensor_index, counts, received, out):
    dp = counts.shape[1]
    rows, cap = received.shape[0], out.shape[1]
    depth = cap // dp
    start = jnp.int32(0)
    for a in range(dp):
        start = start + jnp.where(a < dp_index(), counts[tensor_index(), a], 0)
    own = counts[tensor_index(), dp_index()]
    line = iota((rows, cap), 0)
    giver, level = line >> log2(tensor * depth), line & (depth - 1)
    arrival = ((giver - start) & (dp - 1)) + level * dp
    place = jnp.where((iota((rows, cap), 1) == arrival) & (arrival < own), 1.0, 0.0)
    out[...] = mm(received[...], place, TN, precision=lax.Precision.HIGHEST)


def answers(counts, received, cap):
    return pl.pallas_call(
        functools.partial(
            answers_kernel,
            counts.shape[0],
            lambda: lax.axis_index("dp"),
            lambda: lax.axis_index("tensor"),
        ),
        name="answers",
        out_shape=jax.ShapeDtypeStruct((received.shape[1], cap), F32),
        in_specs=[SMEM, VMEM],
        out_specs=VMEM,
    )(counts, received)


def body(
    frames, counts, slot_ids, reset_flags, hidden_state, cell_state,
    conv_first, conv_second, conv_third, res_first, res_second,
    projection, input_weight, recur_weight, gate_bias, head_weight,
):
    tensor = lax.axis_size("tensor")
    own = hidden_state.astype(BF16)
    pieces = [own] + [
        lax.ppermute(own, "tensor", [(i, (i + back) % tensor) for i in range(tensor)])
        for back in range(1, tensor)
    ]
    kernels = (conv_first, conv_second, conv_third, res_first, res_second)
    features = encode_rows(frames, counts, kernels, projection)
    features, pieces = lax.optimization_barrier((features, pieces))
    features = lax.all_to_all(features, ("dp", "tensor"), 0, 0, tiled=True)
    sums = recurrent(recur_weight, pieces)
    sent, hidden_after, cell_after = core(
        features, sums, gate_bias, input_weight, hidden_state, cell_state, head_weight, slot_ids, counts, reset_flags
    )
    received = lax.all_to_all(sent, ("dp", "tensor"), 0, 0, tiled=True)
    return answers(counts, received, frames.shape[0]), hidden_after, cell_after


def solution(mesh):
    return jax.shard_map(
        body,
        mesh=mesh,
        in_specs=(
            P(("dp", "tensor"), None, None, None),
            P(),
            P("dp", None),
            P("dp", None),
            P("tensor", "dp"),
            P("tensor", "dp"),
            P(),
            P(),
            P(),
            P(),
            P(),
            P(),
            P(None, "tensor", None),
            P(None, "tensor", None),
            P(None, "tensor"),
            P(None, "tensor"),
        ),
        out_specs=(P(None, ("dp", "tensor")), P("tensor", "dp"), P("tensor", "dp")),
        check_vma=False,
    )
```

```python
import functools

import jax
import jax.numpy as jnp
import numpy as np
from jax import lax
from jax.experimental import pallas as pl
from jax.experimental.pallas import tpu as pltpu
from jax.sharding import PartitionSpec as P

F32, BF16, I32 = jnp.float32, jnp.bfloat16, jnp.int32
LANES = 128
VMEM_MOST = 67_043_328
PACK = 16
Y1, Y2 = 12, 3
NN = (((1,), (0,)), ((), ()))
NT = (((1,), (1,)), ((), ()))
TN = (((0,), (0,)), ((), ()))
VMEM = pl.BlockSpec(memory_space=pltpu.VMEM)
SMEM = pl.BlockSpec(memory_space=pltpu.SMEM)
HBM = pl.BlockSpec(memory_space=pltpu.HBM)


def mm(a, b, dims=NN, precision=None):
    return lax.dot_general(a, b, dims, precision=precision, preferred_element_type=F32)


def iota(shape, axis):
    return lax.broadcasted_iota(I32, shape, axis)


def log2(n):
    assert n & (n - 1) == 0
    return n.bit_length() - 1


def one_hot(mask):
    return jnp.where(mask, 1.0, 0.0).astype(BF16)


class Sizes:
    def __init__(self, frames, first, second, projection):
        self.cap, self.c0, self.f, _ = frames
        self.c1, self.c2, self.feat = first[0], second[0], projection[0]
        self.w1 = -(-self.f // 2)
        self.w2 = -(-self.w1 // 2)
        self.w3 = -(-self.w2 // 2)
        self.n1 = LANES // self.w1
        self.n2 = 2 * self.n1
        self.n3 = 2 * self.n2
        assert self.f % 4 == 0 and self.w2 % 2 == 1 and self.n2 * self.w2 <= LANES
        assert self.f % Y1 == 0 and self.w1 % Y2 == 0 and self.w2 % Y2 == 0
        self.pad1 = PACK // self.c0
        self.win1 = Y1 + 2 * self.pad1
        self.win2 = Y2 + 2
        self.pairs = -(-self.cap // self.n3)
        self.blocks4 = -(-self.w3 // Y2)
        self.wide = -(-self.w3 * self.cap // LANES) * LANES
        assert self.wide - self.w3 * self.cap >= self.cap

    def tables(self):
        none = -(1 << 20)
        rows = []
        four = np.arange(4 * LANES)
        quarter, lane = four // LANES, four % LANES

        def source(x, width, live, where):
            return np.where(live & (x >= 0) & (x < width), where, none)

        j, i = lane // self.n1, lane % self.n1
        x = 2 * j + quarter - 1
        rows.append(source(x, self.f, j < self.w1, i * self.f + x))
        j, i = lane // self.n2, lane % self.n2
        x = 2 * j + quarter - 1
        rows.append(source(x, self.w1, j < self.w2, i // self.n1 * LANES + x * self.n1 + i % self.n1))
        six = np.arange(6 * LANES)
        dx, half, lane = six // (2 * LANES), six // LANES % 2, six % LANES
        evens = self.n2 * self.w3
        odd = lane >= evens
        j, i = np.where(odd, lane - evens, lane) // self.n2, lane % self.n2
        x = 2 * j + odd + dx - 1
        rows.append(source(x, self.w2, lane < self.n2 * self.w2, half * LANES + x * self.n2 + i))
        final = np.arange(self.wide)
        x, image = final // self.cap, final % self.cap
        for pair in range(self.pairs):
            i = image - pair * self.n3
            live = (i >= 0) & (i < self.n3)
            rows.append(source(x, self.w3, live, i // self.n2 * LANES + x * self.n2 + i % self.n2))
        for window, c in ((self.win1, self.c0), (self.win2, self.c1), (self.win2, self.c2)):
            k = np.arange(3 * window * c)
            rows += [k // (window * c), k % (window * c) // c, k % c]
        k = np.arange(self.c2 * self.w3)
        rows.append(k % self.w3 * self.c2 + k // self.w3)
        k = np.arange(PACK * self.w3)
        rows += [k % self.w3, k // self.w3]
        width = max(len(r) for r in rows)
        table = np.full((-(-len(rows) // 8) * 8, width), none, np.int32)
        for i, r in enumerate(rows):
            table[i, : len(r)] = r
        return table, [len(r) for r in rows]


def encoder_kernel(z, lengths, dp, tensor, dp_index, tensor_index, *refs):
    far, out, near = refs[:9], refs[9], refs[10:19]
    p1, p2, p3, t1, t2, t3, t4, t5, g1, s1, g2, s2, g3, s3, x4, x5, projx, sems = refs[19:]
    counts, table, w1, w2, w3, r1, r2, frames, proj = near
    copies = [pltpu.make_async_copy(a, b, sems.at[i]) for i, (a, b) in enumerate(zip(far, near))]
    for copy in copies:
        copy.start()

    def row(i):
        return table[i : i + 1, : lengths[i]]

    def pick(rows, i):
        return one_hot(iota((rows, lengths[i]), 0) == row(i))

    maps = [(g1.at[i], PACK, z.f * z.c0) for i in range(4)]
    maps += [(g2.at[i], z.c1, z.w1 * z.c1) for i in range(2)]
    for ref, top, rows in maps + [(g3, z.c2, z.w2 * z.c2)]:
        for q in range(ref.shape[0]):
            ref[q, :top] = jnp.zeros((top, ref.shape[2]), BF16)
            low = ref.shape[1] - top - rows
            ref[q, top + rows :] = jnp.zeros((low, ref.shape[2]), BF16)
    for ref in (x4, x5):
        for q in range(3):
            ref[q, : z.c2] = jnp.zeros((z.c2, z.wide), BF16)
            low = ref.shape[1] - z.c2 - z.w3 * z.c2
            ref[q, z.c2 + z.w3 * z.c2 :] = jnp.zeros((low, z.wide), BF16)
    for copy in copies[:7]:
        copy.wait()
    own = counts[tensor_index(), dp_index()]
    pairs = lax.div(own + (z.n3 - 1), z.n3)
    s3[...] = jnp.zeros(s3.shape, BF16)

    p1[...] = pick(z.n1 * z.f, 0)
    p2[...] = pick(2 * LANES, 1)
    p3[...] = pick(2 * LANES, 2)
    base = 3 + z.pairs

    def banded(weights, target, rows, cin, cout, index, first, dims):
        which, line, channel = row(index), row(index + 1), row(index + 2)
        k = lengths[index]
        spread = [one_hot((iota((cin, k), 0) == channel) & (which == dx)) for dx in range(3)]
        lines = []
        for dy in range(3):
            acc = None
            for dx in range(3):
                part = mm(weights[dy, dx], spread[dx], dims)
                acc = part if acc is None else acc + part
            lines.append(acc)
        for y in range(rows):
            value = jnp.zeros((cout, k), F32)
            for dy in range(3):
                value = jnp.where(line == y + first + dy, lines[dy], value)
            target[y * cout : (y + 1) * cout, :] = value.astype(BF16)

    banded(w1, t1, Y1, z.c0, z.c1, base, z.pad1 - 1, TN)
    banded(w2, t2, Y2, z.c1, z.c2, base + 3, 0, TN)
    for weights, target in ((w3, t3), (r1, t4), (r2, t5)):
        banded(weights, target, Y2, z.c2, z.c2, base + 6, 0, NN)

    def sides(ref, dx, low, rows):
        return jnp.concatenate(
            [ref[dx, low : low + rows, :], ref[dx + 1, low : low + rows, :]], axis=1
        )

    def pool_low(acc, n, half):
        even, odd = acc[:, :LANES], acc[:, LANES:]
        nxt = pltpu.roll(even, LANES - n, 1)
        nxt = jnp.where(iota(even.shape, 1) < (half - 1) * n, nxt, even)
        return jnp.maximum(jnp.maximum(even, odd), nxt)

    def pool_rows(blocks, c, height, before, write):
        held, done = [], 0
        for m in blocks:
            held += [m[y * c : (y + 1) * c] for y in range(m.shape[0] // c)]
            while done < -(-height // 2):
                reach = [y for y in range(2 * done - before, 2 * done - before + 3) if 0 <= y < height]
                if reach[-1] >= len(held):
                    break
                top = held[reach[0]]
                for y in reach[1:]:
                    top = jnp.maximum(top, held[y])
                write(done, top)
                done += 1

    def mix_one(s, slot):
        images = [frames[jnp.minimum(s * z.n1 + i, z.cap - 1)] for i in range(z.n1)]
        mixed = mm(jnp.concatenate(images, axis=1), p1[...]).astype(BF16)
        for q in range(4):
            g1[slot, q, PACK : PACK + z.f * z.c0, :] = mixed[:, q * LANES : (q + 1) * LANES]

    def conv_one(slot):
        def blocks():
            for b in range(z.f // Y1):
                low = b * Y1 * z.c0
                around = jnp.concatenate(
                    [sides(g1.at[slot], dx, low, z.win1 * z.c0) for dx in range(3)], axis=0
                )
                yield pool_low(mm(t1[...], around).astype(BF16), z.n1, z.w1)

        def write(y, top):
            lanes = slice(slot % 2 * LANES, (slot % 2 + 1) * LANES)
            s1[slot // 2, y * z.c1 : (y + 1) * z.c1, lanes] = jnp.maximum(top, 0)

        pool_rows(blocks(), z.c1, z.f, 0, write)

    def conv_two(half):
        mixed = mm(s1[half], p2[...]).astype(BF16)
        for q in range(4):
            g2[half, q, z.c1 : z.c1 + z.w1 * z.c1, :] = mixed[:, q * LANES : (q + 1) * LANES]

        def blocks():
            for b in range(z.w1 // Y2):
                low = b * Y2 * z.c1
                around = jnp.concatenate(
                    [sides(g2.at[half], dx, low, z.win2 * z.c1) for dx in range(3)], axis=0
                )
                yield pool_low(mm(t2[...], around).astype(BF16), z.n2, z.w2)

        def write(y, top):
            s2[y * z.c2 : (y + 1) * z.c2, half * LANES : (half + 1) * LANES] = jnp.maximum(top, 0)

        pool_rows(blocks(), z.c2, z.w1, 0, write)

    def conv_three(p):
        mixed = mm(s2[...], p3[...]).astype(BF16)
        for dx in range(3):
            g3[dx, z.c2 : z.c2 + z.w2 * z.c2, :] = mixed[:, dx * 2 * LANES : (dx + 1) * 2 * LANES]
        evens = z.n2 * z.w3

        def pool(acc):
            lane = iota(acc.shape, 1)
            same = jnp.where(lane < evens - z.n2, pltpu.roll(acc, LANES - evens, 1), acc)
            before = jnp.where(lane >= z.n2, pltpu.roll(acc, LANES - evens + z.n2, 1), acc)
            return jnp.maximum(jnp.maximum(acc, same), before)

        def blocks():
            for b in range(z.w2 // Y2):
                low = b * Y2 * z.c2
                around = jnp.concatenate([g3[dx, low : low + z.win2 * z.c2, :] for dx in range(3)], axis=0)
                acc = mm(t3[...], around).astype(BF16)
                yield jnp.concatenate([pool(acc[:, :LANES]), pool(acc[:, LANES:])], axis=1)

        def write(y, top):
            s3[p, y * z.c2 : (y + 1) * z.c2, :] = top

        pool_rows(blocks(), z.c2, z.w2, 1, write)

    def convolve(p, _):
        for half in range(2):
            for slot in (2 * half, 2 * half + 1):
                mix_one(4 * p + slot, slot)
        for half in range(2):
            for slot in (2 * half, 2 * half + 1):
                conv_one(slot)
        for half in range(2):
            conv_two(half)
        conv_three(p)
        return 0

    copies[7].wait()
    lax.fori_loop(0, pairs, convolve, 0)
    total = None
    for p in range(z.pairs):
        part = mm(s3[p], pick(2 * LANES, 3 + p))
        total = part if total is None else total + part

    c, n = z.c2, z.w3 * z.c2
    live = iota((n, z.wide), 1) < z.w3 * z.cap

    def spread_x(ref, value):
        ref[0, c : c + n, :] = pltpu.roll(value, z.cap, 1).astype(BF16)
        ref[1, c : c + n, :] = value.astype(BF16)
        ref[2, c : c + n, :] = pltpu.roll(value, z.wide - z.cap, 1).astype(BF16)

    def residual(ref, kernel, add):
        pieces = []
        for b in range(z.blocks4):
            low = b * Y2 * c
            around = jnp.concatenate([ref[dx, low : low + z.win2 * c, :] for dx in range(3)], axis=0)
            pieces.append(mm(kernel[...], around)[: min(Y2, z.w3 - b * Y2) * c])
        value = jnp.concatenate(pieces, axis=0)
        if add is not None:
            value = value + add
        return jnp.maximum(value, 0.0)

    spread_x(x4, jnp.maximum(total, 0.0))
    inner = residual(x4, t4, None).astype(BF16).astype(F32)
    spread_x(x5, jnp.where(live, inner, 0.0))
    encoded = residual(x5, t5, total).astype(BF16)

    last = len(lengths) - 3
    order = one_hot(iota((n, n), 0) == row(last))
    turned = jnp.swapaxes(encoded, 0, 1)
    turned = mm(turned, order).astype(BF16)
    copies[8].wait()
    block = PACK * z.w3
    wanted = iota((block, block), 0)
    regroup = one_hot(((wanted >> log2(PACK)) == row(last + 1)) & ((wanted & (PACK - 1)) == row(last + 2)))
    for b in range(n // PACK):
        moved = mm(regroup, proj[b * block : (b + 1) * block, :]).astype(BF16)
        for x in range(z.w3):
            projx[x, b * PACK : (b + 1) * PACK, :] = moved[x * PACK : (x + 1) * PACK]
    acc = None
    for x in range(z.w3):
        part = mm(turned[x * z.cap : (x + 1) * z.cap], projx[x])
        acc = part if acc is None else acc + part
    features = jnp.maximum(acc, 0.0).astype(BF16)

    start = jnp.int32(0)
    for a in range(dp):
        start = start + jnp.where(a < dp_index(), counts[tensor_index(), a], 0)
    depth = z.cap // dp
    shape = (dp * tensor * depth, z.cap)
    r = iota(shape, 0)
    receiver, level = r >> log2(tensor * depth), r & (depth - 1)
    arrival = ((receiver - start) & (dp - 1)) + level * dp
    route = one_hot((iota(shape, 1) == arrival) & (arrival < own))
    out[...] = mm(route, features).astype(BF16).reshape(out.shape)


def encode_rows(frames, counts, kernels, projection):
    first, second, third, res_first, res_second = kernels
    z = Sizes(frames.shape, first.shape, second.shape, projection.shape)
    table, lengths = z.tables()
    dp, tensor = lax.axis_size("dp"), lax.axis_size("tensor")
    images = jnp.transpose(frames, (0, 2, 1, 3)).reshape(z.cap, z.f * z.c0, z.f)
    ci_co, co_ci = (2, 3, 1, 0), (2, 3, 0, 1)
    n = z.w3 * z.c2
    operands = (
        counts,
        jnp.asarray(table),
        jnp.transpose(first, ci_co),
        jnp.transpose(second, ci_co),
        jnp.transpose(third, co_ci),
        jnp.transpose(res_first, co_ci),
        jnp.transpose(res_second, co_ci),
        images,
        jnp.transpose(projection),
    )
    tall = pltpu.VMEM((3, (Y2 * z.blocks4 + 2) * z.c2, z.wide), BF16)
    band = pltpu.VMEM((Y2 * z.c2, 3 * z.win2 * z.c2), BF16)
    scratch = [pltpu.SMEM(counts.shape, I32)]
    scratch += [pltpu.VMEM(x.shape, x.dtype) for x in operands[1:]]
    scratch += [
        pltpu.VMEM((z.n1 * z.f, 4 * LANES), BF16),
        pltpu.VMEM((2 * LANES, 4 * LANES), BF16),
        pltpu.VMEM((2 * LANES, 6 * LANES), BF16),
        pltpu.VMEM((Y1 * z.c1, 3 * z.win1 * z.c0), BF16),
        pltpu.VMEM((Y2 * z.c2, 3 * z.win2 * z.c1), BF16),
        band,
        band,
        band,
        pltpu.VMEM((4, 4, z.f * z.c0 + 2 * PACK, LANES), BF16),
        pltpu.VMEM((2, z.w1 * z.c1, 2 * LANES), BF16),
        pltpu.VMEM((2, 4, (z.w1 + 2) * z.c1, LANES), BF16),
        pltpu.VMEM((z.w2 * z.c2, 2 * LANES), BF16),
        pltpu.VMEM((3, (z.w2 + 2) * z.c2, 2 * LANES), BF16),
        pltpu.VMEM((z.pairs, n, 2 * LANES), BF16),
        tall,
        tall,
        pltpu.VMEM((z.w3, n, z.feat), BF16),
        pltpu.SemaphoreType.DMA((len(operands),)),
    ]
    body = functools.partial(
        encoder_kernel, z, lengths, dp, tensor,
        lambda: lax.axis_index("dp"), lambda: lax.axis_index("tensor"),
    )
    return pl.pallas_call(
        body,
        name="encoder",
        out_shape=jax.ShapeDtypeStruct((dp * tensor, z.cap // dp, z.feat), BF16),
        in_specs=[HBM] * len(operands),
        out_specs=VMEM,
        scratch_shapes=scratch,
        compiler_params=pltpu.CompilerParams(vmem_limit_bytes=VMEM_MOST),
        cost_estimate=pl.CostEstimate(flops=20_000_000_000, bytes_accessed=8_000_000, transcendentals=0),
    )(*operands)


def recurrent_kernel(index, weight, *refs):
    *pieces, out, hidden = refs
    gates, share, _ = weight.shape
    width = pieces[0].shape[0]
    for back, piece in enumerate(pieces):
        low = pl.multiple_of(((index() - back) & (len(pieces) - 1)) * width, width)
        hidden[pl.ds(low, width), :] = piece[...]
    for q in range(gates):
        out[q * share : (q + 1) * share, :] = mm(weight[q], hidden[...])


def recurrent(weight, pieces):
    gates, share, hidden = weight.shape
    slots = pieces[0].shape[1]
    return pl.pallas_call(
        functools.partial(recurrent_kernel, lambda: lax.axis_index("tensor")),
        name="recurrent",
        out_shape=jax.ShapeDtypeStruct((gates * share, slots), F32),
        in_specs=[VMEM] * (1 + len(pieces)),
        out_specs=VMEM,
        scratch_shapes=[pltpu.VMEM((hidden, slots), BF16)],
        compiler_params=pltpu.CompilerParams(vmem_limit_bytes=24 << 20),
        cost_estimate=pl.CostEstimate(
            flops=2 * gates * share * hidden * slots, bytes_accessed=2 * gates * share * hidden, transcendentals=0
        ),
    )(weight, *pieces)


def core_kernel(dp_index, features, sums, bias, weight, hidden, cell, heads, slots, counts, resets, sent, hidden_out, cell_out):
    tensor, dp = counts.shape
    depth, count = features.shape[1], slots.shape[1]
    rows = dp * tensor * depth
    share, places = hidden.shape
    mine = dp_index()
    exact = lax.Precision.HIGHEST
    tallies = counts[...].astype(F32)
    before = jnp.where(iota((dp, dp), 0) < iota((dp, dp), 1), 1.0, 0.0)
    starts = mm(tallies, before, precision=exact)
    line = iota((rows, 1), 0)
    sender, group, level = line >> log2(tensor * depth), (line >> log2(depth)) & (tensor - 1), line & (depth - 1)
    by_group = jnp.where(iota((rows, tensor), 1) == group, 1.0, 0.0)
    own = iota((rows, dp), 1) == sender

    def of_row(table):
        wide = mm(by_group, table, precision=exact)
        return jnp.sum(jnp.where(own, wide, 0.0), axis=1, keepdims=True).astype(I32)

    start = of_row(starts)
    end = of_row(starts + tallies)
    rank = start + ((mine - start) & (dp - 1)) + level * dp
    balanced = group * (count // tensor) + ((rank - mine) >> log2(dp))
    to_row = one_hot((iota((rows, count), 1) == balanced) & (rank < end))
    of_slot = one_hot(iota((places, count), 0) == slots[...])
    chosen = mm(to_row, of_slot, NT)
    taken = jnp.sum(chosen, axis=0, keepdims=True) > 0.5
    inputs = mm(features[...].reshape(rows, -1), chosen.astype(BF16), TN).astype(BF16)
    keep = 1.0 - resets[...].astype(F32)
    old_cell = cell[...]

    def gate(q):
        low = q * share
        column = jnp.transpose(jnp.broadcast_to(bias[q : q + 1, :], (places, share)))
        return mm(weight[q], inputs) + (sums[low : low + share, :] * keep + column)

    next_cell = jax.nn.sigmoid(gate(1)) * (old_cell * keep) + jax.nn.sigmoid(gate(0)) * jnp.tanh(gate(2))
    next_hidden = jax.nn.sigmoid(gate(3)) * jnp.tanh(next_cell)
    values = mm(heads[...], next_hidden.astype(BF16))
    sent[...] = mm(chosen, values, NT, precision=exact)
    cell_out[...] = jnp.where(taken, next_cell, old_cell)
    hidden_out[...] = jnp.where(taken, next_hidden, hidden[...])


def core(features, sums, bias, weight, hidden, cell, heads, slots, counts, resets):
    share = hidden.shape[0]
    return pl.pallas_call(
        functools.partial(core_kernel, lambda: lax.axis_index("dp")),
        name="core",
        out_shape=(
            jax.ShapeDtypeStruct((features.shape[0] * features.shape[1], heads.shape[0]), F32),
            jax.ShapeDtypeStruct(hidden.shape, F32),
            jax.ShapeDtypeStruct(cell.shape, F32),
        ),
        in_specs=[VMEM] * 10,
        out_specs=(VMEM,) * 3,
        compiler_params=pltpu.CompilerParams(vmem_limit_bytes=24 << 20),
        cost_estimate=pl.CostEstimate(
            flops=8 * share * weight.shape[2] * hidden.shape[1], bytes_accessed=4_000_000, transcendentals=0
        ),
    )(features, sums, bias, weight, hidden, cell, heads, slots, counts, resets)


def answers_kernel(tensor, dp_index, tensor_index, counts, received, out):
    dp = counts.shape[1]
    rows, cap = received.shape[0], out.shape[1]
    depth = cap // dp
    start = jnp.int32(0)
    for a in range(dp):
        start = start + jnp.where(a < dp_index(), counts[tensor_index(), a], 0)
    own = counts[tensor_index(), dp_index()]
    line = iota((rows, cap), 0)
    giver, level = line >> log2(tensor * depth), line & (depth - 1)
    arrival = ((giver - start) & (dp - 1)) + level * dp
    place = jnp.where((iota((rows, cap), 1) == arrival) & (arrival < own), 1.0, 0.0)
    out[...] = mm(received[...], place, TN, precision=lax.Precision.HIGHEST)


def answers(counts, received, cap):
    return pl.pallas_call(
        functools.partial(
            answers_kernel,
            counts.shape[0],
            lambda: lax.axis_index("dp"),
            lambda: lax.axis_index("tensor"),
        ),
        name="answers",
        out_shape=jax.ShapeDtypeStruct((received.shape[1], cap), F32),
        in_specs=[SMEM, VMEM],
        out_specs=VMEM,
        compiler_params=pltpu.CompilerParams(vmem_limit_bytes=8 << 20),
    )(counts, received)


def body(
    frames, counts, slot_ids, reset_flags, hidden_state, cell_state,
    conv_first, conv_second, conv_third, res_first, res_second,
    projection, input_weight, recur_weight, gate_bias, head_weight,
):
    tensor = lax.axis_size("tensor")
    own = hidden_state.astype(BF16)
    pieces = [own] + [
        lax.ppermute(own, "tensor", [(i, (i + back) % tensor) for i in range(tensor)])
        for back in range(1, tensor)
    ]
    kernels = (conv_first, conv_second, conv_third, res_first, res_second)
    features = encode_rows(frames, counts, kernels, projection)
    features, pieces = lax.optimization_barrier((features, pieces))
    features = lax.all_to_all(features, ("dp", "tensor"), 0, 0, tiled=True)
    sums = recurrent(recur_weight, pieces)
    sent, hidden_after, cell_after = core(
        features, sums, gate_bias, input_weight, hidden_state, cell_state, head_weight, slot_ids, counts, reset_flags
    )
    received = lax.all_to_all(sent, ("dp", "tensor"), 0, 0, tiled=True)
    return answers(counts, received, frames.shape[0]), hidden_after, cell_after


def solution(mesh):
    return jax.shard_map(
        body,
        mesh=mesh,
        in_specs=(
            P(("dp", "tensor"), None, None, None),
            P(),
            P("dp", None),
            P("dp", None),
            P("tensor", "dp"),
            P("tensor", "dp"),
            P(),
            P(),
            P(),
            P(),
            P(),
            P(),
            P(None, "tensor", None),
            P(None, "tensor", None),
            P(None, "tensor"),
            P(None, "tensor"),
        ),
        out_specs=(P(None, ("dp", "tensor")), P("tensor", "dp"), P("tensor", "dp")),
        check_vma=False,
    )
```

```python
import functools

import jax
import jax.numpy as jnp
from jax import lax
from jax.experimental import pallas as pl
from jax.experimental.pallas import tpu as pltpu
from jax.sharding import PartitionSpec as P

F32, BF16, I32 = jnp.float32, jnp.bfloat16, jnp.int32
LANES = 128
VMEM_MOST = 67_043_328
PACK = 16
Y1, Y2 = 12, 3
NN = (((1,), (0,)), ((), ()))
NT = (((1,), (1,)), ((), ()))
TN = (((0,), (0,)), ((), ()))
VMEM = pl.BlockSpec(memory_space=pltpu.VMEM)
SMEM = pl.BlockSpec(memory_space=pltpu.SMEM)
HBM = pl.BlockSpec(memory_space=pltpu.HBM)


def mm(a, b, dims=NN, precision=None):
    return lax.dot_general(a, b, dims, precision=precision, preferred_element_type=F32)


def iota(shape, axis):
    return lax.broadcasted_iota(I32, shape, axis)


def log2(n):
    assert n & (n - 1) == 0
    return n.bit_length() - 1


def divide(v, n, limit):
    scale = -(-(1 << 16) // n)
    assert all((k * scale) >> 16 == k // n for k in range(limit))
    return (v * scale) >> 16


def one_hot(mask):
    return jnp.where(mask, 1.0, 0.0).astype(BF16)


class Sizes:
    def __init__(self, frames, first, second, projection):
        self.cap, self.c0, self.f, _ = frames
        self.c1, self.c2, self.feat = first[0], second[0], projection[0]
        self.w1 = -(-self.f // 2)
        self.w2 = -(-self.w1 // 2)
        self.w3 = -(-self.w2 // 2)
        self.n1 = LANES // self.w1
        self.n2 = 2 * self.n1
        self.n3 = 2 * self.n2
        assert self.f % 4 == 0 and self.w2 % 2 == 1 and self.n2 * self.w2 <= LANES
        assert self.f % Y1 == 0 and self.w1 % Y2 == 0 and self.w2 % Y2 == 0
        self.pad1 = PACK // self.c0
        self.win1 = Y1 + 2 * self.pad1
        self.win2 = Y2 + 2
        self.pairs = -(-self.cap // self.n3)
        self.blocks4 = -(-self.w3 // Y2)
        self.wide = -(-self.w3 * self.cap // LANES) * LANES
        assert self.wide - self.w3 * self.cap >= self.cap


def encoder_kernel(z, dp, tensor, dp_index, tensor_index, *refs):
    far, out, near = refs[:8], refs[8], refs[9:17]
    p1, p2, p3, t1, t2, t3, t4, t5, g1, s1, g2, s2, g3, s3, x4, x5, p4, flat, sems = refs[17:]
    counts, w1, w2, w3, r1, r2, frames, proj = near
    copies = [pltpu.make_async_copy(a, b, sems.at[i]) for i, (a, b) in enumerate(zip(far, near))]
    for copy in copies:
        copy.start()

    def place(ref, x, width, live, where):
        where = jnp.where(live & (x >= 0) & (x < width), where, -1)
        ref[...] = one_hot(iota(ref.shape, 0) == where)

    def split(columns, n):
        v = iota((1, columns), 1)
        lane = v & (LANES - 1)
        j = divide(lane, n, LANES)
        return v >> log2(LANES), lane, j, lane - j * n

    quarter, _, j, i = split(4 * LANES, z.n1)
    x = 2 * j + quarter - 1
    place(p1, x, z.f, j < z.w1, i * z.f + x)
    quarter, _, j, i = split(4 * LANES, z.n2)
    x = 2 * j + quarter - 1
    upper = (i >= z.n1).astype(I32)
    place(p2, x, z.w1, j < z.w2, upper * (LANES - z.n1) + x * z.n1 + i)
    part, lane, j, i = split(6 * LANES, z.n2)
    odd = (lane >= z.n2 * z.w3).astype(I32)
    x = 2 * (j - odd * z.w3) + odd + (part >> 1) - 1
    place(p3, x, z.w2, lane < z.n2 * z.w2, (part & 1) * LANES + x * z.n2 + i)
    v = iota((1, z.wide), 1)
    for pair in range(z.pairs):
        x, i = v >> log2(z.cap), (v & (z.cap - 1)) - pair * z.n3
        upper = (i >= z.n2).astype(I32)
        place(p4.at[pair], x, z.w3, (i >= 0) & (i < z.n3), upper * (LANES - z.n2) + x * z.n2 + i)

    maps = [(g1.at[i], PACK, z.f * z.c0) for i in range(4)]
    maps += [(g2.at[i], z.c1, z.w1 * z.c1) for i in range(2)]
    for ref, top, rows in maps + [(g3, z.c2, z.w2 * z.c2)]:
        for q in range(ref.shape[0]):
            ref[q, :top] = jnp.zeros((top, ref.shape[2]), BF16)
            low = ref.shape[1] - top - rows
            ref[q, top + rows :] = jnp.zeros((low, ref.shape[2]), BF16)
    for ref in (x4, x5):
        for q in range(3):
            ref[q, : z.c2] = jnp.zeros((z.c2, z.wide), BF16)
            low = ref.shape[1] - z.c2 - z.w3 * z.c2
            ref[q, z.c2 + z.w3 * z.c2 :] = jnp.zeros((low, z.wide), BF16)
    for copy in copies[:6]:
        copy.wait()
    own = counts[tensor_index(), dp_index()]
    pairs = lax.div(own + (z.n3 - 1), z.n3)
    s3[...] = jnp.zeros(s3.shape, BF16)

    def banded(weights, target, rows, cin, cout, window, first, dims):
        k = 3 * window * cin
        v = iota((1, k), 1)
        channel, line = v & (cin - 1), v >> log2(cin)
        which = divide(line, window, 3 * window)
        line = line - which * window
        spread = [one_hot((iota((cin, k), 0) == channel) & (which == dx)) for dx in range(3)]
        lines = []
        for dy in range(3):
            acc = None
            for dx in range(3):
                part = mm(weights[dy, dx], spread[dx], dims)
                acc = part if acc is None else acc + part
            lines.append(acc)
        for y in range(rows):
            value = jnp.zeros((cout, k), F32)
            for dy in range(3):
                value = jnp.where(line == y + first + dy, lines[dy], value)
            target[y * cout : (y + 1) * cout, :] = value.astype(BF16)

    banded(w1, t1, Y1, z.c0, z.c1, z.win1, z.pad1 - 1, TN)
    banded(w2, t2, Y2, z.c1, z.c2, z.win2, 0, TN)
    for weights, target in ((w3, t3), (r1, t4), (r2, t5)):
        banded(weights, target, Y2, z.c2, z.c2, z.win2, 0, NN)

    def sides(ref, dx, low, rows):
        return jnp.concatenate(
            [ref[dx, low : low + rows, :], ref[dx + 1, low : low + rows, :]], axis=1
        )

    def pool_low(acc, n, half):
        even, odd = acc[:, :LANES], acc[:, LANES:]
        nxt = pltpu.roll(even, LANES - n, 1)
        nxt = jnp.where(iota(even.shape, 1) < (half - 1) * n, nxt, even)
        return jnp.maximum(jnp.maximum(even, odd), nxt)

    def pool_rows(blocks, c, height, before, write):
        held, done = [], 0
        for m in blocks:
            held += [m[y * c : (y + 1) * c] for y in range(m.shape[0] // c)]
            while done < -(-height // 2):
                reach = [y for y in range(2 * done - before, 2 * done - before + 3) if 0 <= y < height]
                if reach[-1] >= len(held):
                    break
                top = held[reach[0]]
                for y in reach[1:]:
                    top = jnp.maximum(top, held[y])
                write(done, top)
                done += 1

    def mix_one(s, slot):
        images = [frames[jnp.minimum(s * z.n1 + i, z.cap - 1)] for i in range(z.n1)]
        mixed = mm(jnp.concatenate(images, axis=1), p1[...]).astype(BF16)
        for q in range(4):
            g1[slot, q, PACK : PACK + z.f * z.c0, :] = mixed[:, q * LANES : (q + 1) * LANES]

    def conv_one(slot):
        def blocks():
            for b in range(z.f // Y1):
                low = b * Y1 * z.c0
                around = jnp.concatenate(
                    [sides(g1.at[slot], dx, low, z.win1 * z.c0) for dx in range(3)], axis=0
                )
                yield pool_low(mm(t1[...], around).astype(BF16), z.n1, z.w1)

        def write(y, top):
            lanes = slice(slot % 2 * LANES, (slot % 2 + 1) * LANES)
            s1[slot // 2, y * z.c1 : (y + 1) * z.c1, lanes] = jnp.maximum(top, 0)

        pool_rows(blocks(), z.c1, z.f, 0, write)

    def conv_two(half):
        mixed = mm(s1[half], p2[...]).astype(BF16)
        for q in range(4):
            g2[half, q, z.c1 : z.c1 + z.w1 * z.c1, :] = mixed[:, q * LANES : (q + 1) * LANES]

        def blocks():
            for b in range(z.w1 // Y2):
                low = b * Y2 * z.c1
                around = jnp.concatenate(
                    [sides(g2.at[half], dx, low, z.win2 * z.c1) for dx in range(3)], axis=0
                )
                yield pool_low(mm(t2[...], around).astype(BF16), z.n2, z.w2)

        def write(y, top):
            s2[y * z.c2 : (y + 1) * z.c2, half * LANES : (half + 1) * LANES] = jnp.maximum(top, 0)

        pool_rows(blocks(), z.c2, z.w1, 0, write)

    def conv_three(p):
        mixed = mm(s2[...], p3[...]).astype(BF16)
        for dx in range(3):
            g3[dx, z.c2 : z.c2 + z.w2 * z.c2, :] = mixed[:, dx * 2 * LANES : (dx + 1) * 2 * LANES]
        evens = z.n2 * z.w3

        def pool(acc):
            lane = iota(acc.shape, 1)
            same = jnp.where(lane < evens - z.n2, pltpu.roll(acc, LANES - evens, 1), acc)
            before = jnp.where(lane >= z.n2, pltpu.roll(acc, LANES - evens + z.n2, 1), acc)
            return jnp.maximum(jnp.maximum(acc, same), before)

        def blocks():
            for b in range(z.w2 // Y2):
                low = b * Y2 * z.c2
                around = jnp.concatenate([g3[dx, low : low + z.win2 * z.c2, :] for dx in range(3)], axis=0)
                acc = mm(t3[...], around).astype(BF16)
                yield jnp.concatenate([pool(acc[:, :LANES]), pool(acc[:, LANES:])], axis=1)

        def write(y, top):
            s3[p, y * z.c2 : (y + 1) * z.c2, :] = top

        pool_rows(blocks(), z.c2, z.w2, 1, write)

    def convolve(p, _):
        for half in range(2):
            for slot in (2 * half, 2 * half + 1):
                mix_one(4 * p + slot, slot)
        for half in range(2):
            for slot in (2 * half, 2 * half + 1):
                conv_one(slot)
        for half in range(2):
            conv_two(half)
        conv_three(p)
        return 0

    copies[6].wait()
    lax.fori_loop(0, pairs, convolve, 0)
    total = None
    for p in range(z.pairs):
        part = mm(s3[p], p4[p])
        total = part if total is None else total + part

    c, n = z.c2, z.w3 * z.c2
    live = iota((n, z.wide), 1) < z.w3 * z.cap

    def spread_x(ref, value):
        ref[0, c : c + n, :] = pltpu.roll(value, z.cap, 1).astype(BF16)
        ref[1, c : c + n, :] = value.astype(BF16)
        ref[2, c : c + n, :] = pltpu.roll(value, z.wide - z.cap, 1).astype(BF16)

    def residual(ref, kernel, add):
        pieces = []
        for b in range(z.blocks4):
            low = b * Y2 * c
            around = jnp.concatenate([ref[dx, low : low + z.win2 * c, :] for dx in range(3)], axis=0)
            pieces.append(mm(kernel[...], around)[: min(Y2, z.w3 - b * Y2) * c])
        value = jnp.concatenate(pieces, axis=0)
        if add is not None:
            value = value + add
        return jnp.maximum(value, 0.0)

    spread_x(x4, jnp.maximum(total, 0.0))
    inner = residual(x4, t4, None).astype(BF16).astype(F32)
    spread_x(x5, jnp.where(live, inner, 0.0))
    encoded = residual(x5, t5, total).astype(BF16).astype(F32)

    for y in range(z.w3):
        for x in range(z.w3):
            flat[pl.ds(y * z.w3 + x, c, stride=z.w3 * z.w3), :] = encoded[
                y * c : (y + 1) * c, x * z.cap : (x + 1) * z.cap
            ]
    copies[7].wait()
    features = jnp.maximum(mm(flat[...].astype(BF16), proj[...], TN), 0.0).astype(BF16)

    start = jnp.int32(0)
    for a in range(dp):
        start = start + jnp.where(a < dp_index(), counts[tensor_index(), a], 0)
    depth = z.cap // dp
    shape = (dp * tensor * depth, z.cap)
    r = iota(shape, 0)
    receiver, level = r >> log2(tensor * depth), r & (depth - 1)
    arrival = ((receiver - start) & (dp - 1)) + level * dp
    route = one_hot((iota(shape, 1) == arrival) & (arrival < own))
    out[...] = mm(route, features).astype(BF16).reshape(out.shape)


def encode_rows(frames, counts, kernels, projection):
    first, second, third, res_first, res_second = kernels
    z = Sizes(frames.shape, first.shape, second.shape, projection.shape)
    dp, tensor = lax.axis_size("dp"), lax.axis_size("tensor")
    images = jnp.transpose(frames, (0, 2, 1, 3)).reshape(z.cap, z.f * z.c0, z.f)
    ci_co, co_ci = (2, 3, 1, 0), (2, 3, 0, 1)
    n = z.w3 * z.c2
    operands = (
        counts,
        jnp.transpose(first, ci_co),
        jnp.transpose(second, ci_co),
        jnp.transpose(third, co_ci),
        jnp.transpose(res_first, co_ci),
        jnp.transpose(res_second, co_ci),
        images,
        jnp.transpose(projection),
    )
    tall = pltpu.VMEM((3, (Y2 * z.blocks4 + 2) * z.c2, z.wide), BF16)
    band = pltpu.VMEM((Y2 * z.c2, 3 * z.win2 * z.c2), BF16)
    scratch = [pltpu.SMEM(counts.shape, I32)]
    scratch += [pltpu.VMEM(x.shape, x.dtype) for x in operands[1:]]
    scratch += [
        pltpu.VMEM((z.n1 * z.f, 4 * LANES), BF16),
        pltpu.VMEM((2 * LANES, 4 * LANES), BF16),
        pltpu.VMEM((2 * LANES, 6 * LANES), BF16),
        pltpu.VMEM((Y1 * z.c1, 3 * z.win1 * z.c0), BF16),
        pltpu.VMEM((Y2 * z.c2, 3 * z.win2 * z.c1), BF16),
        band,
        band,
        band,
        pltpu.VMEM((4, 4, z.f * z.c0 + 2 * PACK, LANES), BF16),
        pltpu.VMEM((2, z.w1 * z.c1, 2 * LANES), BF16),
        pltpu.VMEM((2, 4, (z.w1 + 2) * z.c1, LANES), BF16),
        pltpu.VMEM((z.w2 * z.c2, 2 * LANES), BF16),
        pltpu.VMEM((3, (z.w2 + 2) * z.c2, 2 * LANES), BF16),
        pltpu.VMEM((z.pairs, n, 2 * LANES), BF16),
        tall,
        tall,
        pltpu.VMEM((z.pairs, 2 * LANES, z.wide), BF16),
        pltpu.VMEM((n * z.w3, z.cap), F32),
        pltpu.SemaphoreType.DMA((len(operands),)),
    ]
    body = functools.partial(
        encoder_kernel, z, dp, tensor,
        lambda: lax.axis_index("dp"), lambda: lax.axis_index("tensor"),
    )
    return pl.pallas_call(
        body,
        name="encoder",
        out_shape=jax.ShapeDtypeStruct((dp * tensor, z.cap // dp, z.feat), BF16),
        in_specs=[HBM] * len(operands),
        out_specs=VMEM,
        scratch_shapes=scratch,
        compiler_params=pltpu.CompilerParams(vmem_limit_bytes=VMEM_MOST),
        cost_estimate=pl.CostEstimate(flops=20_000_000_000, bytes_accessed=8_000_000, transcendentals=0),
    )(*operands)


def recurrent_kernel(index, dp_index, weight, bias, counts, slots, resets, *refs):
    *pieces, out, chosen, hidden = refs
    gates, share, _ = weight.shape
    tensor, dp = counts.shape
    width, places = pieces[0].shape
    for back, piece in enumerate(pieces):
        low = pl.multiple_of(((index() - back) & (tensor - 1)) * width, width)
        hidden[pl.ds(low, width), :] = piece[...]

    rows, count = chosen.shape[0], slots.shape[1]
    depth = rows // (dp * tensor)
    mine = dp_index()
    exact = lax.Precision.HIGHEST
    tallies = counts[...].astype(F32)
    before = jnp.where(iota((dp, dp), 0) < iota((dp, dp), 1), 1.0, 0.0)
    starts = mm(tallies, before, precision=exact)
    line = iota((rows, 1), 0)
    sender, group, level = line >> log2(tensor * depth), (line >> log2(depth)) & (tensor - 1), line & (depth - 1)
    by_group = jnp.where(iota((rows, tensor), 1) == group, 1.0, 0.0)
    own = iota((rows, dp), 1) == sender

    def of_row(table):
        wide = mm(by_group, table, precision=exact)
        return jnp.sum(jnp.where(own, wide, 0.0), axis=1, keepdims=True).astype(I32)

    start = of_row(starts)
    end = of_row(starts + tallies)
    rank = start + ((mine - start) & (dp - 1)) + level * dp
    balanced = group * (count // tensor) + ((rank - mine) >> log2(dp))
    to_row = one_hot((iota((rows, count), 1) == balanced) & (rank < end))
    of_slot = one_hot(iota((places, count), 0) == slots[...])
    chosen[...] = mm(to_row, of_slot, NT).astype(BF16)

    keep = 1.0 - resets[...].astype(F32)
    for q in range(gates):
        column = jnp.transpose(jnp.broadcast_to(bias[q : q + 1, :], (places, share)))
        out[q * share : (q + 1) * share, :] = mm(weight[q], hidden[...]) * keep + column


def recurrent(weight, bias, counts, slots, resets, pieces, rows):
    gates, share, hidden = weight.shape
    places = pieces[0].shape[1]
    return pl.pallas_call(
        functools.partial(recurrent_kernel, lambda: lax.axis_index("tensor"), lambda: lax.axis_index("dp")),
        name="recurrent",
        out_shape=(
            jax.ShapeDtypeStruct((gates * share, places), F32),
            jax.ShapeDtypeStruct((rows, places), BF16),
        ),
        in_specs=[VMEM] * (5 + len(pieces)),
        out_specs=(VMEM, VMEM),
        scratch_shapes=[pltpu.VMEM((hidden, places), BF16)],
        compiler_params=pltpu.CompilerParams(vmem_limit_bytes=24 << 20),
        cost_estimate=pl.CostEstimate(
            flops=2 * gates * share * hidden * places, bytes_accessed=2 * gates * share * hidden, transcendentals=0
        ),
    )(weight, bias, counts, slots, resets, *pieces)


def core_kernel(features, sums, chosen, weight, hidden, cell, heads, resets, sent, hidden_out, cell_out):
    share = hidden.shape[0]
    rows = chosen.shape[0]
    picked = chosen[...].astype(F32)
    taken = jnp.sum(picked, axis=0, keepdims=True) > 0.5
    inputs = mm(features[...].reshape(rows, -1), chosen[...], TN).astype(BF16)
    keep = 1.0 - resets[...].astype(F32)
    old_cell = cell[...]

    def gate(q):
        return mm(weight[q], inputs) + sums[q * share : (q + 1) * share, :]

    next_cell = jax.nn.sigmoid(gate(1)) * (old_cell * keep) + jax.nn.sigmoid(gate(0)) * jnp.tanh(gate(2))
    next_hidden = jax.nn.sigmoid(gate(3)) * jnp.tanh(next_cell)
    values = mm(heads[...], next_hidden.astype(BF16))
    sent[...] = mm(picked, values, NT, precision=lax.Precision.HIGHEST)
    cell_out[...] = jnp.where(taken, next_cell, old_cell)
    hidden_out[...] = jnp.where(taken, next_hidden, hidden[...])


def core(features, sums, chosen, weight, hidden, cell, heads, resets):
    share = hidden.shape[0]
    return pl.pallas_call(
        core_kernel,
        name="core",
        out_shape=(
            jax.ShapeDtypeStruct((chosen.shape[0], heads.shape[0]), F32),
            jax.ShapeDtypeStruct(hidden.shape, F32),
            jax.ShapeDtypeStruct(cell.shape, F32),
        ),
        in_specs=[VMEM] * 8,
        out_specs=(VMEM,) * 3,
        compiler_params=pltpu.CompilerParams(vmem_limit_bytes=24 << 20),
        cost_estimate=pl.CostEstimate(
            flops=8 * share * weight.shape[2] * hidden.shape[1], bytes_accessed=4_000_000, transcendentals=0
        ),
    )(features, sums, chosen, weight, hidden, cell, heads, resets)


def answers_kernel(tensor, dp_index, tensor_index, counts, received, out):
    dp = counts.shape[1]
    rows, cap = received.shape[0], out.shape[1]
    depth = cap // dp
    start = jnp.int32(0)
    for a in range(dp):
        start = start + jnp.where(a < dp_index(), counts[tensor_index(), a], 0)
    own = counts[tensor_index(), dp_index()]
    line = iota((rows, cap), 0)
    giver, level = line >> log2(tensor * depth), line & (depth - 1)
    arrival = ((giver - start) & (dp - 1)) + level * dp
    place = jnp.where((iota((rows, cap), 1) == arrival) & (arrival < own), 1.0, 0.0)
    out[...] = mm(received[...], place, TN, precision=lax.Precision.HIGHEST)


def answers(counts, received, cap):
    return pl.pallas_call(
        functools.partial(
            answers_kernel,
            counts.shape[0],
            lambda: lax.axis_index("dp"),
            lambda: lax.axis_index("tensor"),
        ),
        name="answers",
        out_shape=jax.ShapeDtypeStruct((received.shape[1], cap), F32),
        in_specs=[SMEM, VMEM],
        out_specs=VMEM,
        compiler_params=pltpu.CompilerParams(vmem_limit_bytes=8 << 20),
    )(counts, received)


def body(
    frames, counts, slot_ids, reset_flags, hidden_state, cell_state,
    conv_first, conv_second, conv_third, res_first, res_second,
    projection, input_weight, recur_weight, gate_bias, head_weight,
):
    tensor = lax.axis_size("tensor")
    own = hidden_state.astype(BF16)
    pieces = [own] + [
        lax.ppermute(own, "tensor", [(i, (i + back) % tensor) for i in range(tensor)])
        for back in range(1, tensor)
    ]
    kernels = (conv_first, conv_second, conv_third, res_first, res_second)
    features = encode_rows(frames, counts, kernels, projection)
    features, pieces = lax.optimization_barrier((features, pieces))
    features = lax.all_to_all(features, ("dp", "tensor"), 0, 0, tiled=True)
    rows = features.shape[0] * features.shape[1]
    sums, chosen = recurrent(recur_weight, gate_bias, counts, slot_ids, reset_flags, pieces, rows)
    sent, hidden_after, cell_after = core(
        features, sums, chosen, input_weight, hidden_state, cell_state, head_weight, reset_flags
    )
    received = lax.all_to_all(sent, ("dp", "tensor"), 0, 0, tiled=True)
    return answers(counts, received, frames.shape[0]), hidden_after, cell_after


def solution(mesh):
    return jax.shard_map(
        body,
        mesh=mesh,
        in_specs=(
            P(("dp", "tensor"), None, None, None),
            P(),
            P("dp", None),
            P("dp", None),
            P("tensor", "dp"),
            P("tensor", "dp"),
            P(),
            P(),
            P(),
            P(),
            P(),
            P(),
            P(None, "tensor", None),
            P(None, "tensor", None),
            P(None, "tensor"),
            P(None, "tensor"),
        ),
        out_specs=(P(None, ("dp", "tensor")), P("tensor", "dp"), P("tensor", "dp")),
        check_vma=False,
    )
```

```python
import functools

import jax
import jax.numpy as jnp
from jax import lax
from jax.experimental import pallas as pl
from jax.experimental.pallas import tpu as pltpu
from jax.sharding import PartitionSpec as P

F32, BF16, I32 = jnp.float32, jnp.bfloat16, jnp.int32
LANES = 128
PACK = 16
Y1, Y2 = 12, 3
NN = (((1,), (0,)), ((), ()))
NT = (((1,), (1,)), ((), ()))
TN = (((0,), (0,)), ((), ()))
VMEM = pl.BlockSpec(memory_space=pltpu.VMEM)
SMEM = pl.BlockSpec(memory_space=pltpu.SMEM)
HBM = pl.BlockSpec(memory_space=pltpu.HBM)


def mm(a, b, dims=NN, precision=None):
    return lax.dot_general(a, b, dims, precision=precision, preferred_element_type=F32)


def iota(shape, axis):
    return lax.broadcasted_iota(I32, shape, axis)


def log2(n):
    assert n & (n - 1) == 0
    return n.bit_length() - 1


def divide(v, n, limit):
    scale = -(-(1 << 16) // n)
    assert all((k * scale) >> 16 == k // n for k in range(limit))
    return (v * scale) >> 16


def one_hot(mask):
    return jnp.where(mask, 1.0, 0.0).astype(BF16)


class Sizes:
    def __init__(self, frames, first, second, projection):
        self.cap, self.c0, self.f, _ = frames
        self.c1, self.c2, self.feat = first[0], second[0], projection[0]
        self.w1 = -(-self.f // 2)
        self.w2 = -(-self.w1 // 2)
        self.w3 = -(-self.w2 // 2)
        self.n1 = LANES // self.w1
        self.n2 = 2 * self.n1
        self.n3 = 2 * self.n2
        assert self.f % 4 == 0 and self.w2 % 2 == 1 and self.n2 * self.w2 <= LANES
        assert self.f % Y1 == 0 and self.w1 % Y2 == 0 and self.w2 % Y2 == 0
        self.pad1 = PACK // self.c0
        self.win1 = Y1 + 2 * self.pad1
        self.win2 = Y2 + 2
        self.pairs = -(-self.cap // self.n3)
        self.blocks4 = -(-self.w3 // Y2)
        self.wide = -(-self.w3 * self.cap // LANES) * LANES
        assert self.wide - self.w3 * self.cap >= self.cap


def encoder_kernel(z, dp, tensor, dp_index, tensor_index, *refs):
    far, out, near = refs[:8], refs[8], refs[9:17]
    p1, p2, p3, t1, t2, t3, t4, t5, g1, s1, g2, s2, g3, s3, x4, x5, p4, flat, sems = refs[17:]
    counts, w1, w2, w3, r1, r2, frames, proj = near
    copies = [pltpu.make_async_copy(a, b, sems.at[i]) for i, (a, b) in enumerate(zip(far, near))]
    for copy in copies:
        copy.start()

    def place(ref, x, width, live, where):
        where = jnp.where(live & (x >= 0) & (x < width), where, -1)
        ref[...] = one_hot(iota(ref.shape, 0) == where)

    def split(columns, n):
        v = iota((1, columns), 1)
        lane = v & (LANES - 1)
        j = divide(lane, n, LANES)
        return v >> log2(LANES), lane, j, lane - j * n

    quarter, _, j, i = split(4 * LANES, z.n1)
    x = 2 * j + quarter - 1
    place(p1, x, z.f, j < z.w1, i * z.f + x)
    quarter, _, j, i = split(4 * LANES, z.n2)
    x = 2 * j + quarter - 1
    upper = (i >= z.n1).astype(I32)
    place(p2, x, z.w1, j < z.w2, upper * (LANES - z.n1) + x * z.n1 + i)
    part, lane, j, i = split(6 * LANES, z.n2)
    odd = (lane >= z.n2 * z.w3).astype(I32)
    x = 2 * (j - odd * z.w3) + odd + (part >> 1) - 1
    place(p3, x, z.w2, lane < z.n2 * z.w2, (part & 1) * LANES + x * z.n2 + i)
    v = iota((1, z.wide), 1)
    for pair in range(z.pairs):
        x, i = v >> log2(z.cap), (v & (z.cap - 1)) - pair * z.n3
        upper = (i >= z.n2).astype(I32)
        place(p4.at[pair], x, z.w3, (i >= 0) & (i < z.n3), upper * (LANES - z.n2) + x * z.n2 + i)

    maps = [(g1.at[i], PACK, z.f * z.c0) for i in range(4)]
    maps += [(g2.at[i], z.c1, z.w1 * z.c1) for i in range(2)]
    for ref, top, rows in maps + [(g3, z.c2, z.w2 * z.c2)]:
        for q in range(ref.shape[0]):
            ref[q, :top] = jnp.zeros((top, ref.shape[2]), BF16)
            low = ref.shape[1] - top - rows
            ref[q, top + rows :] = jnp.zeros((low, ref.shape[2]), BF16)
    for ref in (x4, x5):
        for q in range(3):
            ref[q, : z.c2] = jnp.zeros((z.c2, z.wide), BF16)
            low = ref.shape[1] - z.c2 - z.w3 * z.c2
            ref[q, z.c2 + z.w3 * z.c2 :] = jnp.zeros((low, z.wide), BF16)
    for copy in copies[:6]:
        copy.wait()
    own = counts[tensor_index(), dp_index()]
    pairs = lax.div(own + (z.n3 - 1), z.n3)
    s3[...] = jnp.zeros(s3.shape, BF16)

    def banded(weights, target, rows, cin, cout, window, first, dims):
        k = 3 * window * cin
        v = iota((1, k), 1)
        channel, line = v & (cin - 1), v >> log2(cin)
        which = divide(line, window, 3 * window)
        line = line - which * window
        spread = [one_hot((iota((cin, k), 0) == channel) & (which == dx)) for dx in range(3)]
        lines = []
        for dy in range(3):
            acc = None
            for dx in range(3):
                part = mm(weights[dy, dx], spread[dx], dims)
                acc = part if acc is None else acc + part
            lines.append(acc)
        for y in range(rows):
            value = jnp.zeros((cout, k), F32)
            for dy in range(3):
                value = jnp.where(line == y + first + dy, lines[dy], value)
            target[y * cout : (y + 1) * cout, :] = value.astype(BF16)

    banded(w1, t1, Y1, z.c0, z.c1, z.win1, z.pad1 - 1, TN)
    banded(w2, t2, Y2, z.c1, z.c2, z.win2, 0, TN)
    for weights, target in ((w3, t3), (r1, t4), (r2, t5)):
        banded(weights, target, Y2, z.c2, z.c2, z.win2, 0, NN)

    def sides(ref, dx, low, rows):
        return jnp.concatenate(
            [ref[dx, low : low + rows, :], ref[dx + 1, low : low + rows, :]], axis=1
        )

    def pool_low(acc, n, half):
        even, odd = acc[:, :LANES], acc[:, LANES:]
        nxt = pltpu.roll(even, LANES - n, 1)
        nxt = jnp.where(iota(even.shape, 1) < (half - 1) * n, nxt, even)
        return jnp.maximum(jnp.maximum(even, odd), nxt)

    def pool_rows(blocks, c, height, before, write):
        held, done = [], 0
        for m in blocks:
            held += [m[y * c : (y + 1) * c] for y in range(m.shape[0] // c)]
            while done < -(-height // 2):
                reach = [y for y in range(2 * done - before, 2 * done - before + 3) if 0 <= y < height]
                if reach[-1] >= len(held):
                    break
                top = held[reach[0]]
                for y in reach[1:]:
                    top = jnp.maximum(top, held[y])
                write(done, top)
                done += 1

    def mix_one(s, slot):
        images = [frames[jnp.minimum(s * z.n1 + i, z.cap - 1)] for i in range(z.n1)]
        mixed = mm(jnp.concatenate(images, axis=1), p1[...]).astype(BF16)
        for q in range(4):
            g1[slot, q, PACK : PACK + z.f * z.c0, :] = mixed[:, q * LANES : (q + 1) * LANES]

    def conv_one(slot):
        def blocks():
            for b in range(z.f // Y1):
                low = b * Y1 * z.c0
                around = jnp.concatenate(
                    [sides(g1.at[slot], dx, low, z.win1 * z.c0) for dx in range(3)], axis=0
                )
                yield pool_low(mm(t1[...], around).astype(BF16), z.n1, z.w1)

        def write(y, top):
            lanes = slice(slot % 2 * LANES, (slot % 2 + 1) * LANES)
            s1[slot // 2, y * z.c1 : (y + 1) * z.c1, lanes] = jnp.maximum(top, 0)

        pool_rows(blocks(), z.c1, z.f, 0, write)

    def conv_two(half):
        mixed = mm(s1[half], p2[...]).astype(BF16)
        for q in range(4):
            g2[half, q, z.c1 : z.c1 + z.w1 * z.c1, :] = mixed[:, q * LANES : (q + 1) * LANES]

        def blocks():
            for b in range(z.w1 // Y2):
                low = b * Y2 * z.c1
                around = jnp.concatenate(
                    [sides(g2.at[half], dx, low, z.win2 * z.c1) for dx in range(3)], axis=0
                )
                yield pool_low(mm(t2[...], around).astype(BF16), z.n2, z.w2)

        def write(y, top):
            s2[y * z.c2 : (y + 1) * z.c2, half * LANES : (half + 1) * LANES] = jnp.maximum(top, 0)

        pool_rows(blocks(), z.c2, z.w1, 0, write)

    def conv_three(p):
        mixed = mm(s2[...], p3[...]).astype(BF16)
        for dx in range(3):
            g3[dx, z.c2 : z.c2 + z.w2 * z.c2, :] = mixed[:, dx * 2 * LANES : (dx + 1) * 2 * LANES]
        evens = z.n2 * z.w3

        def pool(acc):
            lane = iota(acc.shape, 1)
            same = jnp.where(lane < evens - z.n2, pltpu.roll(acc, LANES - evens, 1), acc)
            before = jnp.where(lane >= z.n2, pltpu.roll(acc, LANES - evens + z.n2, 1), acc)
            return jnp.maximum(jnp.maximum(acc, same), before)

        def blocks():
            for b in range(z.w2 // Y2):
                low = b * Y2 * z.c2
                around = jnp.concatenate([g3[dx, low : low + z.win2 * z.c2, :] for dx in range(3)], axis=0)
                acc = mm(t3[...], around).astype(BF16)
                yield jnp.concatenate([pool(acc[:, :LANES]), pool(acc[:, LANES:])], axis=1)

        def write(y, top):
            s3[p, y * z.c2 : (y + 1) * z.c2, :] = top

        pool_rows(blocks(), z.c2, z.w2, 1, write)

    def convolve(p, _):
        for half in range(2):
            for slot in (2 * half, 2 * half + 1):
                mix_one(4 * p + slot, slot)
        for half in range(2):
            for slot in (2 * half, 2 * half + 1):
                conv_one(slot)
        for half in range(2):
            conv_two(half)
        conv_three(p)
        return 0

    copies[6].wait()
    lax.fori_loop(0, pairs, convolve, 0)
    total = None
    for p in range(z.pairs):
        part = mm(s3[p], p4[p])
        total = part if total is None else total + part

    c, n = z.c2, z.w3 * z.c2
    live = iota((n, z.wide), 1) < z.w3 * z.cap

    def spread_x(ref, value):
        ref[0, c : c + n, :] = pltpu.roll(value, z.cap, 1).astype(BF16)
        ref[1, c : c + n, :] = value.astype(BF16)
        ref[2, c : c + n, :] = pltpu.roll(value, z.wide - z.cap, 1).astype(BF16)

    def residual(ref, kernel, add):
        pieces = []
        for b in range(z.blocks4):
            low = b * Y2 * c
            around = jnp.concatenate([ref[dx, low : low + z.win2 * c, :] for dx in range(3)], axis=0)
            pieces.append(mm(kernel[...], around)[: min(Y2, z.w3 - b * Y2) * c])
        value = jnp.concatenate(pieces, axis=0)
        if add is not None:
            value = value + add
        return jnp.maximum(value, 0.0)

    spread_x(x4, jnp.maximum(total, 0.0))
    inner = residual(x4, t4, None).astype(BF16).astype(F32)
    spread_x(x5, jnp.where(live, inner, 0.0))
    encoded = residual(x5, t5, total).astype(BF16).astype(F32)

    for y in range(z.w3):
        for x in range(z.w3):
            flat[pl.ds(y * z.w3 + x, c, stride=z.w3 * z.w3), :] = encoded[
                y * c : (y + 1) * c, x * z.cap : (x + 1) * z.cap
            ]
    copies[7].wait()
    features = jnp.maximum(mm(flat[...].astype(BF16), proj[...], TN), 0.0).astype(BF16)

    start = jnp.int32(0)
    for a in range(dp):
        start = start + jnp.where(a < dp_index(), counts[tensor_index(), a], 0)
    depth = z.cap // dp
    shape = (dp * tensor * depth, z.cap)
    r = iota(shape, 0)
    receiver, level = r >> log2(tensor * depth), r & (depth - 1)
    arrival = ((receiver - start) & (dp - 1)) + level * dp
    route = one_hot((iota(shape, 1) == arrival) & (arrival < own))
    out[...] = mm(route, features).astype(BF16).reshape(out.shape)


def encode_rows(frames, counts, kernels, projection):
    first, second, third, res_first, res_second = kernels
    z = Sizes(frames.shape, first.shape, second.shape, projection.shape)
    dp, tensor = lax.axis_size("dp"), lax.axis_size("tensor")
    images = jnp.transpose(frames, (0, 2, 1, 3)).reshape(z.cap, z.f * z.c0, z.f)
    ci_co, co_ci = (2, 3, 1, 0), (2, 3, 0, 1)
    n = z.w3 * z.c2
    operands = (
        counts,
        jnp.transpose(first, ci_co),
        jnp.transpose(second, ci_co),
        jnp.transpose(third, co_ci),
        jnp.transpose(res_first, co_ci),
        jnp.transpose(res_second, co_ci),
        images,
        jnp.transpose(projection),
    )
    tall = pltpu.VMEM((3, (Y2 * z.blocks4 + 2) * z.c2, z.wide), BF16)
    band = pltpu.VMEM((Y2 * z.c2, 3 * z.win2 * z.c2), BF16)
    scratch = [pltpu.SMEM(counts.shape, I32)]
    scratch += [pltpu.VMEM(x.shape, x.dtype) for x in operands[1:]]
    scratch += [
        pltpu.VMEM((z.n1 * z.f, 4 * LANES), BF16),
        pltpu.VMEM((2 * LANES, 4 * LANES), BF16),
        pltpu.VMEM((2 * LANES, 6 * LANES), BF16),
        pltpu.VMEM((Y1 * z.c1, 3 * z.win1 * z.c0), BF16),
        pltpu.VMEM((Y2 * z.c2, 3 * z.win2 * z.c1), BF16),
        band,
        band,
        band,
        pltpu.VMEM((4, 4, z.f * z.c0 + 2 * PACK, LANES), BF16),
        pltpu.VMEM((2, z.w1 * z.c1, 2 * LANES), BF16),
        pltpu.VMEM((2, 4, (z.w1 + 2) * z.c1, LANES), BF16),
        pltpu.VMEM((z.w2 * z.c2, 2 * LANES), BF16),
        pltpu.VMEM((3, (z.w2 + 2) * z.c2, 2 * LANES), BF16),
        pltpu.VMEM((z.pairs, n, 2 * LANES), BF16),
        tall,
        tall,
        pltpu.VMEM((z.pairs, 2 * LANES, z.wide), BF16),
        pltpu.VMEM((n * z.w3, z.cap), F32),
        pltpu.SemaphoreType.DMA((len(operands),)),
    ]
    body = functools.partial(
        encoder_kernel, z, dp, tensor,
        lambda: lax.axis_index("dp"), lambda: lax.axis_index("tensor"),
    )
    return pl.pallas_call(
        body,
        name="encoder",
        out_shape=jax.ShapeDtypeStruct((dp * tensor, z.cap // dp, z.feat), BF16),
        in_specs=[HBM] * len(operands),
        out_specs=VMEM,
        scratch_shapes=scratch,
        compiler_params=pltpu.CompilerParams(vmem_limit_bytes=40 << 20),
        cost_estimate=pl.CostEstimate(flops=20_000_000_000, bytes_accessed=8_000_000, transcendentals=0),
    )(*[pltpu.with_memory_space_constraint(x, pltpu.HBM) for x in operands])


def recurrent_kernel(index, dp_index, weight, bias, counts, slots, resets, *refs):
    *pieces, out, chosen, hidden, held, sems = refs
    gates, share, _ = weight.shape
    slot_count, tall, _ = held.shape
    chunks = gates * share // tall

    def copy(i):
        q, low = divmod(i * tall, share)
        slot = i % slot_count
        return pltpu.make_async_copy(weight.at[q, pl.ds(low, tall)], held.at[slot], sems.at[slot])

    for i in range(slot_count - 1):
        copy(i).start()
    tensor, dp = counts.shape
    width, places = pieces[0].shape
    for back, piece in enumerate(pieces):
        low = pl.multiple_of(((index() - back) & (tensor - 1)) * width, width)
        hidden[pl.ds(low, width), :] = piece[...]

    rows, count = chosen.shape[0], slots.shape[1]
    depth = rows // (dp * tensor)
    mine = dp_index()
    exact = lax.Precision.HIGHEST
    tallies = counts[...].astype(F32)
    before = jnp.where(iota((dp, dp), 0) < iota((dp, dp), 1), 1.0, 0.0)
    starts = mm(tallies, before, precision=exact)
    line = iota((rows, 1), 0)
    sender, group, level = line >> log2(tensor * depth), (line >> log2(depth)) & (tensor - 1), line & (depth - 1)
    by_group = jnp.where(iota((rows, tensor), 1) == group, 1.0, 0.0)
    own = iota((rows, dp), 1) == sender

    def of_row(table):
        wide = mm(by_group, table, precision=exact)
        return jnp.sum(jnp.where(own, wide, 0.0), axis=1, keepdims=True).astype(I32)

    start = of_row(starts)
    end = of_row(starts + tallies)
    rank = start + ((mine - start) & (dp - 1)) + level * dp
    balanced = group * (count // tensor) + ((rank - mine) >> log2(dp))
    to_row = one_hot((iota((rows, count), 1) == balanced) & (rank < end))
    of_slot = one_hot(iota((places, count), 0) == slots[...])
    chosen[...] = mm(to_row, of_slot, NT).astype(BF16)

    keep = 1.0 - resets[...].astype(F32)
    for i in range(chunks):
        q, low = divmod(i * tall, share)
        column = jnp.transpose(jnp.broadcast_to(bias[q : q + 1, low : low + tall], (places, tall)))
        copy(i).wait()
        if i + slot_count - 1 < chunks:
            copy(i + slot_count - 1).start()
        out[i * tall : (i + 1) * tall, :] = mm(held[i % slot_count], hidden[...]) * keep + column


def recurrent(weight, bias, counts, slots, resets, pieces, rows):
    gates, share, hidden = weight.shape
    places = pieces[0].shape[1]
    return pl.pallas_call(
        functools.partial(recurrent_kernel, lambda: lax.axis_index("tensor"), lambda: lax.axis_index("dp")),
        name="recurrent",
        out_shape=(
            jax.ShapeDtypeStruct((gates * share, places), F32),
            jax.ShapeDtypeStruct((rows, places), BF16),
        ),
        in_specs=[HBM] + [VMEM] * (4 + len(pieces)),
        out_specs=(VMEM, VMEM),
        scratch_shapes=[
            pltpu.VMEM((hidden, places), BF16),
            pltpu.VMEM((4, share // 2, hidden), BF16),
            pltpu.SemaphoreType.DMA((4,)),
        ],
        compiler_params=pltpu.CompilerParams(vmem_limit_bytes=24 << 20),
        cost_estimate=pl.CostEstimate(
            flops=2 * gates * share * hidden * places, bytes_accessed=2 * gates * share * hidden, transcendentals=0
        ),
    )(pltpu.with_memory_space_constraint(weight, pltpu.HBM), bias, counts, slots, resets, *pieces)


def core_kernel(features, sums, chosen, weight, hidden, cell, heads, resets, sent, hidden_out, cell_out):
    share = hidden.shape[0]
    rows = chosen.shape[0]
    picked = chosen[...].astype(F32)
    taken = jnp.sum(picked, axis=0, keepdims=True) > 0.5
    inputs = mm(features[...].reshape(rows, -1), chosen[...], TN).astype(BF16)
    keep = 1.0 - resets[...].astype(F32)
    old_cell = cell[...]

    def gate(q):
        return mm(weight[q], inputs) + sums[q * share : (q + 1) * share, :]

    next_cell = jax.nn.sigmoid(gate(1)) * (old_cell * keep) + jax.nn.sigmoid(gate(0)) * jnp.tanh(gate(2))
    next_hidden = jax.nn.sigmoid(gate(3)) * jnp.tanh(next_cell)
    values = mm(heads[...], next_hidden.astype(BF16))
    sent[...] = mm(picked, values, NT, precision=lax.Precision.HIGHEST)
    cell_out[...] = jnp.where(taken, next_cell, old_cell)
    hidden_out[...] = jnp.where(taken, next_hidden, hidden[...])


def core(features, sums, chosen, weight, hidden, cell, heads, resets):
    share = hidden.shape[0]
    return pl.pallas_call(
        core_kernel,
        name="core",
        out_shape=(
            jax.ShapeDtypeStruct((chosen.shape[0], heads.shape[0]), F32),
            jax.ShapeDtypeStruct(hidden.shape, F32),
            jax.ShapeDtypeStruct(cell.shape, F32),
        ),
        in_specs=[VMEM] * 8,
        out_specs=(VMEM,) * 3,
        compiler_params=pltpu.CompilerParams(vmem_limit_bytes=24 << 20),
        cost_estimate=pl.CostEstimate(
            flops=8 * share * weight.shape[2] * hidden.shape[1], bytes_accessed=4_000_000, transcendentals=0
        ),
    )(features, sums, chosen, weight, hidden, cell, heads, resets)


def answers_kernel(tensor, dp_index, tensor_index, counts, received, out):
    dp = counts.shape[1]
    rows, cap = received.shape[0], out.shape[1]
    depth = cap // dp
    start = jnp.int32(0)
    for a in range(dp):
        start = start + jnp.where(a < dp_index(), counts[tensor_index(), a], 0)
    own = counts[tensor_index(), dp_index()]
    line = iota((rows, cap), 0)
    giver, level = line >> log2(tensor * depth), line & (depth - 1)
    arrival = ((giver - start) & (dp - 1)) + level * dp
    place = jnp.where((iota((rows, cap), 1) == arrival) & (arrival < own), 1.0, 0.0)
    out[...] = mm(received[...], place, TN, precision=lax.Precision.HIGHEST)


def answers(counts, received, cap):
    return pl.pallas_call(
        functools.partial(
            answers_kernel,
            counts.shape[0],
            lambda: lax.axis_index("dp"),
            lambda: lax.axis_index("tensor"),
        ),
        name="answers",
        out_shape=jax.ShapeDtypeStruct((received.shape[1], cap), F32),
        in_specs=[SMEM, VMEM],
        out_specs=VMEM,
        compiler_params=pltpu.CompilerParams(vmem_limit_bytes=8 << 20),
    )(counts, received)


def body(
    frames, counts, slot_ids, reset_flags, hidden_state, cell_state,
    conv_first, conv_second, conv_third, res_first, res_second,
    projection, input_weight, recur_weight, gate_bias, head_weight,
):
    tensor = lax.axis_size("tensor")
    own = hidden_state.astype(BF16)
    pieces = [own] + [
        lax.ppermute(own, "tensor", [(i, (i + back) % tensor) for i in range(tensor)])
        for back in range(1, tensor)
    ]
    kernels = (conv_first, conv_second, conv_third, res_first, res_second)
    features = encode_rows(frames, counts, kernels, projection)
    features, pieces = lax.optimization_barrier((features, pieces))
    features = lax.all_to_all(features, ("dp", "tensor"), 0, 0, tiled=True)
    rows = features.shape[0] * features.shape[1]
    sums, chosen = recurrent(recur_weight, gate_bias, counts, slot_ids, reset_flags, pieces, rows)
    sent, hidden_after, cell_after = core(
        features, sums, chosen, input_weight, hidden_state, cell_state, head_weight, reset_flags
    )
    received = lax.all_to_all(sent, ("dp", "tensor"), 0, 0, tiled=True)
    return answers(counts, received, frames.shape[0]), hidden_after, cell_after


def solution(mesh):
    return jax.shard_map(
        body,
        mesh=mesh,
        in_specs=(
            P(("dp", "tensor"), None, None, None),
            P(),
            P("dp", None),
            P("dp", None),
            P("tensor", "dp"),
            P("tensor", "dp"),
            P(),
            P(),
            P(),
            P(),
            P(),
            P(),
            P(None, "tensor", None),
            P(None, "tensor", None),
            P(None, "tensor"),
            P(None, "tensor"),
        ),
        out_specs=(P(None, ("dp", "tensor")), P("tensor", "dp"), P("tensor", "dp")),
        check_vma=False,
    )
```

```python
import functools

import jax
import jax.numpy as jnp
from jax import lax
from jax.experimental import pallas as pl
from jax.experimental.pallas import tpu as pltpu
from jax.sharding import PartitionSpec as P

F32, BF16, I32 = jnp.float32, jnp.bfloat16, jnp.int32
LANES = 128
PACK = 16
Y1, Y2 = 12, 3
NN = (((1,), (0,)), ((), ()))
NT = (((1,), (1,)), ((), ()))
TN = (((0,), (0,)), ((), ()))
VMEM = pl.BlockSpec(memory_space=pltpu.VMEM)
HBM = pl.BlockSpec(memory_space=pltpu.HBM)


def mm(a, b, dims=NN, precision=None):
    return lax.dot_general(a, b, dims, precision=precision, preferred_element_type=F32)


def iota(shape, axis):
    return lax.broadcasted_iota(I32, shape, axis)


def log2(n):
    assert n & (n - 1) == 0
    return n.bit_length() - 1


def divide(v, n, limit):
    scale = -(-(1 << 16) // n)
    assert all((k * scale) >> 16 == k // n for k in range(limit))
    return (v * scale) >> 16


def one_hot(mask):
    return jnp.where(mask, 1.0, 0.0).astype(BF16)


class Sizes:
    def __init__(self, frames, first, second, projection):
        self.cap, self.c0, self.f, _ = frames
        self.c1, self.c2, self.feat = first[0], second[0], projection[0]
        self.w1 = -(-self.f // 2)
        self.w2 = -(-self.w1 // 2)
        self.w3 = -(-self.w2 // 2)
        self.n1 = LANES // self.w1
        self.n2 = 2 * self.n1
        self.n3 = 2 * self.n2
        assert self.f % 4 == 0 and self.w2 % 2 == 1 and self.n2 * self.w2 <= LANES
        assert self.f % Y1 == 0 and self.w1 % Y2 == 0 and self.w2 % Y2 == 0
        self.pad1 = PACK // self.c0
        self.win1 = Y1 + 2 * self.pad1
        self.win2 = Y2 + 2
        self.pairs = -(-self.cap // self.n3)
        self.blocks4 = -(-self.w3 // Y2)
        self.wide = -(-self.w3 * self.cap // LANES) * LANES
        assert self.wide - self.w3 * self.cap >= self.cap


def encoder_kernel(z, dp, tensor, dp_index, tensor_index, *refs):
    far, out, near = refs[:8], refs[8], refs[9:17]
    p1, p2, p3, t1, t2, t3, t4, t5, g1, s1, g2, s2, g3, s3, x4, x5, p4, flat, sems = refs[17:]
    counts, w1, w2, w3, r1, r2, frames, proj = near
    pairs = list(zip(far, near))
    first = [pltpu.make_async_copy(a, b, sems.at[i]) for i, (a, b) in enumerate(pairs[:6])]
    arriving = []
    for low in range(0, z.cap, z.n3):
        part = pl.ds(low, min(z.n3, z.cap - low))
        sem = sems.at[len(first) + len(arriving)]
        arriving.append(pltpu.make_async_copy(far[6].at[part], frames.at[part], sem))
    final = pltpu.make_async_copy(far[7], proj, sems.at[len(first) + len(arriving)])
    for copy in first + arriving + [final]:
        copy.start()

    def place(ref, x, width, live, where):
        where = jnp.where(live & (x >= 0) & (x < width), where, -1)
        ref[...] = one_hot(iota(ref.shape, 0) == where)

    def split(columns, n):
        v = iota((1, columns), 1)
        lane = v & (LANES - 1)
        j = divide(lane, n, LANES)
        return v >> log2(LANES), lane, j, lane - j * n

    quarter, _, j, i = split(4 * LANES, z.n1)
    x = 2 * j + quarter - 1
    place(p1, x, z.f, j < z.w1, i * z.f + x)
    quarter, _, j, i = split(4 * LANES, z.n2)
    x = 2 * j + quarter - 1
    upper = (i >= z.n1).astype(I32)
    place(p2, x, z.w1, j < z.w2, upper * (LANES - z.n1) + x * z.n1 + i)
    part, lane, j, i = split(6 * LANES, z.n2)
    odd = (lane >= z.n2 * z.w3).astype(I32)
    x = 2 * (j - odd * z.w3) + odd + (part >> 1) - 1
    place(p3, x, z.w2, lane < z.n2 * z.w2, (part & 1) * LANES + x * z.n2 + i)
    v = iota((1, z.wide), 1)
    for pair in range(z.pairs):
        x, i = v >> log2(z.cap), (v & (z.cap - 1)) - pair * z.n3
        upper = (i >= z.n2).astype(I32)
        place(p4.at[pair], x, z.w3, (i >= 0) & (i < z.n3), upper * (LANES - z.n2) + x * z.n2 + i)

    maps = [(g1.at[i], PACK, z.f * z.c0) for i in range(4)]
    maps += [(g2.at[i], z.c1, z.w1 * z.c1) for i in range(2)]
    for ref, top, rows in maps + [(g3, z.c2, z.w2 * z.c2)]:
        for q in range(ref.shape[0]):
            ref[q, :top] = jnp.zeros((top, ref.shape[2]), BF16)
            low = ref.shape[1] - top - rows
            ref[q, top + rows :] = jnp.zeros((low, ref.shape[2]), BF16)
    for ref in (x4, x5):
        for q in range(3):
            ref[q, : z.c2] = jnp.zeros((z.c2, z.wide), BF16)
            low = ref.shape[1] - z.c2 - z.w3 * z.c2
            ref[q, z.c2 + z.w3 * z.c2 :] = jnp.zeros((low, z.wide), BF16)
    for copy in first:
        copy.wait()
    own = counts[tensor_index(), dp_index()]
    steps = lax.div(own + (z.n3 - 1), z.n3)
    s3[...] = jnp.zeros(s3.shape, BF16)

    def banded(weights, target, rows, cin, cout, window, first, dims):
        k = 3 * window * cin
        v = iota((1, k), 1)
        channel, line = v & (cin - 1), v >> log2(cin)
        which = divide(line, window, 3 * window)
        line = line - which * window
        spread = [one_hot((iota((cin, k), 0) == channel) & (which == dx)) for dx in range(3)]
        lines = []
        for dy in range(3):
            acc = None
            for dx in range(3):
                part = mm(weights[dy, dx], spread[dx], dims)
                acc = part if acc is None else acc + part
            lines.append(acc)
        for y in range(rows):
            value = jnp.zeros((cout, k), F32)
            for dy in range(3):
                value = jnp.where(line == y + first + dy, lines[dy], value)
            target[y * cout : (y + 1) * cout, :] = value.astype(BF16)

    banded(w1, t1, Y1, z.c0, z.c1, z.win1, z.pad1 - 1, TN)
    banded(w2, t2, Y2, z.c1, z.c2, z.win2, 0, TN)
    for weights, target in ((w3, t3), (r1, t4), (r2, t5)):
        banded(weights, target, Y2, z.c2, z.c2, z.win2, 0, NN)

    def sides(ref, dx, low, rows):
        return jnp.concatenate(
            [ref[dx, low : low + rows, :], ref[dx + 1, low : low + rows, :]], axis=1
        )

    def pool_low(acc, n, half):
        even, odd = acc[:, :LANES], acc[:, LANES:]
        nxt = pltpu.roll(even, LANES - n, 1)
        nxt = jnp.where(iota(even.shape, 1) < (half - 1) * n, nxt, even)
        return jnp.maximum(jnp.maximum(even, odd), nxt)

    def pool_rows(blocks, c, height, before, write):
        held, done = [], 0
        for m in blocks:
            held += [m[y * c : (y + 1) * c] for y in range(m.shape[0] // c)]
            while done < -(-height // 2):
                reach = [y for y in range(2 * done - before, 2 * done - before + 3) if 0 <= y < height]
                if reach[-1] >= len(held):
                    break
                top = held[reach[0]]
                for y in reach[1:]:
                    top = jnp.maximum(top, held[y])
                write(done, top)
                done += 1

    def mix_one(s, slot):
        images = [frames[jnp.minimum(s * z.n1 + i, z.cap - 1)] for i in range(z.n1)]
        mixed = mm(jnp.concatenate(images, axis=1), p1[...]).astype(BF16)
        for q in range(4):
            g1[slot, q, PACK : PACK + z.f * z.c0, :] = mixed[:, q * LANES : (q + 1) * LANES]

    def conv_one(slot):
        def blocks():
            for b in range(z.f // Y1):
                low = b * Y1 * z.c0
                around = jnp.concatenate(
                    [sides(g1.at[slot], dx, low, z.win1 * z.c0) for dx in range(3)], axis=0
                )
                yield pool_low(mm(t1[...], around).astype(BF16), z.n1, z.w1)

        def write(y, top):
            lanes = slice(slot % 2 * LANES, (slot % 2 + 1) * LANES)
            s1[slot // 2, y * z.c1 : (y + 1) * z.c1, lanes] = jnp.maximum(top, 0)

        pool_rows(blocks(), z.c1, z.f, 0, write)

    def conv_two(half):
        mixed = mm(s1[half], p2[...]).astype(BF16)
        for q in range(4):
            g2[half, q, z.c1 : z.c1 + z.w1 * z.c1, :] = mixed[:, q * LANES : (q + 1) * LANES]

        def blocks():
            for b in range(z.w1 // Y2):
                low = b * Y2 * z.c1
                around = jnp.concatenate(
                    [sides(g2.at[half], dx, low, z.win2 * z.c1) for dx in range(3)], axis=0
                )
                yield pool_low(mm(t2[...], around).astype(BF16), z.n2, z.w2)

        def write(y, top):
            s2[y * z.c2 : (y + 1) * z.c2, half * LANES : (half + 1) * LANES] = jnp.maximum(top, 0)

        pool_rows(blocks(), z.c2, z.w1, 0, write)

    def conv_three(p):
        mixed = mm(s2[...], p3[...]).astype(BF16)
        for dx in range(3):
            g3[dx, z.c2 : z.c2 + z.w2 * z.c2, :] = mixed[:, dx * 2 * LANES : (dx + 1) * 2 * LANES]
        evens = z.n2 * z.w3

        def pool(acc):
            lane = iota(acc.shape, 1)
            same = jnp.where(lane < evens - z.n2, pltpu.roll(acc, LANES - evens, 1), acc)
            before = jnp.where(lane >= z.n2, pltpu.roll(acc, LANES - evens + z.n2, 1), acc)
            return jnp.maximum(jnp.maximum(acc, same), before)

        def blocks():
            for b in range(z.w2 // Y2):
                low = b * Y2 * z.c2
                around = jnp.concatenate([g3[dx, low : low + z.win2 * z.c2, :] for dx in range(3)], axis=0)
                acc = mm(t3[...], around).astype(BF16)
                yield jnp.concatenate([pool(acc[:, :LANES]), pool(acc[:, LANES:])], axis=1)

        def write(y, top):
            s3[p, y * z.c2 : (y + 1) * z.c2, :] = top

        pool_rows(blocks(), z.c2, z.w2, 1, write)

    def convolve(p, _):
        for k, copy in enumerate(arriving):
            pl.when(p == k)(copy.wait)
        for half in range(2):
            for slot in (2 * half, 2 * half + 1):
                mix_one(4 * p + slot, slot)
        for half in range(2):
            for slot in (2 * half, 2 * half + 1):
                conv_one(slot)
        for half in range(2):
            conv_two(half)
        conv_three(p)
        return 0

    lax.fori_loop(0, steps, convolve, 0)
    for k, copy in enumerate(arriving):
        pl.when(k >= steps)(copy.wait)
    total = None
    for p in range(z.pairs):
        part = mm(s3[p], p4[p])
        total = part if total is None else total + part

    c, n = z.c2, z.w3 * z.c2
    live = iota((n, z.wide), 1) < z.w3 * z.cap

    def spread_x(ref, value):
        ref[0, c : c + n, :] = pltpu.roll(value, z.cap, 1).astype(BF16)
        ref[1, c : c + n, :] = value.astype(BF16)
        ref[2, c : c + n, :] = pltpu.roll(value, z.wide - z.cap, 1).astype(BF16)

    def residual(ref, kernel, add):
        pieces = []
        for b in range(z.blocks4):
            low = b * Y2 * c
            around = jnp.concatenate([ref[dx, low : low + z.win2 * c, :] for dx in range(3)], axis=0)
            pieces.append(mm(kernel[...], around)[: min(Y2, z.w3 - b * Y2) * c])
        value = jnp.concatenate(pieces, axis=0)
        if add is not None:
            value = value + add
        return jnp.maximum(value, 0.0)

    spread_x(x4, jnp.maximum(total, 0.0))
    inner = residual(x4, t4, None).astype(BF16).astype(F32)
    spread_x(x5, jnp.where(live, inner, 0.0))
    encoded = residual(x5, t5, total).astype(BF16).astype(F32)

    for y in range(z.w3):
        for x in range(z.w3):
            flat[pl.ds(y * z.w3 + x, c, stride=z.w3 * z.w3), :] = encoded[
                y * c : (y + 1) * c, x * z.cap : (x + 1) * z.cap
            ]
    final.wait()
    features = jnp.maximum(mm(flat[...].astype(BF16), proj[...], TN), 0.0).astype(BF16)

    start = jnp.int32(0)
    for a in range(dp):
        start = start + jnp.where(a < dp_index(), counts[tensor_index(), a], 0)
    depth = z.cap // dp
    shape = (dp * tensor * depth, z.cap)
    r = iota(shape, 0)
    receiver, level = r >> log2(tensor * depth), r & (depth - 1)
    arrival = ((receiver - start) & (dp - 1)) + level * dp
    route = one_hot((iota(shape, 1) == arrival) & (arrival < own))
    out[...] = mm(route, features).astype(BF16).reshape(out.shape)


def encode_rows(frames, counts, kernels, projection):
    first, second, third, res_first, res_second = kernels
    z = Sizes(frames.shape, first.shape, second.shape, projection.shape)
    dp, tensor = lax.axis_size("dp"), lax.axis_size("tensor")
    images = jnp.transpose(frames, (0, 2, 1, 3)).reshape(z.cap, z.f * z.c0, z.f)
    ci_co, co_ci = (2, 3, 1, 0), (2, 3, 0, 1)
    n = z.w3 * z.c2
    operands = (
        counts,
        jnp.transpose(first, ci_co),
        jnp.transpose(second, ci_co),
        jnp.transpose(third, co_ci),
        jnp.transpose(res_first, co_ci),
        jnp.transpose(res_second, co_ci),
        images,
        jnp.transpose(projection),
    )
    tall = pltpu.VMEM((3, (Y2 * z.blocks4 + 2) * z.c2, z.wide), BF16)
    band = pltpu.VMEM((Y2 * z.c2, 3 * z.win2 * z.c2), BF16)
    scratch = [pltpu.SMEM(counts.shape, I32)]
    scratch += [pltpu.VMEM(x.shape, x.dtype) for x in operands[1:]]
    scratch += [
        pltpu.VMEM((z.n1 * z.f, 4 * LANES), BF16),
        pltpu.VMEM((2 * LANES, 4 * LANES), BF16),
        pltpu.VMEM((2 * LANES, 6 * LANES), BF16),
        pltpu.VMEM((Y1 * z.c1, 3 * z.win1 * z.c0), BF16),
        pltpu.VMEM((Y2 * z.c2, 3 * z.win2 * z.c1), BF16),
        band,
        band,
        band,
        pltpu.VMEM((4, 4, z.f * z.c0 + 2 * PACK, LANES), BF16),
        pltpu.VMEM((2, z.w1 * z.c1, 2 * LANES), BF16),
        pltpu.VMEM((2, 4, (z.w1 + 2) * z.c1, LANES), BF16),
        pltpu.VMEM((z.w2 * z.c2, 2 * LANES), BF16),
        pltpu.VMEM((3, (z.w2 + 2) * z.c2, 2 * LANES), BF16),
        pltpu.VMEM((z.pairs, n, 2 * LANES), BF16),
        tall,
        tall,
        pltpu.VMEM((z.pairs, 2 * LANES, z.wide), BF16),
        pltpu.VMEM((n * z.w3, z.cap), F32),
        pltpu.SemaphoreType.DMA((len(operands) - 1 + z.pairs,)),
    ]
    body = functools.partial(
        encoder_kernel, z, dp, tensor,
        lambda: lax.axis_index("dp"), lambda: lax.axis_index("tensor"),
    )
    return pl.pallas_call(
        body,
        name="encoder",
        out_shape=jax.ShapeDtypeStruct((dp * tensor, z.cap // dp, z.feat), BF16),
        in_specs=[HBM] * len(operands),
        out_specs=VMEM,
        scratch_shapes=scratch,
        compiler_params=pltpu.CompilerParams(vmem_limit_bytes=40 << 20),
        cost_estimate=pl.CostEstimate(flops=20_000_000_000, bytes_accessed=8_000_000, transcendentals=0),
    )(*[pltpu.with_memory_space_constraint(x, pltpu.HBM) for x in operands])


def recurrent_kernel(index, dp_index, weight, bias, counts, slots, resets, *refs):
    *pieces, out, chosen, back, hidden, held, sems = refs
    gates, share, _ = weight.shape
    slot_count, tall, _ = held.shape
    chunks = gates * share // tall

    def copy(i):
        q, low = divmod(i * tall, share)
        slot = i % slot_count
        return pltpu.make_async_copy(weight.at[q, pl.ds(low, tall)], held.at[slot], sems.at[slot])

    for i in range(slot_count - 1):
        copy(i).start()
    tensor, dp = counts.shape
    width, places = pieces[0].shape
    for behind, piece in enumerate(pieces):
        low = pl.multiple_of(((index() - behind) & (tensor - 1)) * width, width)
        hidden[pl.ds(low, width), :] = piece[...]

    rows, count = chosen.shape[0], slots.shape[1]
    depth = rows // (dp * tensor)
    mine = dp_index()
    exact = lax.Precision.HIGHEST
    tallies = counts[...].astype(F32)
    before = jnp.where(iota((dp, dp), 0) < iota((dp, dp), 1), 1.0, 0.0)
    starts = mm(tallies, before, precision=exact)
    line = iota((rows, 1), 0)
    sender, group, level = line >> log2(tensor * depth), (line >> log2(depth)) & (tensor - 1), line & (depth - 1)
    by_group = jnp.where(iota((rows, tensor), 1) == group, 1.0, 0.0)
    own = iota((rows, dp), 1) == sender

    def of_row(table):
        wide = mm(by_group, table, precision=exact)
        return jnp.sum(jnp.where(own, wide, 0.0), axis=1, keepdims=True).astype(I32)

    start = of_row(starts)
    end = of_row(starts + tallies)
    rank = start + ((mine - start) & (dp - 1)) + level * dp
    balanced = group * (count // tensor) + ((rank - mine) >> log2(dp))
    to_row = one_hot((iota((rows, count), 1) == balanced) & (rank < end))
    of_slot = one_hot(iota((places, count), 0) == slots[...])
    chosen[...] = mm(to_row, of_slot, NT).astype(BF16)

    here = (iota((tensor, dp), 0) == index()) & (iota((tensor, dp), 1) == mine)

    def at_home(table):
        return jnp.sum(jnp.where(here, table, 0.0), axis=(0, 1), keepdims=True).astype(I32)

    arrival = ((sender - at_home(starts)) & (dp - 1)) + level * dp
    live = (iota(back.shape, 1) == arrival) & (arrival < at_home(tallies))
    back[...] = jnp.where(live, 1.0, 0.0)

    keep = 1.0 - resets[...].astype(F32)
    for i in range(chunks):
        q, low = divmod(i * tall, share)
        column = jnp.transpose(jnp.broadcast_to(bias[q : q + 1, low : low + tall], (places, tall)))
        copy(i).wait()
        if i + slot_count - 1 < chunks:
            copy(i + slot_count - 1).start()
        out[i * tall : (i + 1) * tall, :] = mm(held[i % slot_count], hidden[...]) * keep + column


def recurrent(weight, bias, counts, slots, resets, pieces, rows, cap):
    gates, share, hidden = weight.shape
    places = pieces[0].shape[1]
    return pl.pallas_call(
        functools.partial(recurrent_kernel, lambda: lax.axis_index("tensor"), lambda: lax.axis_index("dp")),
        name="recurrent",
        out_shape=(
            jax.ShapeDtypeStruct((gates * share, places), F32),
            jax.ShapeDtypeStruct((rows, places), BF16),
            jax.ShapeDtypeStruct((rows, cap), F32),
        ),
        in_specs=[HBM] + [VMEM] * (4 + len(pieces)),
        out_specs=(VMEM, VMEM, VMEM),
        scratch_shapes=[
            pltpu.VMEM((hidden, places), BF16),
            pltpu.VMEM((6, share // 2, hidden), BF16),
            pltpu.SemaphoreType.DMA((6,)),
        ],
        compiler_params=pltpu.CompilerParams(vmem_limit_bytes=24 << 20),
        cost_estimate=pl.CostEstimate(
            flops=2 * gates * share * hidden * places, bytes_accessed=2 * gates * share * hidden, transcendentals=0
        ),
    )(pltpu.with_memory_space_constraint(weight, pltpu.HBM), bias, counts, slots, resets, *pieces)


def core_kernel(features, sums, chosen, weight, hidden, cell, heads, resets, sent, hidden_out, cell_out):
    share = hidden.shape[0]
    rows = chosen.shape[0]
    picked = chosen[...].astype(F32)
    taken = jnp.sum(picked, axis=0, keepdims=True) > 0.5
    inputs = mm(features[...].reshape(rows, -1), chosen[...], TN).astype(BF16)
    keep = 1.0 - resets[...].astype(F32)
    old_cell = cell[...]

    def gate(q):
        return mm(weight[q], inputs) + sums[q * share : (q + 1) * share, :]

    next_cell = jax.nn.sigmoid(gate(1)) * (old_cell * keep) + jax.nn.sigmoid(gate(0)) * jnp.tanh(gate(2))
    next_hidden = jax.nn.sigmoid(gate(3)) * jnp.tanh(next_cell)
    values = mm(heads[...], next_hidden.astype(BF16))
    sent[...] = mm(picked, values, NT, precision=lax.Precision.HIGHEST)
    cell_out[...] = jnp.where(taken, next_cell, old_cell)
    hidden_out[...] = jnp.where(taken, next_hidden, hidden[...])


def core(features, sums, chosen, weight, hidden, cell, heads, resets):
    share = hidden.shape[0]
    return pl.pallas_call(
        core_kernel,
        name="core",
        out_shape=(
            jax.ShapeDtypeStruct((chosen.shape[0], heads.shape[0]), F32),
            jax.ShapeDtypeStruct(hidden.shape, F32),
            jax.ShapeDtypeStruct(cell.shape, F32),
        ),
        in_specs=[VMEM] * 8,
        out_specs=(VMEM,) * 3,
        compiler_params=pltpu.CompilerParams(vmem_limit_bytes=24 << 20),
        cost_estimate=pl.CostEstimate(
            flops=8 * share * weight.shape[2] * hidden.shape[1], bytes_accessed=4_000_000, transcendentals=0
        ),
    )(features, sums, chosen, weight, hidden, cell, heads, resets)


def answers_kernel(received, back, out):
    out[...] = mm(received[...], back[...], TN, precision=lax.Precision.HIGHEST)


def answers(received, back):
    return pl.pallas_call(
        answers_kernel,
        name="answers",
        out_shape=jax.ShapeDtypeStruct((received.shape[1], back.shape[1]), F32),
        in_specs=[VMEM, VMEM],
        out_specs=VMEM,
        compiler_params=pltpu.CompilerParams(vmem_limit_bytes=8 << 20),
    )(received, back)


def body(
    frames, counts, slot_ids, reset_flags, hidden_state, cell_state,
    conv_first, conv_second, conv_third, res_first, res_second,
    projection, input_weight, recur_weight, gate_bias, head_weight,
):
    tensor = lax.axis_size("tensor")
    own = hidden_state.astype(BF16)
    pieces = [own] + [
        lax.ppermute(own, "tensor", [(i, (i + back) % tensor) for i in range(tensor)])
        for back in range(1, tensor)
    ]
    kernels = (conv_first, conv_second, conv_third, res_first, res_second)
    features = encode_rows(frames, counts, kernels, projection)
    features, pieces = lax.optimization_barrier((features, pieces))
    features = lax.all_to_all(features, ("dp", "tensor"), 0, 0, tiled=True)
    rows = features.shape[0] * features.shape[1]
    sums, chosen, back = recurrent(
        recur_weight, gate_bias, counts, slot_ids, reset_flags, pieces, rows, frames.shape[0]
    )
    sent, hidden_after, cell_after = core(
        features, sums, chosen, input_weight, hidden_state, cell_state, head_weight, reset_flags
    )
    received = lax.all_to_all(sent, ("dp", "tensor"), 0, 0, tiled=True)
    return answers(received, back), hidden_after, cell_after


def solution(mesh):
    return jax.shard_map(
        body,
        mesh=mesh,
        in_specs=(
            P(("dp", "tensor"), None, None, None),
            P(),
            P("dp", None),
            P("dp", None),
            P("tensor", "dp"),
            P("tensor", "dp"),
            P(),
            P(),
            P(),
            P(),
            P(),
            P(),
            P(None, "tensor", None),
            P(None, "tensor", None),
            P(None, "tensor"),
            P(None, "tensor"),
        ),
        out_specs=(P(None, ("dp", "tensor")), P("tensor", "dp"), P("tensor", "dp")),
        check_vma=False,
    )
```
